32 devices in a mesh: dp: 2 (over x), tp: 4 (over z), cp: 4 (over y, core).
Axes of the slice: x: 2, y: 2, z: 4, core: 2. Of those that a mesh axis runs over, the one named last changes fastest.
Arguments:
- hidden: bfloat16 [8192, 4096], P(('dp', 'cp')), parts along dimension 0
- tok_pos: int32 [8192], P(('dp', 'cp')), parts along dimension 0
- norm_gain: float32 [4096], replicated
- w_query: bfloat16 [4096, 4096], P(None, 'tp')
- w_key: bfloat16 [4096, 1024], P(None, 'tp')
- w_value: bfloat16 [4096, 1024], P(None, 'tp')
- w_out: bfloat16 [4096, 4096], P('tp')
Outputs:
- output 1: bfloat16 [8192, 4096], P(('dp', 'cp')), parts along dimension 0
- output 2: bfloat16 [8192, 8, 128], P(('dp', 'cp'), 'tp'), parts along dimension 0
- output 3: bfloat16 [8192, 8, 128], P(('dp', 'cp'), 'tp'), parts along dimension 0
There are 2 independent parts. The reference program is written for one: setup_inputs(seed, part) draws one part's arguments, and reference() takes and returns one part's arrays. A program takes and returns all parts, laid end to end along the dimension named above; an argument that names none is the same for every part.
All inputs are finite; a program needn't handle non-finite values.
Results may differ from the reference program's by a relative error of at most 0.00439956.
Values are sent between devices in bfloat16 or wider.
A program may use at most 1 GiB of HBM per device.

```python
import math
import jax
import jax.numpy as jnp
from jax import lax

D = 4096
HEADS = 32
KV_HEADS = 8
HEAD = 128
SEQ = 4096
RUN_LEN = 128
Q_BLOCK = 128
THETA = 1000000
EPS = 1e-5


def setup_inputs(seed: int = 0, part: int = 0) -> dict:
    shared = jax.random.split(jax.random.key(seed), 5)
    local = jax.random.split(jax.random.fold_in(jax.random.key(seed + 1), part), 4)
    run_order = jax.random.permutation(local[0], SEQ // RUN_LEN)
    tok_pos = (run_order[:, None] * RUN_LEN + jnp.arange(RUN_LEN)[None, :]).reshape(SEQ).astype(jnp.int32)
    waves = jax.random.normal(local[1], (4, D), jnp.float32)
    phases = jax.random.uniform(local[2], (4,), jnp.float32, 0.0, 2.0 * math.pi)
    cycles = jnp.array([0.5, 1.0, 1.5, 2.5], jnp.float32)
    angle = tok_pos.astype(jnp.float32)[:, None] * (cycles * (2.0 * math.pi / SEQ))[None, :] + phases[None, :]
    signal = jnp.dot(jnp.cos(angle), waves)
    noise = jax.random.normal(local[3], (SEQ, D), jnp.float32)
    hidden = (0.25 * signal + 0.2 * noise).astype(jnp.bfloat16)
    norm_gain = 1.0 + 0.3 * jax.random.normal(shared[0], (D,), jnp.float32)
    w_query = (jax.random.normal(shared[1], (D, HEADS * HEAD), jnp.float32) * D ** -0.5).astype(jnp.bfloat16)
    w_key = (jax.random.normal(shared[2], (D, KV_HEADS * HEAD), jnp.float32) * D ** -0.5).astype(jnp.bfloat16)
    w_value = (jax.random.normal(shared[3], (D, KV_HEADS * HEAD), jnp.float32) * D ** -0.5).astype(jnp.bfloat16)
    w_out = (jax.random.normal(shared[4], (HEADS * HEAD, D), jnp.float32) * (HEADS * HEAD) ** -0.5).astype(jnp.bfloat16)
    return {"hidden": hidden, "tok_pos": tok_pos, "norm_gain": norm_gain, "w_query": w_query, "w_key": w_key, "w_value": w_value, "w_out": w_out}


def rope_tables(tok_pos):
    inv_freq = 1.0 / (THETA ** (jnp.arange(0, HEAD, 2, dtype=jnp.float32) / HEAD))
    angles = tok_pos.astype(jnp.float32)[:, None] * inv_freq[None, :]
    return jnp.cos(angles)[:, None, :], jnp.sin(angles)[:, None, :]


def rotate_half(head_vecs, cos_tab, sin_tab):
    half_dim = head_vecs.shape[-1] // 2
    first_half = head_vecs[..., :half_dim].astype(jnp.float32)
    second_half = head_vecs[..., half_dim:].astype(jnp.float32)
    rotated = jnp.concatenate([first_half * cos_tab - second_half * sin_tab, second_half * cos_tab + first_half * sin_tab], axis=-1)
    return rotated.astype(jnp.bfloat16)


def reference(hidden, tok_pos, norm_gain, w_query, w_key, w_value, w_out):
    q_per_kv = HEADS // KV_HEADS
    n_blocks = SEQ // Q_BLOCK
    hid_f32 = hidden.astype(jnp.float32)
    normed = (hid_f32 * lax.rsqrt(jnp.mean(hid_f32 * hid_f32, axis=-1, keepdims=True) + EPS) * norm_gain).astype(jnp.bfloat16)
    queries = jnp.dot(normed, w_query, preferred_element_type=jnp.float32).astype(jnp.bfloat16).reshape(SEQ, HEADS, HEAD)
    keys_raw = jnp.dot(normed, w_key, preferred_element_type=jnp.float32).astype(jnp.bfloat16).reshape(SEQ, KV_HEADS, HEAD)
    values = jnp.dot(normed, w_value, preferred_element_type=jnp.float32).astype(jnp.bfloat16).reshape(SEQ, KV_HEADS, HEAD)
    cos_tab, sin_tab = rope_tables(tok_pos)
    q_rot = rotate_half(queries, cos_tab, sin_tab)
    k_rot = rotate_half(keys_raw, cos_tab, sin_tab)
    attn_scale = HEAD ** -0.5
    k_heads = jnp.transpose(k_rot, (1, 0, 2)).astype(jnp.float32)
    v_heads = jnp.transpose(values, (1, 0, 2)).astype(jnp.float32)
    q_blocks = jnp.transpose(q_rot.reshape(n_blocks, Q_BLOCK, KV_HEADS, q_per_kv, HEAD), (0, 2, 1, 3, 4))
    pos_blocks = tok_pos.reshape(n_blocks, Q_BLOCK)

    def one_block(block_in):
        q_blk, pos_blk = block_in
        allowed = tok_pos[None, :] <= pos_blk[:, None]

        def one_head(head_in):
            q_head, k_head, v_head = head_in
            scores = jnp.einsum("qgd,td->gqt", q_head.astype(jnp.float32), k_head) * attn_scale
            scores = jnp.where(allowed[None], scores, -jnp.inf)
            softmaxed = jax.nn.softmax(scores, axis=-1)
            return jnp.einsum("gqt,td->qgd", softmaxed, v_head)

        return lax.map(one_head, (q_blk, k_heads, v_heads))

    context = lax.map(one_block, (q_blocks, pos_blocks))
    attn_out = jnp.transpose(context, (0, 2, 1, 3, 4)).reshape(SEQ, HEADS * HEAD).astype(jnp.bfloat16)
    attn_proj = jnp.dot(attn_out, w_out, preferred_element_type=jnp.float32)
    return (hid_f32 + attn_proj).astype(jnp.bfloat16), k_rot, values
```

```python
import functools
import math

import jax
import jax.numpy as jnp
from jax import lax
from jax.experimental import pallas as pl
from jax.experimental.pallas import tpu as pltpu
from jax.sharding import PartitionSpec as P

HEAD = 128
THETA = 1000000
EPS = 1e-5
NEG_BIG = -1e30
KB = 128
GROUP = 4
QB = 128


def rope_tables(tok_pos):
    inv_freq = 1.0 / (THETA ** (jnp.arange(0, HEAD, 2, dtype=jnp.float32) / HEAD))
    inv_freq = jnp.concatenate([inv_freq, inv_freq])
    sign = jnp.where(jnp.arange(HEAD) < HEAD // 2, -1.0, 1.0).astype(jnp.float32)
    angles = tok_pos.astype(jnp.float32)[:, None] * inv_freq[None, :]
    return jnp.cos(angles), jnp.sin(angles) * sign[None, :]


def rotate(x_f32, cos_tab, sin_tab):
    x = x_f32.astype(jnp.bfloat16).astype(jnp.float32)
    return (x * cos_tab + pltpu.roll(x, HEAD // 2, 1) * sin_tab).astype(jnp.bfloat16)


def kv_kernel(x_ref, gain_ref, wk_ref, wv_ref, cos_ref, sin_ref, normed_ref, kv_ref):
    x = x_ref[...].astype(jnp.float32)
    var = jnp.mean(x * x, axis=-1, keepdims=True)
    normed = (x * lax.rsqrt(var + EPS) * gain_ref[...]).astype(jnp.bfloat16)
    normed_ref[...] = normed
    n_k = wk_ref.shape[1]
    k = jnp.dot(normed, wk_ref[...], preferred_element_type=jnp.float32)
    v = jnp.dot(normed, wv_ref[...], preferred_element_type=jnp.float32)
    for h in range(n_k // HEAD):
        cols = slice(h * HEAD, (h + 1) * HEAD)
        kv_ref[:, cols] = rotate(k[:, cols], cos_ref[...], sin_ref[...])
    kv_ref[:, n_k:] = v.astype(jnp.bfloat16)


def q_kernel(normed_ref, wq_ref, cos_ref, sin_ref, q_ref):
    for c in range(0, wq_ref.shape[1], 2 * HEAD):
        q = jnp.dot(normed_ref[...], wq_ref[:, c:c + 2 * HEAD], preferred_element_type=jnp.float32)
        for h in range(2):
            q_ref[:, c + h * HEAD:c + (h + 1) * HEAD] = rotate(q[:, h * HEAD:(h + 1) * HEAD], cos_ref[...], sin_ref[...])


def attn_kernel(head, n_kv, kmin_ref, kmax_ref, qmin_ref, qmax_ref, q_ref, posq_ref, posk_ref, kv0, kv1, kv2, kv3, o_ref,
                k_s, v_s, q_s, pq_s, m_s, l_s, acc_s, full_l, part_l, sems):
    step = pl.program_id(0)
    rows = kv0.shape[0]
    n_blocks = kmin_ref.shape[0]
    n_heads = q_ref.shape[1] // HEAD

    @pl.when(step == 0)
    def _():
        copies = []
        for i, src in enumerate((kv0, kv1, kv2, kv3)):
            copies.append(pltpu.make_async_copy(src.at[:, pl.ds(head * HEAD, HEAD)], k_s.at[pl.ds(i * rows, rows), :], sems.at[2 * i]))
            copies.append(pltpu.make_async_copy(src.at[:, pl.ds((n_kv + head) * HEAD, HEAD)], v_s.at[pl.ds(i * rows, rows), :], sems.at[2 * i + 1]))
        for c in copies:
            c.start()
        for c in copies:
            c.wait()

    q_lo = qmin_ref[step]
    q_hi = qmax_ref[step]

    def classify(j, counts):
        n_full, n_part = counts
        lo, hi = kmin_ref[j], kmax_ref[j]
        is_full = hi <= q_lo
        is_part = jnp.logical_and(lo <= q_hi, jnp.logical_not(is_full))

        @pl.when(is_full)
        def _():
            full_l[n_full] = j

        @pl.when(is_part)
        def _():
            part_l[n_part] = j

        return n_full + is_full.astype(jnp.int32), n_part + is_part.astype(jnp.int32)

    n_full, n_part = lax.fori_loop(0, n_blocks, classify, (0, 0))
    n_groups = n_full // GROUP

    def move(i, n_part):
        part_l[n_part] = full_l[n_groups * GROUP + i]
        return n_part + 1

    n_part = lax.fori_loop(0, n_full - n_groups * GROUP, move, n_part)
    n_mgroups = (n_part + GROUP - 1) // GROUP

    def pad(i, _):
        part_l[n_part + i] = 0
        return 0

    lax.fori_loop(0, n_mgroups * GROUP - n_part, pad, 0)

    for h in range(n_heads):
        q_s[h * QB:(h + 1) * QB, :] = q_ref[:, h * HEAD:(h + 1) * HEAD]
        pq_s[h * QB:(h + 1) * QB, :] = posq_ref[...]
    m_s[...] = jnp.full_like(m_s, NEG_BIG)
    l_s[...] = jnp.zeros_like(l_s)
    acc_s[...] = jnp.zeros_like(acc_s)

    scale = HEAD ** -0.5 * math.log2(math.e)
    half = n_heads * QB // 2

    def absorb(blocks, pos_row):
        k = jnp.concatenate([k_s[pl.ds(pl.multiple_of(b * KB, KB), KB), :] for b in blocks], axis=0)
        v = jnp.concatenate([v_s[pl.ds(pl.multiple_of(b * KB, KB), KB), :] for b in blocks], axis=0)
        for part in range(2):
            sl = slice(part * half, (part + 1) * half)
            s = lax.dot_general(q_s[sl, :], k, (((1,), (1,)), ((), ())), preferred_element_type=jnp.float32) * scale
            if pos_row is not None:
                s = jnp.where(pos_row <= pq_s[sl, :], s, NEG_BIG)
            m_old = m_s[sl, :]
            m_new = jnp.maximum(m_old, jnp.max(s, axis=-1, keepdims=True))
            alpha = jnp.exp2(m_old - m_new)
            p = jnp.exp2(s - m_new)
            l_new = p[:, :HEAD]
            for c in range(1, GROUP):
                l_new = l_new + p[:, c * HEAD:(c + 1) * HEAD]
            l_s[sl, :] = l_s[sl, :] * alpha + l_new
            acc_s[sl, :] = acc_s[sl, :] * alpha + jnp.dot(p.astype(jnp.bfloat16), v, preferred_element_type=jnp.float32)
            m_s[sl, :] = m_new

    def full_step(i, _):
        absorb([full_l[i * GROUP + c] for c in range(GROUP)], None)
        return 0

    lax.fori_loop(0, n_groups, full_step, 0)

    def part_step(i, _):
        blocks = [part_l[i * GROUP + c] for c in range(GROUP)]
        rows_pos = [posk_ref[b] + jnp.where(i * GROUP + c < n_part, 0, 1 << 30) for c, b in enumerate(blocks)]
        absorb(blocks, jnp.concatenate(rows_pos, axis=1))
        return 0

    lax.fori_loop(0, n_mgroups, part_step, 0)

    out = (acc_s[...] / jnp.sum(l_s[...], axis=-1, keepdims=True)).astype(jnp.bfloat16)
    for h in range(n_heads):
        o_ref[:, h * HEAD:(h + 1) * HEAD] = out[h * QB:(h + 1) * QB, :]


def solution(mesh):
    n_tp, n_cp, n_dp = mesh.shape["tp"], mesh.shape["cp"], mesh.shape["dp"]
    plane = n_dp * n_cp
    ring = [(i, (i + 1) % n_tp) for i in range(n_tp)]
    swap_core = [(i, i ^ 1) for i in range(n_cp)]
    swap_chip = [(i, i ^ 2) for i in range(n_cp)]

    def local_block(hidden, tok_pos, norm_gain, w_query, w_key, w_value, w_out):
        rows, width = hidden.shape
        q_cols, k_cols = w_query.shape[1], w_key.shape[1]
        n_kv = k_cols // HEAD
        g_cols = q_cols // n_kv
        tp = lax.axis_index("tp")
        plane_idx = lax.axis_index("dp") * n_cp + lax.axis_index("cp")

        slice_rows = w_out.shape[0] // plane
        own_slice = lax.dynamic_slice_in_dim(w_out, plane_idx * slice_rows, slice_rows, axis=0)
        z_slices = lax.all_gather(own_slice, "tp", axis=0, tiled=False)

        cos_tab, sin_tab = rope_tables(tok_pos)
        rb = 256
        row_blk = lambda cols: pl.BlockSpec((rb, cols), lambda i: (i, 0))
        whole = lambda r, c: pl.BlockSpec((r, c), lambda i: (0, 0))
        normed, kv = pl.pallas_call(
            kv_kernel,
            grid=(rows // rb,),
            out_shape=(jax.ShapeDtypeStruct((rows, width), jnp.bfloat16), jax.ShapeDtypeStruct((rows, 2 * k_cols), jnp.bfloat16)),
            in_specs=[row_blk(width), whole(1, width), whole(width, k_cols), whole(width, k_cols), row_blk(HEAD), row_blk(HEAD)],
            out_specs=(row_blk(width), row_blk(2 * k_cols)),
            cost_estimate=pl.CostEstimate(flops=4 * rows * width * k_cols, bytes_accessed=24 << 20, transcendentals=0),
            name="norm_kv",
        )(hidden, norm_gain.reshape(1, width), w_key, w_value, cos_tab, sin_tab)

        pos_row = tok_pos.reshape(rows // KB, 1, KB)
        kv_core = lax.ppermute(kv, "cp", swap_core)
        kv_chip = lax.ppermute(kv, "cp", swap_chip)
        swap_diag = [(i, i ^ 3) for i in range(n_cp)]
        pos_rel = jnp.concatenate([pos_row] + [lax.ppermute(pos_row, "cp", pairs) for pairs in (swap_core, swap_chip, swap_diag)], axis=0)

        q_rot = pl.pallas_call(
            q_kernel,
            grid=(rows // rb,),
            out_shape=jax.ShapeDtypeStruct((rows, q_cols), jnp.bfloat16),
            in_specs=[row_blk(width), whole(width, q_cols), row_blk(HEAD), row_blk(HEAD)],
            out_specs=row_blk(q_cols),
            cost_estimate=pl.CostEstimate(flops=2 * rows * width * q_cols, bytes_accessed=20 << 20, transcendentals=0),
            name="q_rope",
        )(normed, w_query, cos_tab, sin_tab)

        kv_chip, q_rot = lax.optimization_barrier((kv_chip, q_rot))
        kv_diag = lax.ppermute(kv_chip, "cp", swap_core)

        kmin, kmax = jnp.min(pos_rel, axis=(1, 2)), jnp.max(pos_rel, axis=(1, 2))
        n_q = rows // QB
        qpos = tok_pos.reshape(n_q, QB)
        qmin, qmax = jnp.min(qpos, axis=1), jnp.max(qpos, axis=1)
        pos_col = tok_pos.reshape(rows, 1)
        hq = g_cols // HEAD
        smem = pl.BlockSpec(memory_space=pltpu.SMEM)
        anym = pl.BlockSpec(memory_space=pl.ANY)

        def attend(head):
            return pl.pallas_call(
                functools.partial(attn_kernel, head, n_kv),
                grid=(n_q,),
                out_shape=jax.ShapeDtypeStruct((rows, g_cols), jnp.bfloat16),
                in_specs=[smem] * 4 + [pl.BlockSpec((QB, g_cols), lambda i: (i, head)), pl.BlockSpec((QB, 1), lambda i: (i, 0)),
                                       pl.BlockSpec(pos_rel.shape, lambda i: (0, 0, 0))] + [anym] * 4,
                out_specs=pl.BlockSpec((QB, g_cols), lambda i: (i, 0)),
                scratch_shapes=[
                    pltpu.VMEM((n_cp * rows, HEAD), jnp.bfloat16),
                    pltpu.VMEM((n_cp * rows, HEAD), jnp.bfloat16),
                    pltpu.VMEM((hq * QB, HEAD), jnp.bfloat16),
                    pltpu.VMEM((hq * QB, 1), jnp.int32),
                    pltpu.VMEM((hq * QB, 1), jnp.float32),
                    pltpu.VMEM((hq * QB, HEAD), jnp.float32),
                    pltpu.VMEM((hq * QB, HEAD), jnp.float32),
                    pltpu.SMEM((n_cp * rows // KB + GROUP,), jnp.int32),
                    pltpu.SMEM((n_cp * rows // KB + 2 * GROUP,), jnp.int32),
                    pltpu.SemaphoreType.DMA((8,)),
                ],
                cost_estimate=pl.CostEstimate(flops=4 * rows * n_cp * rows * g_cols, bytes_accessed=8 << 20, transcendentals=0),
                name="attend",
            )(kmin, kmax, qmin, qmax, q_rot, pos_col, pos_rel, kv, kv_core, kv_chip, kv_diag)

        acc = None
        blocks = [attend(g) for g in range(n_kv)]
        z_slices, blocks[0] = lax.optimization_barrier((z_slices, blocks[0]))
        w_blocks = [w_out]
        for s in range(1, n_tp):
            piece = lax.dynamic_index_in_dim(z_slices, (tp - s + n_tp) % n_tp, axis=0, keepdims=False)
            w_blocks.append(lax.all_gather(piece, ("dp", "cp"), axis=0, tiled=True))
        for s in range(n_tp):
            nxt = [lax.ppermute(b, "tp", ring) for b in blocks] if s < n_tp - 1 else None
            for g in range(n_kv):
                term = jnp.dot(blocks[g], w_blocks[s][g * g_cols:(g + 1) * g_cols], preferred_element_type=jnp.float32)
                acc = term if acc is None else acc + term
            blocks = nxt
        hidden_out = (hidden.astype(jnp.float32) + acc).astype(jnp.bfloat16)
        k_cache = kv[:, :k_cols].reshape(rows, n_kv, HEAD)
        v_cache = kv[:, k_cols:].reshape(rows, n_kv, HEAD)
        return hidden_out, k_cache, v_cache

    row_spec = P(("dp", "cp"), None)
    cache_spec = P(("dp", "cp"), "tp", None)
    return jax.shard_map(local_block, mesh=mesh, in_specs=(row_spec, P(("dp", "cp")), P(None), P(None, "tp"), P(None, "tp"), P(None, "tp"), P("tp", None)), out_specs=(row_spec, cache_spec, cache_spec), check_vma=False)
```

```python
import functools
import math

import jax
import jax.numpy as jnp
from jax import lax
from jax.experimental import pallas as pl
from jax.experimental.pallas import tpu as pltpu
from jax.sharding import PartitionSpec as P

HEAD = 128
THETA = 1000000
EPS = 1e-5
NEG_BIG = -1e30
KB = 128
GROUP = 4
QB = 128


def rope_tables(tok_pos):
    inv_freq = 1.0 / (THETA ** (jnp.arange(0, HEAD, 2, dtype=jnp.float32) / HEAD))
    inv_freq = jnp.concatenate([inv_freq, inv_freq])
    sign = jnp.where(jnp.arange(HEAD) < HEAD // 2, -1.0, 1.0).astype(jnp.float32)
    angles = tok_pos.astype(jnp.float32)[:, None] * inv_freq[None, :]
    return jnp.cos(angles), jnp.sin(angles) * sign[None, :]


def rotate(x_f32, cos_tab, sin_tab):
    x = x_f32.astype(jnp.bfloat16).astype(jnp.float32)
    return (x * cos_tab + pltpu.roll(x, HEAD // 2, 1) * sin_tab).astype(jnp.bfloat16)


def kv_kernel(x_ref, gain_ref, wk_ref, wv_ref, cos_ref, sin_ref, normed_ref, kv_ref):
    x = x_ref[...].astype(jnp.float32)
    var = jnp.mean(x * x, axis=-1, keepdims=True)
    normed = (x * lax.rsqrt(var + EPS) * gain_ref[...]).astype(jnp.bfloat16)
    normed_ref[...] = normed
    n_k = wk_ref.shape[1]
    k = jnp.dot(normed, wk_ref[...], preferred_element_type=jnp.float32)
    v = jnp.dot(normed, wv_ref[...], preferred_element_type=jnp.float32)
    for h in range(n_k // HEAD):
        cols = slice(h * HEAD, (h + 1) * HEAD)
        kv_ref[:, cols] = rotate(k[:, cols], cos_ref[...], sin_ref[...])
    kv_ref[:, n_k:] = v.astype(jnp.bfloat16)


def q_kernel(normed_ref, wq_ref, cos_ref, sin_ref, q_ref):
    for c in range(0, wq_ref.shape[1], 2 * HEAD):
        q = jnp.dot(normed_ref[...], wq_ref[:, c:c + 2 * HEAD], preferred_element_type=jnp.float32)
        for h in range(2):
            q_ref[:, c + h * HEAD:c + (h + 1) * HEAD] = rotate(q[:, h * HEAD:(h + 1) * HEAD], cos_ref[...], sin_ref[...])


def attn_kernel(head, n_kv, kmin_ref, kmax_ref, qmin_ref, qmax_ref, q_ref, posq_ref, posk_ref, kv0, kv1, kv2, kv3, o_ref,
                k_s, v_s, q_s, pq_s, m_s, l_s, acc_s, full_l, part_l, sems):
    step = pl.program_id(0)
    rows = kv0.shape[0]
    n_blocks = kmin_ref.shape[0]
    n_heads = q_ref.shape[1] // HEAD

    @pl.when(step == 0)
    def _():
        copies = []
        for i, src in enumerate((kv0, kv1, kv2, kv3)):
            copies.append(pltpu.make_async_copy(src.at[:, pl.ds(head * HEAD, HEAD)], k_s.at[pl.ds(i * rows, rows), :], sems.at[2 * i]))
            copies.append(pltpu.make_async_copy(src.at[:, pl.ds((n_kv + head) * HEAD, HEAD)], v_s.at[pl.ds(i * rows, rows), :], sems.at[2 * i + 1]))
        for c in copies:
            c.start()
        for c in copies:
            c.wait()

    q_lo = qmin_ref[step]
    q_hi = qmax_ref[step]

    def classify(j, counts):
        n_full, n_part = counts
        lo, hi = kmin_ref[j], kmax_ref[j]
        is_full = hi <= q_lo
        is_part = jnp.logical_and(lo <= q_hi, jnp.logical_not(is_full))

        @pl.when(is_full)
        def _():
            full_l[n_full] = j

        @pl.when(is_part)
        def _():
            part_l[n_part] = j

        return n_full + is_full.astype(jnp.int32), n_part + is_part.astype(jnp.int32)

    n_full, n_part = lax.fori_loop(0, n_blocks, classify, (0, 0))
    n_groups = n_full // GROUP

    def move(i, n_part):
        part_l[n_part] = full_l[n_groups * GROUP + i]
        return n_part + 1

    n_part = lax.fori_loop(0, n_full - n_groups * GROUP, move, n_part)
    n_mgroups = (n_part + GROUP - 1) // GROUP

    def pad(i, _):
        part_l[n_part + i] = 0
        return 0

    lax.fori_loop(0, n_mgroups * GROUP - n_part, pad, 0)

    for h in range(n_heads):
        q_s[h * QB:(h + 1) * QB, :] = q_ref[:, h * HEAD:(h + 1) * HEAD]
        pq_s[h * QB:(h + 1) * QB, :] = posq_ref[...]
    m_s[...] = jnp.full_like(m_s, NEG_BIG)
    l_s[...] = jnp.zeros_like(l_s)
    acc_s[...] = jnp.zeros_like(acc_s)

    scale = HEAD ** -0.5 * math.log2(math.e)
    half = n_heads * QB // 2

    def absorb(blocks, pos_row):
        k = jnp.concatenate([k_s[pl.ds(pl.multiple_of(b * KB, KB), KB), :] for b in blocks], axis=0)
        v = jnp.concatenate([v_s[pl.ds(pl.multiple_of(b * KB, KB), KB), :] for b in blocks], axis=0)
        for part in range(2):
            sl = slice(part * half, (part + 1) * half)
            s = lax.dot_general(q_s[sl, :], k, (((1,), (1,)), ((), ())), preferred_element_type=jnp.float32) * scale
            if pos_row is not None:
                s = jnp.where(pos_row <= pq_s[sl, :], s, NEG_BIG)
            m_old = m_s[sl, :]
            m_new = jnp.maximum(m_old, jnp.max(s, axis=-1, keepdims=True))
            alpha = jnp.exp2(m_old - m_new)
            p = jnp.exp2(s - m_new)
            l_new = p[:, :HEAD]
            for c in range(1, GROUP):
                l_new = l_new + p[:, c * HEAD:(c + 1) * HEAD]
            l_s[sl, :] = l_s[sl, :] * alpha + l_new
            acc_s[sl, :] = acc_s[sl, :] * alpha + jnp.dot(p.astype(jnp.bfloat16), v, preferred_element_type=jnp.float32)
            m_s[sl, :] = m_new

    def full_step(i, _):
        absorb([full_l[i * GROUP + c] for c in range(GROUP)], None)
        return 0

    lax.fori_loop(0, n_groups, full_step, 0)

    def part_step(i, _):
        blocks = [part_l[i * GROUP + c] for c in range(GROUP)]
        rows_pos = [posk_ref[b] + jnp.where(i * GROUP + c < n_part, 0, 1 << 30) for c, b in enumerate(blocks)]
        absorb(blocks, jnp.concatenate(rows_pos, axis=1))
        return 0

    lax.fori_loop(0, n_mgroups, part_step, 0)

    out = (acc_s[...] / jnp.sum(l_s[...], axis=-1, keepdims=True)).astype(jnp.bfloat16)
    for h in range(n_heads):
        o_ref[:, h * HEAD:(h + 1) * HEAD] = out[h * QB:(h + 1) * QB, :]

TILE = 512
CHUNK = 256


def out_kernel(n_tp, n_cp, o_hbm, w_hbm, z_hbm, x_hbm, out_hbm, o_buf, w_buf, acc, w_t, x_t, y_t,
               o_send, o_recv, w_send, w_recv, w_local, ld_sem, st_sem, own_sem):
    mesh_id = pl.DeviceIdType.MESH
    tp, dp, cp = lax.axis_index("tp"), lax.axis_index("dp"), lax.axis_index("cp")
    core, chip = cp % 2, cp // 2
    cp_y = cp + 2 - 4 * chip
    to_right, to_left = {"tp": (tp + 1) % n_tp}, {"tp": (tp + n_tp - 1) % n_tp}
    to_x, to_y, to_p = {"dp": 1 - dp}, {"cp": cp_y}, {"cp": cp + 1 - 2 * core}
    p_me, p_x, p_y, p_d = dp * n_cp + cp, (1 - dp) * n_cp + cp, dp * n_cp + cp_y, (1 - dp) * n_cp + cp_y
    sl = z_hbm.shape[1]
    width = acc.shape[1]
    n_chunk = o_buf.shape[2] // CHUNK
    n_tile = width // TILE

    barrier = pltpu.get_barrier_semaphore()
    for peer in (to_right, to_left, to_x, to_y, to_p):
        pl.semaphore_signal(barrier, inc=1, device_id=peer, device_id_type=mesh_id)
    pl.semaphore_wait(barrier, 5)

    def o_copy(s, c):
        cols = pl.ds(c * CHUNK, CHUNK)
        src = o_hbm.at[:, cols] if s == 0 else o_buf.at[s, :, cols]
        return pltpu.make_async_remote_copy(src_ref=src, dst_ref=o_buf.at[s + 1, :, cols], send_sem=o_send.at[s, c],
                                            recv_sem=o_recv.at[s, c], device_id=to_right, device_id_type=mesh_id)

    def rows(p, first=0, n=None):
        return pl.ds(pl.multiple_of(p * sl + first, sl // 2), sl if n is None else n)

    def w_copy(k, kind):
        half = sl // 2
        own = z_hbm.at[(tp + n_tp - k - 1) % n_tp]
        idx, peer, where = {
            "own_x": (0, to_x, rows(p_me)), "own_y": (1, to_y, rows(p_me)), "own_p": (2, to_p, rows(p_me)),
            "dx": (3, to_x, rows(p_y, half, half)), "dy": (4, to_y, rows(p_x, 0, half)),
            "px": (5, to_p, rows(p_x)), "py": (6, to_p, rows(p_y)),
            "pd0": (7, to_p, rows(p_d, 0, half)), "pd1": (8, to_p, rows(p_d, half, half)),
        }[kind]
        src = own if idx < 3 else w_buf.at[k, where, :]
        return pltpu.make_async_remote_copy(src_ref=src, dst_ref=w_buf.at[k, where, :], send_sem=w_send.at[k, idx],
                                            recv_sem=w_recv.at[k, idx], device_id=peer, device_id_type=mesh_id)

    def w_own_local(k):
        return pltpu.make_async_copy(z_hbm.at[(tp + n_tp - k - 1) % n_tp], w_buf.at[k, rows(p_me), :], w_local.at[k])

    def start_own(k):
        for kind in ("own_x", "own_y", "own_p"):
            w_copy(k, kind).start()
        w_own_local(k).start()

    def pass_on(k):
        w_copy(k, "own_x").wait_recv()
        w_copy(k, "own_y").wait_recv()
        for kind in ("dx", "dy", "px", "py"):
            w_copy(k, kind).start()

    def pass_diag(k):
        w_copy(k, "dy").wait_recv()
        w_copy(k, "pd0").start()
        w_copy(k, "dx").wait_recv()
        w_copy(k, "pd1").start()

    def complete(k):
        w_own_local(k).wait()
        for kind in ("own_p", "px", "py", "pd0", "pd1"):
            w_copy(k, kind).wait_recv()

    def arrive(s, c):
        o_copy(s, c).wait_recv()
        if s + 1 < n_tp - 1:
            o_copy(s + 1, c).start()

    def tile_cols(t):
        return pl.ds(pl.multiple_of(t * TILE, TILE), TILE)

    def accum(s, k0, k1):
        def body(t, _):
            cols = tile_cols(t)
            acc[:, cols] += jnp.dot(o_buf[s, :, k0:k1], w_buf[s - 1, k0:k1, cols], preferred_element_type=jnp.float32)
            return 0

        lax.fori_loop(0, n_tile, body, 0)

    for c in range(n_chunk):
        o_copy(0, c).start()
    start_own(0)
    own = pltpu.make_async_copy(o_hbm, o_buf.at[0], own_sem)
    own.start()

    def loads(t, slot):
        cols = tile_cols(t)
        return (pltpu.make_async_copy(w_hbm.at[:, cols], w_t.at[slot], ld_sem.at[slot, 0]),
                pltpu.make_async_copy(x_hbm.at[:, cols], x_t.at[slot], ld_sem.at[slot, 1]))

    for d in loads(0, 0):
        d.start()
    own.wait()

    def first(t, _):
        slot = t % 2

        @pl.when(t + 1 < n_tile)
        def _():
            for d in loads(t + 1, (t + 1) % 2):
                d.start()

        for d in loads(t, slot):
            d.wait()
        acc[:, tile_cols(t)] = x_t[slot].astype(jnp.float32) + jnp.dot(o_buf[0], w_t[slot], preferred_element_type=jnp.float32)
        return 0

    lax.fori_loop(0, n_tile, first, 0)

    half_k = n_chunk * CHUNK // 2
    for s in range(1, n_tp):
        last = s == n_tp - 1
        pass_on(s - 1)
        if not last:
            start_own(s)
        arrive(s - 1, 0)
        arrive(s - 1, 1)
        pass_diag(s - 1)
        if not last:
            arrive(s - 1, 2)
        complete(s - 1)
        accum(s, 0, half_k)
        if last:
            arrive(s - 1, 2)
            accum(s, half_k, half_k + CHUNK)
        arrive(s - 1, 3)
        if not last:
            accum(s, half_k, 2 * half_k)

    def store(t, slot):
        return pltpu.make_async_copy(y_t.at[slot], out_hbm.at[:, tile_cols(t)], st_sem.at[slot])

    k0 = half_k + CHUNK

    def final(t, _):
        slot = t % 2

        @pl.when(t >= 2)
        def _():
            store(t - 2, slot).wait()

        cols = tile_cols(t)
        y = acc[:, cols] + jnp.dot(o_buf[n_tp - 1, :, k0:], w_buf[n_tp - 2, k0:, cols], preferred_element_type=jnp.float32)
        y_t[slot] = y.astype(jnp.bfloat16)
        store(t, slot).start()
        return 0

    lax.fori_loop(0, n_tile, final, 0)
    store(n_tile - 2, n_tile % 2).wait()
    store(n_tile - 1, (n_tile - 1) % 2).wait()
    for s in range(n_tp - 1):
        for c in range(n_chunk):
            o_copy(s, c).wait_send()
        for kind in ("own_x", "own_y", "own_p", "dx", "dy", "px", "py", "pd0", "pd1"):
            w_copy(s, kind).wait_send()


def solution(mesh):
    n_tp, n_cp, n_dp = mesh.shape["tp"], mesh.shape["cp"], mesh.shape["dp"]
    plane = n_dp * n_cp
    swap_core = [(i, i ^ 1) for i in range(n_cp)]
    swap_chip = [(i, i ^ 2) for i in range(n_cp)]

    def local_block(hidden, tok_pos, norm_gain, w_query, w_key, w_value, w_out):
        rows, width = hidden.shape
        q_cols, k_cols = w_query.shape[1], w_key.shape[1]
        n_kv = k_cols // HEAD
        g_cols = q_cols // n_kv
        plane_idx = lax.axis_index("dp") * n_cp + lax.axis_index("cp")

        slice_rows = w_out.shape[0] // plane
        own_slice = lax.dynamic_slice_in_dim(w_out, plane_idx * slice_rows, slice_rows, axis=0)
        z_slices = lax.all_gather(own_slice, "tp", axis=0, tiled=False)

        cos_tab, sin_tab = rope_tables(tok_pos)
        rb = 256
        row_blk = lambda cols: pl.BlockSpec((rb, cols), lambda i: (i, 0))
        whole = lambda r, c: pl.BlockSpec((r, c), lambda i: (0, 0))
        normed, kv = pl.pallas_call(
            kv_kernel,
            grid=(rows // rb,),
            out_shape=(jax.ShapeDtypeStruct((rows, width), jnp.bfloat16), jax.ShapeDtypeStruct((rows, 2 * k_cols), jnp.bfloat16)),
            in_specs=[row_blk(width), whole(1, width), whole(width, k_cols), whole(width, k_cols), row_blk(HEAD), row_blk(HEAD)],
            out_specs=(row_blk(width), row_blk(2 * k_cols)),
            cost_estimate=pl.CostEstimate(flops=4 * rows * width * k_cols, bytes_accessed=24 << 20, transcendentals=0),
            name="norm_kv",
        )(hidden, norm_gain.reshape(1, width), w_key, w_value, cos_tab, sin_tab)

        pos_row = tok_pos.reshape(rows // KB, 1, KB)
        kv_core = lax.ppermute(kv, "cp", swap_core)
        kv_chip = lax.ppermute(kv, "cp", swap_chip)
        swap_diag = [(i, i ^ 3) for i in range(n_cp)]
        pos_rel = jnp.concatenate([pos_row] + [lax.ppermute(pos_row, "cp", pairs) for pairs in (swap_core, swap_chip, swap_diag)], axis=0)

        q_rot = pl.pallas_call(
            q_kernel,
            grid=(rows // rb,),
            out_shape=jax.ShapeDtypeStruct((rows, q_cols), jnp.bfloat16),
            in_specs=[row_blk(width), whole(width, q_cols), row_blk(HEAD), row_blk(HEAD)],
            out_specs=row_blk(q_cols),
            cost_estimate=pl.CostEstimate(flops=2 * rows * width * q_cols, bytes_accessed=20 << 20, transcendentals=0),
            name="q_rope",
        )(normed, w_query, cos_tab, sin_tab)

        kv_chip, q_rot = lax.optimization_barrier((kv_chip, q_rot))
        kv_diag = lax.ppermute(kv_chip, "cp", swap_core)

        kmin, kmax = jnp.min(pos_rel, axis=(1, 2)), jnp.max(pos_rel, axis=(1, 2))
        n_q = rows // QB
        qpos = tok_pos.reshape(n_q, QB)
        qmin, qmax = jnp.min(qpos, axis=1), jnp.max(qpos, axis=1)
        pos_col = tok_pos.reshape(rows, 1)
        hq = g_cols // HEAD
        smem = pl.BlockSpec(memory_space=pltpu.SMEM)
        anym = pl.BlockSpec(memory_space=pl.ANY)

        def attend(head):
            return pl.pallas_call(
                functools.partial(attn_kernel, head, n_kv),
                grid=(n_q,),
                out_shape=jax.ShapeDtypeStruct((rows, g_cols), jnp.bfloat16),
                in_specs=[smem] * 4 + [pl.BlockSpec((QB, g_cols), lambda i: (i, head)), pl.BlockSpec((QB, 1), lambda i: (i, 0)),
                                       pl.BlockSpec(pos_rel.shape, lambda i: (0, 0, 0))] + [anym] * 4,
                out_specs=pl.BlockSpec((QB, g_cols), lambda i: (i, 0)),
                scratch_shapes=[
                    pltpu.VMEM((n_cp * rows, HEAD), jnp.bfloat16),
                    pltpu.VMEM((n_cp * rows, HEAD), jnp.bfloat16),
                    pltpu.VMEM((hq * QB, HEAD), jnp.bfloat16),
                    pltpu.VMEM((hq * QB, 1), jnp.int32),
                    pltpu.VMEM((hq * QB, 1), jnp.float32),
                    pltpu.VMEM((hq * QB, HEAD), jnp.float32),
                    pltpu.VMEM((hq * QB, HEAD), jnp.float32),
                    pltpu.SMEM((n_cp * rows // KB + GROUP,), jnp.int32),
                    pltpu.SMEM((n_cp * rows // KB + 2 * GROUP,), jnp.int32),
                    pltpu.SemaphoreType.DMA((8,)),
                ],
                cost_estimate=pl.CostEstimate(flops=4 * rows * n_cp * rows * g_cols, bytes_accessed=8 << 20, transcendentals=0),
                name="attend",
            )(kmin, kmax, qmin, qmax, q_rot, pos_col, pos_rel, kv, kv_core, kv_chip, kv_diag)

        o = jnp.concatenate([attend(g) for g in range(n_kv)], axis=1)
        n_chunk = q_cols // CHUNK
        sl = w_out.shape[0] // plane
        hidden_out = pl.pallas_call(
            functools.partial(out_kernel, n_tp, n_cp),
            out_shape=jax.ShapeDtypeStruct((rows, width), jnp.bfloat16),
            in_specs=[anym] * 4,
            out_specs=anym,
            scratch_shapes=[
                pltpu.VMEM((n_tp, rows, q_cols), jnp.bfloat16),
                pltpu.VMEM((n_tp - 1, q_cols, width), jnp.bfloat16),
                pltpu.VMEM((rows, width), jnp.float32),
                pltpu.VMEM((2, q_cols, TILE), jnp.bfloat16),
                pltpu.VMEM((2, rows, TILE), jnp.bfloat16),
                pltpu.VMEM((2, rows, TILE), jnp.bfloat16),
                pltpu.SemaphoreType.DMA((n_tp - 1, n_chunk)),
                pltpu.SemaphoreType.DMA((n_tp - 1, n_chunk)),
                pltpu.SemaphoreType.DMA((n_tp - 1, 9)),
                pltpu.SemaphoreType.DMA((n_tp - 1, 9)),
                pltpu.SemaphoreType.DMA((n_tp - 1,)),
                pltpu.SemaphoreType.DMA((2, 2)),
                pltpu.SemaphoreType.DMA((2,)),
                pltpu.SemaphoreType.DMA,
            ],
            compiler_params=pltpu.CompilerParams(collective_id=0, has_side_effects=True, vmem_limit_bytes=63 << 20),
            cost_estimate=pl.CostEstimate(flops=2 * n_tp * rows * q_cols * width, bytes_accessed=48 << 20, transcendentals=0),
            name="out_gather",
        )(o, w_out, z_slices, hidden)
        k_cache = kv[:, :k_cols].reshape(rows, n_kv, HEAD)
        v_cache = kv[:, k_cols:].reshape(rows, n_kv, HEAD)
        return hidden_out, k_cache, v_cache

    row_spec = P(("dp", "cp"), None)
    cache_spec = P(("dp", "cp"), "tp", None)
    return jax.shard_map(local_block, mesh=mesh, in_specs=(row_spec, P(("dp", "cp")), P(None), P(None, "tp"), P(None, "tp"), P(None, "tp"), P("tp", None)), out_specs=(row_spec, cache_spec, cache_spec), check_vma=False)
```

```python
import functools
import math

import jax
import jax.numpy as jnp
from jax import lax
from jax.experimental import pallas as pl
from jax.experimental.pallas import tpu as pltpu
from jax.sharding import PartitionSpec as P

HEAD = 128
THETA = 1000000
EPS = 1e-5
NEG_BIG = -1e30
KB = 128
GROUP = 4
WIDE = 8
PARTS = 1
AHEAD = 2
QB = 128


def rope_tables(tok_pos):
    inv_freq = 1.0 / (THETA ** (jnp.arange(0, HEAD, 2, dtype=jnp.float32) / HEAD))
    inv_freq = jnp.concatenate([inv_freq, inv_freq])
    sign = jnp.where(jnp.arange(HEAD) < HEAD // 2, -1.0, 1.0).astype(jnp.float32)
    angles = tok_pos.astype(jnp.float32)[:, None] * inv_freq[None, :]
    return jnp.cos(angles), jnp.sin(angles) * sign[None, :]


def rotate(x_f32, cos_tab, sin_tab):
    x = x_f32.astype(jnp.bfloat16).astype(jnp.float32)
    return (x * cos_tab + pltpu.roll(x, HEAD // 2, 1) * sin_tab).astype(jnp.bfloat16)


def kv_kernel(x_ref, gain_ref, wk_ref, wv_ref, cos_ref, sin_ref, normed_ref, kv_ref):
    x = x_ref[...].astype(jnp.float32)
    var = jnp.mean(x * x, axis=-1, keepdims=True)
    normed = (x * lax.rsqrt(var + EPS) * gain_ref[...]).astype(jnp.bfloat16)
    normed_ref[...] = normed
    n_k = wk_ref.shape[1]
    k = jnp.dot(normed, wk_ref[...], preferred_element_type=jnp.float32)
    v = jnp.dot(normed, wv_ref[...], preferred_element_type=jnp.float32)
    for h in range(n_k // HEAD):
        cols = slice(h * HEAD, (h + 1) * HEAD)
        kv_ref[:, cols] = rotate(k[:, cols], cos_ref[...], sin_ref[...])
    kv_ref[:, n_k:] = v.astype(jnp.bfloat16)


def q_kernel(normed_ref, wq_ref, cos_ref, sin_ref, q_ref):
    for c in range(0, wq_ref.shape[1], 2 * HEAD):
        q = jnp.dot(normed_ref[...], wq_ref[:, c:c + 2 * HEAD], preferred_element_type=jnp.float32)
        for h in range(2):
            q_ref[:, c + h * HEAD:c + (h + 1) * HEAD] = rotate(q[:, h * HEAD:(h + 1) * HEAD], cos_ref[...], sin_ref[...])


def attn_kernel(first, kmin_ref, kmax_ref, qmin_ref, qmax_ref, q_ref, posq_ref, posk_ref, kv0, kv1, kv2, kv3, o_ref,
                kv_s, q_s, pq_s, m_s, l_s, acc_s, full_l, part_l, sems):
    step = pl.program_id(0)
    rows = kv0.shape[0]
    n_blocks = kmin_ref.shape[0]
    n_kv = kv0.shape[1] // (2 * HEAD)
    n_heads = q_ref.shape[1] // HEAD
    per_kv = n_heads // n_kv

    @pl.when(step == 0)
    def _():
        copies = [pltpu.make_async_copy(src, kv_s.at[pl.ds(i * rows, rows), :], sems.at[i]) for i, src in enumerate((kv0, kv1, kv2, kv3))]
        for c in copies:
            c.start()
        for c in copies:
            c.wait()

    q_lo = qmin_ref[first + step]
    q_hi = qmax_ref[first + step]

    def classify(j, counts):
        n_full, n_part = counts
        lo, hi = kmin_ref[j], kmax_ref[j]
        is_full = hi <= q_lo
        is_part = jnp.logical_and(lo <= q_hi, jnp.logical_not(is_full))

        @pl.when(is_full)
        def _():
            full_l[n_full] = j

        @pl.when(is_part)
        def _():
            part_l[n_part] = j

        return n_full + is_full.astype(jnp.int32), n_part + is_part.astype(jnp.int32)

    n_full, n_part = lax.fori_loop(0, n_blocks, classify, (0, 0))
    n_groups = n_full // WIDE

    def move(i, n_part):
        part_l[n_part] = full_l[n_groups * WIDE + i]
        return n_part + 1

    n_part = lax.fori_loop(0, n_full - n_groups * WIDE, move, n_part)
    n_mgroups = (n_part + GROUP - 1) // GROUP

    def pad(i, _):
        part_l[n_part + i] = 0
        return 0

    lax.fori_loop(0, n_mgroups * GROUP - n_part, pad, 0)

    for h in range(n_heads):
        q_s[h * QB:(h + 1) * QB, :] = q_ref[:, h * HEAD:(h + 1) * HEAD]
    part_rows = per_kv * QB // PARTS
    for h in range(part_rows // QB):
        pq_s[h * QB:(h + 1) * QB, :] = jnp.broadcast_to(posq_ref[...], (QB, HEAD))
    m_s[...] = jnp.full_like(m_s, NEG_BIG)
    l_s[...] = jnp.zeros_like(l_s)
    acc_s[...] = jnp.zeros_like(acc_s)

    scale = HEAD ** -0.5 * math.log2(math.e)

    def absorb(blocks, pos_rows):
        def gather(c0):
            return jnp.concatenate([kv_s[pl.ds(pl.multiple_of(b * KB, KB), KB), c0:c0 + HEAD] for b in blocks], axis=0)

        ks = [gather(g * HEAD) for g in range(n_kv)]
        vs = [gather((n_kv + g) * HEAD) for g in range(n_kv)]
        n = len(blocks)
        chains = [(g, slice((g * PARTS + i) * part_rows, (g * PARTS + i + 1) * part_rows)) for i in range(PARTS) for g in range(n_kv)]

        def scores(g, sl):
            return lax.dot_general(q_s[sl, :], ks[g], (((1,), (1,)), ((), ())), preferred_element_type=jnp.float32)

        ahead = [scores(*c) for c in chains[:AHEAD]]
        for i, (g, sl) in enumerate(chains):
            s = ahead[i]
            if i + AHEAD < len(chains):
                ahead.append(scores(*chains[i + AHEAD]))
            cols = [s[:, c * KB:(c + 1) * KB] * scale for c in range(n)]
            if pos_rows is not None:
                cols = [jnp.where(pr <= pq_s[...], c, NEG_BIG) for pr, c in zip(pos_rows, cols)]
            top = cols[0]
            for c in cols[1:]:
                top = jnp.maximum(top, c)
            m_old = m_s[sl, :]
            m_new = jnp.maximum(m_old, jnp.max(top, axis=-1, keepdims=True))
            alpha = jnp.exp2(m_old - m_new)
            p = [jnp.exp2(c - m_new) for c in cols]
            total = p[0]
            for c in p[1:]:
                total = total + c
            l_s[sl, :] = l_s[sl, :] * alpha + total
            pv = jnp.dot(jnp.concatenate([c.astype(jnp.bfloat16) for c in p], axis=1), vs[g], preferred_element_type=jnp.float32)
            acc_s[sl, :] = acc_s[sl, :] * alpha + pv
            m_s[sl, :] = m_new

    def full_step(i, _):
        absorb([full_l[i * WIDE + c] for c in range(WIDE)], None)
        return 0

    lax.fori_loop(0, n_groups, full_step, 0)

    def part_step(i, _):
        blocks = [part_l[i * GROUP + c] for c in range(GROUP)]
        absorb(blocks, [posk_ref[b] + jnp.where(i * GROUP + c < n_part, 0, 1 << 30) for c, b in enumerate(blocks)])
        return 0

    lax.fori_loop(0, n_mgroups, part_step, 0)

    for h in range(n_heads):
        sl = slice(h * QB, (h + 1) * QB)
        o_ref[:, h * HEAD:(h + 1) * HEAD] = (acc_s[sl, :] / jnp.sum(l_s[sl, :], axis=-1, keepdims=True)).astype(jnp.bfloat16)


TILE = 512
N_CHUNK = 4


def out_kernel(n_tp, n_cp, oa_hbm, ob_hbm, la_hbm, w_hbm, z_hbm, x_hbm, out_hbm, o_buf, w_buf, acc, w_t, x_t, y_t,
               o_send, o_recv, w_send, w_recv, w_local, ld_sem, st_sem, own_sem):
    mesh_id = pl.DeviceIdType.MESH
    tp, dp, cp = lax.axis_index("tp"), lax.axis_index("dp"), lax.axis_index("cp")
    core, chip = cp % 2, cp // 2
    cp_y = cp + 2 - 4 * chip
    to_right, to_left = {"tp": (tp + 1) % n_tp}, {"tp": (tp + n_tp - 1) % n_tp}
    to_x, to_y, to_p = {"dp": 1 - dp}, {"cp": cp_y}, {"cp": cp + 1 - 2 * core}
    p_me, p_x, p_y, p_d = dp * n_cp + cp, (1 - dp) * n_cp + cp, dp * n_cp + cp_y, (1 - dp) * n_cp + cp_y
    sl = z_hbm.shape[1]
    n_rows, width = acc.shape
    half = n_rows // 2
    ch = n_rows // N_CHUNK
    n_tile = width // TILE
    last = n_tp - 1

    barrier = pltpu.get_barrier_semaphore()
    for peer in (to_right, to_left, to_x, to_y, to_p):
        pl.semaphore_signal(barrier, inc=1, device_id=peer, device_id_type=mesh_id)
    pl.semaphore_wait(barrier, 5)

    def o_copy(s, c):
        at = pl.ds(c * ch, ch)
        if s == 0:
            src = ob_hbm.at[pl.ds(c * ch - half, ch), :]
        elif s == 1 and c * ch < half:
            src = la_hbm.at[at, :]
        else:
            src = o_buf.at[s, at, :]
        return pltpu.make_async_remote_copy(src_ref=src, dst_ref=o_buf.at[s + 1, at, :], send_sem=o_send.at[s, c],
                                            recv_sem=o_recv.at[s, c], device_id=to_right, device_id_type=mesh_id)

    def rows(p, first=0, n=None):
        return pl.ds(pl.multiple_of(p * sl + first, sl // 2), sl if n is None else n)

    def w_copy(k, kind):
        hs = sl // 2
        own = z_hbm.at[(tp + n_tp - k - 1) % n_tp]
        idx, peer, where = {
            "own_x": (0, to_x, rows(p_me)), "own_y": (1, to_y, rows(p_me)), "own_p": (2, to_p, rows(p_me)),
            "dx": (3, to_x, rows(p_y, hs, hs)), "dy": (4, to_y, rows(p_x, 0, hs)),
            "px": (5, to_p, rows(p_x)), "py": (6, to_p, rows(p_y)),
            "pd0": (7, to_p, rows(p_d, 0, hs)), "pd1": (8, to_p, rows(p_d, hs, hs)),
        }[kind]
        src = own if idx < 3 else w_buf.at[k, where, :]
        return pltpu.make_async_remote_copy(src_ref=src, dst_ref=w_buf.at[k, where, :], send_sem=w_send.at[k, idx],
                                            recv_sem=w_recv.at[k, idx], device_id=peer, device_id_type=mesh_id)

    def w_own_local(k):
        return pltpu.make_async_copy(z_hbm.at[(tp + n_tp - k - 1) % n_tp], w_buf.at[k, rows(p_me), :], w_local.at[k])

    def start_own(k):
        for kind in ("own_x", "own_y", "own_p"):
            w_copy(k, kind).start()
        w_own_local(k).start()

    def pass_on(k):
        w_copy(k, "own_x").wait_recv()
        w_copy(k, "own_y").wait_recv()
        for kind in ("dx", "dy", "px", "py"):
            w_copy(k, kind).start()

    def pass_diag(k):
        w_copy(k, "dy").wait_recv()
        w_copy(k, "pd0").start()
        w_copy(k, "dx").wait_recv()
        w_copy(k, "pd1").start()

    def complete(k):
        w_own_local(k).wait()
        for kind in ("own_p", "px", "py", "pd0", "pd1"):
            w_copy(k, kind).wait_recv()

    def arrive(s, c):
        o_copy(s - 1, c).wait_recv()
        if s < last:
            o_copy(s, c).start()

    def tile_cols(t):
        return pl.ds(pl.multiple_of(t * TILE, TILE), TILE)

    def accum(s, r0, r1):
        def body(t, _):
            cols = tile_cols(t)
            acc[r0:r1, cols] += jnp.dot(o_buf[s, r0:r1, :], w_buf[s - 1, :, cols], preferred_element_type=jnp.float32)
            return 0

        lax.fori_loop(0, n_tile, body, 0)

    for c in (0, 1):
        o_copy(1, c).start()
    for c in (2, 3):
        o_copy(0, c).start()
    start_own(0)
    own = [pltpu.make_async_copy(oa_hbm, o_buf.at[0, pl.ds(0, half), :], own_sem.at[0]),
           pltpu.make_async_copy(ob_hbm, o_buf.at[0, pl.ds(half, half), :], own_sem.at[1]),
           pltpu.make_async_copy(la_hbm, o_buf.at[1, pl.ds(0, half), :], own_sem.at[2])]
    for d in own:
        d.start()

    def loads(t, slot):
        cols = tile_cols(t)
        return (pltpu.make_async_copy(w_hbm.at[:, cols], w_t.at[slot], ld_sem.at[slot, 0]),
                pltpu.make_async_copy(x_hbm.at[:, cols], x_t.at[slot], ld_sem.at[slot, 1]))

    for d in loads(0, 0):
        d.start()
    for d in own:
        d.wait()

    def first(t, _):
        slot = t % 2

        @pl.when(t + 1 < n_tile)
        def _():
            for d in loads(t + 1, (t + 1) % 2):
                d.start()

        for d in loads(t, slot):
            d.wait()
        acc[:, tile_cols(t)] = x_t[slot].astype(jnp.float32) + jnp.dot(o_buf[0], w_t[slot], preferred_element_type=jnp.float32)
        return 0

    lax.fori_loop(0, n_tile, first, 0)

    def store(r0, t, slot):
        return pltpu.make_async_copy(y_t.at[slot], out_hbm.at[pl.ds(r0, ch), tile_cols(t)], st_sem.at[slot])

    def finish(c):
        r0 = c * ch

        def body(t, _):
            slot = t % 2

            @pl.when(t >= 2)
            def _():
                store(r0, t - 2, slot).wait()

            cols = tile_cols(t)
            y = acc[r0:r0 + ch, cols] + jnp.dot(o_buf[last, r0:r0 + ch, :], w_buf[last - 1, :, cols], preferred_element_type=jnp.float32)
            y_t[slot] = y.astype(jnp.bfloat16)
            store(r0, t, slot).start()
            return 0

        lax.fori_loop(0, n_tile, body, 0)
        store(r0, n_tile - 2, n_tile % 2).wait()
        store(r0, n_tile - 1, (n_tile - 1) % 2).wait()

    pass_on(0)
    start_own(1)
    arrive(2, 0)
    arrive(2, 1)
    pass_diag(0)
    arrive(1, 2)
    complete(0)
    accum(1, 0, half)
    arrive(1, 3)
    accum(1, half, n_rows)
    pass_on(1)
    start_own(2)
    arrive(3, 0)
    pass_diag(1)
    arrive(3, 1)
    complete(1)
    accum(2, 0, half)
    arrive(2, 2)
    pass_on(2)
    arrive(2, 3)
    accum(2, half, n_rows)
    pass_diag(2)
    complete(2)
    finish(0)
    finish(1)
    arrive(3, 2)
    finish(2)
    arrive(3, 3)
    finish(3)

    for s in range(last):
        for c in range(N_CHUNK):
            if s > 0 or c >= 2:
                o_copy(s, c).wait_send()
        for kind in ("own_x", "own_y", "own_p", "dx", "dy", "px", "py", "pd0", "pd1"):
            w_copy(s, kind).wait_send()


def solution(mesh):
    n_tp, n_cp, n_dp = mesh.shape["tp"], mesh.shape["cp"], mesh.shape["dp"]
    plane = n_dp * n_cp
    ring = [(i, (i + 1) % n_tp) for i in range(n_tp)]
    swap_core = [(i, i ^ 1) for i in range(n_cp)]
    swap_chip = [(i, i ^ 2) for i in range(n_cp)]

    def local_block(hidden, tok_pos, norm_gain, w_query, w_key, w_value, w_out):
        rows, width = hidden.shape
        q_cols, k_cols = w_query.shape[1], w_key.shape[1]
        n_kv = k_cols // HEAD
        plane_idx = lax.axis_index("dp") * n_cp + lax.axis_index("cp")

        slice_rows = w_out.shape[0] // plane
        own_slice = lax.dynamic_slice_in_dim(w_out, plane_idx * slice_rows, slice_rows, axis=0)
        z_slices = lax.all_gather(own_slice, "tp", axis=0, tiled=False)

        cos_tab, sin_tab = rope_tables(tok_pos)
        rb = 256
        row_blk = lambda cols: pl.BlockSpec((rb, cols), lambda i: (i, 0))
        whole = lambda r, c: pl.BlockSpec((r, c), lambda i: (0, 0))
        normed, kv = pl.pallas_call(
            kv_kernel,
            grid=(rows // rb,),
            out_shape=(jax.ShapeDtypeStruct((rows, width), jnp.bfloat16), jax.ShapeDtypeStruct((rows, 2 * k_cols), jnp.bfloat16)),
            in_specs=[row_blk(width), whole(1, width), whole(width, k_cols), whole(width, k_cols), row_blk(HEAD), row_blk(HEAD)],
            out_specs=(row_blk(width), row_blk(2 * k_cols)),
            cost_estimate=pl.CostEstimate(flops=4 * rows * width * k_cols, bytes_accessed=24 << 20, transcendentals=0),
            name="norm_kv",
        )(hidden, norm_gain.reshape(1, width), w_key, w_value, cos_tab, sin_tab)

        pos_row = tok_pos.reshape(rows // KB, 1, KB)
        kv_core = lax.ppermute(kv, "cp", swap_core)
        kv_chip = lax.ppermute(kv, "cp", swap_chip)
        swap_diag = [(i, i ^ 3) for i in range(n_cp)]
        pos_rel = jnp.concatenate([pos_row] + [lax.ppermute(pos_row, "cp", pairs) for pairs in (swap_core, swap_chip, swap_diag)], axis=0)

        q_rot = pl.pallas_call(
            q_kernel,
            grid=(rows // rb,),
            out_shape=jax.ShapeDtypeStruct((rows, q_cols), jnp.bfloat16),
            in_specs=[row_blk(width), whole(width, q_cols), row_blk(HEAD), row_blk(HEAD)],
            out_specs=row_blk(q_cols),
            cost_estimate=pl.CostEstimate(flops=2 * rows * width * q_cols, bytes_accessed=20 << 20, transcendentals=0),
            name="q_rope",
        )(normed, w_query, cos_tab, sin_tab)

        kv_chip, q_rot = lax.optimization_barrier((kv_chip, q_rot))
        kv_diag = lax.ppermute(kv_chip, "cp", swap_core)

        kmin, kmax = jnp.min(pos_rel, axis=(1, 2)), jnp.max(pos_rel, axis=(1, 2))
        n_q = rows // QB
        qpos = tok_pos.reshape(n_q, QB)
        qmin, qmax = jnp.min(qpos, axis=1), jnp.max(qpos, axis=1)
        pos_col = tok_pos.reshape(rows, 1)
        smem = pl.BlockSpec(memory_space=pltpu.SMEM)
        anym = pl.BlockSpec(memory_space=pl.ANY)

        def attend(part, n_parts):
            steps = n_q // n_parts
            first = part * steps
            n_rows = (q_cols // HEAD) * QB
            blocks_max = n_cp * rows // KB
            return pl.pallas_call(
                functools.partial(attn_kernel, first),
                grid=(steps,),
                out_shape=jax.ShapeDtypeStruct((rows // n_parts, q_cols), jnp.bfloat16),
                in_specs=[smem] * 4 + [pl.BlockSpec((QB, q_cols), lambda i: (first + i, 0)), pl.BlockSpec((QB, 1), lambda i: (first + i, 0)),
                                       pl.BlockSpec(pos_rel.shape, lambda i: (0, 0, 0))] + [anym] * 4,
                out_specs=pl.BlockSpec((QB, q_cols), lambda i: (i, 0)),
                scratch_shapes=[
                    pltpu.VMEM((n_cp * rows, 2 * k_cols), jnp.bfloat16),
                    pltpu.VMEM((n_rows, HEAD), jnp.bfloat16),
                    pltpu.VMEM((n_rows // n_kv // PARTS, HEAD), jnp.int32),
                    pltpu.VMEM((n_rows, HEAD), jnp.float32),
                    pltpu.VMEM((n_rows, HEAD), jnp.float32),
                    pltpu.VMEM((n_rows, HEAD), jnp.float32),
                    pltpu.SMEM((blocks_max + WIDE,), jnp.int32),
                    pltpu.SMEM((blocks_max + WIDE + GROUP,), jnp.int32),
                    pltpu.SemaphoreType.DMA((4,)),
                ],
                cost_estimate=pl.CostEstimate(flops=4 * rows // n_parts * n_cp * rows * q_cols, bytes_accessed=8 << 20, transcendentals=0),
                name="attend",
            )(kmin, kmax, qmin, qmax, q_rot, pos_col, pos_rel, kv, kv_core, kv_chip, kv_diag)

        o_a = attend(0, 2)
        left_a = lax.ppermute(o_a, "tp", ring)
        o_b = attend(1, 2)
        hidden_out = pl.pallas_call(
            functools.partial(out_kernel, n_tp, n_cp),
            out_shape=jax.ShapeDtypeStruct((rows, width), jnp.bfloat16),
            in_specs=[anym] * 6,
            out_specs=anym,
            scratch_shapes=[
                pltpu.VMEM((n_tp, rows, q_cols), jnp.bfloat16),
                pltpu.VMEM((n_tp - 1, q_cols, width), jnp.bfloat16),
                pltpu.VMEM((rows, width), jnp.float32),
                pltpu.VMEM((2, q_cols, TILE), jnp.bfloat16),
                pltpu.VMEM((2, rows, TILE), jnp.bfloat16),
                pltpu.VMEM((2, rows // N_CHUNK, TILE), jnp.bfloat16),
                pltpu.SemaphoreType.DMA((n_tp - 1, N_CHUNK)),
                pltpu.SemaphoreType.DMA((n_tp - 1, N_CHUNK)),
                pltpu.SemaphoreType.DMA((n_tp - 1, 9)),
                pltpu.SemaphoreType.DMA((n_tp - 1, 9)),
                pltpu.SemaphoreType.DMA((n_tp - 1,)),
                pltpu.SemaphoreType.DMA((2, 2)),
                pltpu.SemaphoreType.DMA((2,)),
                pltpu.SemaphoreType.DMA((3,)),
            ],
            compiler_params=pltpu.CompilerParams(collective_id=0, has_side_effects=True, vmem_limit_bytes=63 << 20),
            cost_estimate=pl.CostEstimate(flops=2 * n_tp * rows * q_cols * width, bytes_accessed=48 << 20, transcendentals=0),
            name="out_gather",
        )(o_a, o_b, left_a, w_out, z_slices, hidden)
        k_cache = kv[:, :k_cols].reshape(rows, n_kv, HEAD)
        v_cache = kv[:, k_cols:].reshape(rows, n_kv, HEAD)
        return hidden_out, k_cache, v_cache

    row_spec = P(("dp", "cp"), None)
    cache_spec = P(("dp", "cp"), "tp", None)
    return jax.shard_map(local_block, mesh=mesh, in_specs=(row_spec, P(("dp", "cp")), P(None), P(None, "tp"), P(None, "tp"), P(None, "tp"), P("tp", None)), out_specs=(row_spec, cache_spec, cache_spec), check_vma=False)
```

```python
import functools
import math

import jax
import jax.numpy as jnp
from jax import lax
from jax.experimental import pallas as pl
from jax.experimental.pallas import tpu as pltpu
from jax.sharding import PartitionSpec as P

HEAD = 128
THETA = 1000000
EPS = 1e-5
NEG_BIG = -1e30
KB = 128
GROUP = 4
WIDE = 8
PARTS = 1
AHEAD = 2
QB = 128


def rope_tables(tok_pos):
    inv_freq = 1.0 / (THETA ** (jnp.arange(0, HEAD, 2, dtype=jnp.float32) / HEAD))
    inv_freq = jnp.concatenate([inv_freq, inv_freq])
    sign = jnp.where(jnp.arange(HEAD) < HEAD // 2, -1.0, 1.0).astype(jnp.float32)
    angles = tok_pos.astype(jnp.float32)[:, None] * inv_freq[None, :]
    return jnp.cos(angles), jnp.sin(angles) * sign[None, :]


def rotate(x_f32, cos_tab, sin_tab):
    x = x_f32.astype(jnp.bfloat16).astype(jnp.float32)
    return (x * cos_tab + pltpu.roll(x, HEAD // 2, 1) * sin_tab).astype(jnp.bfloat16)


FRONT_ROWS = 256
FRONT_COLS = 256


def front_kernel(n_cp, x_hbm, pos_hbm, gain_ref, wk_hbm, wv_hbm, wq_hbm, cos_ref, sin_ref, kv_hbm, pos_out, q_hbm,
                 x_t, normed, wkv, wq_v, kv_t, q_t, x_sem, w_sem, kv_sem, q_sem, p_send, p_recv, s_send, s_recv):
    mesh_id = pl.DeviceIdType.MESH
    cp = lax.axis_index("cp")
    core, chip = cp % 2, cp // 2
    cp_p, cp_y = cp + 1 - 2 * core, cp + 2 - 4 * chip
    to_p, to_y, to_d = {"cp": cp_p}, {"cp": cp_y}, {"cp": cp_y + 1 - 2 * core}
    rows = normed.shape[0]
    k_cols = wk_hbm.shape[1]
    n_rb = rows // FRONT_ROWS
    n_cb = wq_hbm.shape[1] // FRONT_COLS

    def x_load(r):
        return pltpu.make_async_copy(x_hbm.at[pl.ds(r * FRONT_ROWS, FRONT_ROWS), :], x_t.at[r % 2], x_sem.at[r % 2])

    weights = [pltpu.make_async_copy(wk_hbm, wkv.at[:, pl.ds(0, k_cols)], w_sem.at[0]),
               pltpu.make_async_copy(wv_hbm, wkv.at[:, pl.ds(k_cols, k_cols)], w_sem.at[1]),
               pltpu.make_async_copy(wq_hbm, wq_v, w_sem.at[2])]
    x_load(0).start()
    weights[0].start()
    weights[1].start()
    x_load(1).start()
    weights[2].start()

    barrier = pltpu.get_barrier_semaphore()
    for peer in (to_p, to_y, to_d):
        pl.semaphore_signal(barrier, inc=1, device_id=peer, device_id_type=mesh_id)
    pl.semaphore_wait(barrier, 3)

    pos_copies = [pltpu.make_async_remote_copy(src_ref=pos_hbm, dst_ref=pos_out.at[i], send_sem=p_send.at[i], recv_sem=p_recv.at[i],
                                               device_id=peer, device_id_type=mesh_id) for i, peer in enumerate((to_p, to_y, to_d))]
    for c in pos_copies:
        c.start()

    def send(kind, r):
        src = (0, 0, 2)[kind] * rows + r * FRONT_ROWS
        dst = (1, 2, 3)[kind] * rows + r * FRONT_ROWS
        return pltpu.make_async_remote_copy(src_ref=kv_hbm.at[pl.ds(src, FRONT_ROWS), :], dst_ref=kv_hbm.at[pl.ds(dst, FRONT_ROWS), :],
                                            send_sem=s_send.at[kind, r], recv_sem=s_recv.at[kind, r],
                                            device_id=(to_p, to_y, to_p)[kind], device_id_type=mesh_id)

    def kv_store(r):
        return pltpu.make_async_copy(kv_t.at[r], kv_hbm.at[pl.ds(r * FRONT_ROWS, FRONT_ROWS), :], kv_sem.at[r])

    def spread(r):
        kv_store(r).wait()
        send(1, r).start()
        send(0, r).start()

    for r in range(n_rb):
        at = slice(r * FRONT_ROWS, (r + 1) * FRONT_ROWS)
        x_load(r).wait()
        x = x_t[r % 2].astype(jnp.float32)
        var = jnp.mean(x * x, axis=-1, keepdims=True)
        normed[at, :] = (x * lax.rsqrt(var + EPS) * gain_ref[...]).astype(jnp.bfloat16)
        if r + 2 < n_rb:
            x_load(r + 2).start()
        if r == 0:
            weights[0].wait()
            weights[1].wait()
        kv = jnp.dot(normed[at, :], wkv[...], preferred_element_type=jnp.float32)
        for h in range(k_cols // HEAD):
            kv_t[r, :, h * HEAD:(h + 1) * HEAD] = rotate(kv[:, h * HEAD:(h + 1) * HEAD], cos_ref[at, :], sin_ref[at, :])
        kv_t[r, :, k_cols:] = kv[:, k_cols:].astype(jnp.bfloat16)
        kv_store(r).start()
        if r > 0:
            spread(r - 1)

    weights[2].wait()

    def q_store(c):
        return pltpu.make_async_copy(q_t.at[c % 2], q_hbm.at[:, pl.ds(c * FRONT_COLS, FRONT_COLS)], q_sem.at[c % 2])

    for c in range(n_cb):
        if c == 0:
            spread(n_rb - 1)
        if c >= 2:
            q_store(c - 2).wait()
        q = jnp.dot(normed[...], wq_v[:, c * FRONT_COLS:(c + 1) * FRONT_COLS], preferred_element_type=jnp.float32)
        for h in range(FRONT_COLS // HEAD):
            q_t[c % 2, :, h * HEAD:(h + 1) * HEAD] = rotate(q[:, h * HEAD:(h + 1) * HEAD], cos_ref[...], sin_ref[...])
        q_store(c).start()
        if c < n_rb:
            send(1, c).wait_recv()
            send(2, c).start()
    for r in range(n_cb, n_rb):
        send(1, r).wait_recv()
        send(2, r).start()

    q_store(n_cb - 2).wait()
    q_store(n_cb - 1).wait()
    for r in range(n_rb):
        send(0, r).wait_recv()
        send(2, r).wait_recv()
    for c in pos_copies:
        c.wait()
    for kind in range(3):
        for r in range(n_rb):
            send(kind, r).wait_send()


def attn_kernel(first, kmin_ref, kmax_ref, qmin_ref, qmax_ref, q_ref, posq_ref, posk_ref, kv_hbm, o_ref,
                kv_s, q_s, pq_s, m_s, l_s, acc_s, full_l, part_l, sem):
    step = pl.program_id(0)
    n_blocks = kmin_ref.shape[0]
    n_kv = kv_hbm.shape[1] // (2 * HEAD)
    n_heads = q_ref.shape[1] // HEAD
    per_kv = n_heads // n_kv

    @pl.when(step == 0)
    def _():
        load = pltpu.make_async_copy(kv_hbm, kv_s, sem)
        load.start()
        load.wait()

    q_lo = qmin_ref[first + step]
    q_hi = qmax_ref[first + step]

    def classify(j, counts):
        n_full, n_part = counts
        lo, hi = kmin_ref[j], kmax_ref[j]
        is_full = hi <= q_lo
        is_part = jnp.logical_and(lo <= q_hi, jnp.logical_not(is_full))

        @pl.when(is_full)
        def _():
            full_l[n_full] = j

        @pl.when(is_part)
        def _():
            part_l[n_part] = j

        return n_full + is_full.astype(jnp.int32), n_part + is_part.astype(jnp.int32)

    n_full, n_part = lax.fori_loop(0, n_blocks, classify, (0, 0))
    n_groups = n_full // WIDE

    def move(i, n_part):
        part_l[n_part] = full_l[n_groups * WIDE + i]
        return n_part + 1

    n_part = lax.fori_loop(0, n_full - n_groups * WIDE, move, n_part)
    n_mgroups = (n_part + GROUP - 1) // GROUP

    def pad(i, _):
        part_l[n_part + i] = 0
        return 0

    lax.fori_loop(0, n_mgroups * GROUP - n_part, pad, 0)

    for h in range(n_heads):
        q_s[h * QB:(h + 1) * QB, :] = q_ref[:, h * HEAD:(h + 1) * HEAD]
    part_rows = per_kv * QB // PARTS
    for h in range(part_rows // QB):
        pq_s[h * QB:(h + 1) * QB, :] = jnp.broadcast_to(posq_ref[...], (QB, HEAD))
    m_s[...] = jnp.full_like(m_s, NEG_BIG)
    l_s[...] = jnp.zeros_like(l_s)
    acc_s[...] = jnp.zeros_like(acc_s)

    scale = HEAD ** -0.5 * math.log2(math.e)

    def absorb(blocks, pos_rows):
        def gather(c0):
            return jnp.concatenate([kv_s[pl.ds(pl.multiple_of(b * KB, KB), KB), c0:c0 + HEAD] for b in blocks], axis=0)

        ks = [gather(g * HEAD) for g in range(n_kv)]
        vs = [gather((n_kv + g) * HEAD) for g in range(n_kv)]
        n = len(blocks)
        chains = [(g, slice((g * PARTS + i) * part_rows, (g * PARTS + i + 1) * part_rows)) for i in range(PARTS) for g in range(n_kv)]

        def scores(g, sl):
            return lax.dot_general(q_s[sl, :], ks[g], (((1,), (1,)), ((), ())), preferred_element_type=jnp.float32)

        ahead = [scores(*c) for c in chains[:AHEAD]]
        for i, (g, sl) in enumerate(chains):
            s = ahead[i]
            if i + AHEAD < len(chains):
                ahead.append(scores(*chains[i + AHEAD]))
            cols = [s[:, c * KB:(c + 1) * KB] * scale for c in range(n)]
            if pos_rows is not None:
                cols = [jnp.where(pr <= pq_s[...], c, NEG_BIG) for pr, c in zip(pos_rows, cols)]
            top = cols[0]
            for c in cols[1:]:
                top = jnp.maximum(top, c)
            m_old = m_s[sl, :]
            m_new = jnp.maximum(m_old, jnp.max(top, axis=-1, keepdims=True))
            alpha = jnp.exp2(m_old - m_new)
            p = [jnp.exp2(c - m_new) for c in cols]
            total = p[0]
            for c in p[1:]:
                total = total + c
            l_s[sl, :] = l_s[sl, :] * alpha + total
            pv = jnp.dot(jnp.concatenate([c.astype(jnp.bfloat16) for c in p], axis=1), vs[g], preferred_element_type=jnp.float32)
            acc_s[sl, :] = acc_s[sl, :] * alpha + pv
            m_s[sl, :] = m_new

    def full_step(i, _):
        absorb([full_l[i * WIDE + c] for c in range(WIDE)], None)
        return 0

    lax.fori_loop(0, n_groups, full_step, 0)

    def part_step(i, _):
        blocks = [part_l[i * GROUP + c] for c in range(GROUP)]
        absorb(blocks, [posk_ref[b] + jnp.where(i * GROUP + c < n_part, 0, 1 << 30) for c, b in enumerate(blocks)])
        return 0

    lax.fori_loop(0, n_mgroups, part_step, 0)

    for h in range(n_heads):
        sl = slice(h * QB, (h + 1) * QB)
        o_ref[:, h * HEAD:(h + 1) * HEAD] = (acc_s[sl, :] / jnp.sum(l_s[sl, :], axis=-1, keepdims=True)).astype(jnp.bfloat16)


TILE = 512
N_CHUNK = 4


def out_kernel(n_tp, n_cp, oa_hbm, ob_hbm, la_hbm, w_hbm, z_hbm, x_hbm, out_hbm, o_buf, w_buf, acc, w_t, x_t, y_t,
               o_send, o_recv, w_send, w_recv, w_local, ld_sem, st_sem, own_sem):
    mesh_id = pl.DeviceIdType.MESH
    tp, dp, cp = lax.axis_index("tp"), lax.axis_index("dp"), lax.axis_index("cp")
    core, chip = cp % 2, cp // 2
    cp_y = cp + 2 - 4 * chip
    to_right, to_left = {"tp": (tp + 1) % n_tp}, {"tp": (tp + n_tp - 1) % n_tp}
    to_x, to_y, to_p = {"dp": 1 - dp}, {"cp": cp_y}, {"cp": cp + 1 - 2 * core}
    p_me, p_x, p_y, p_d = dp * n_cp + cp, (1 - dp) * n_cp + cp, dp * n_cp + cp_y, (1 - dp) * n_cp + cp_y
    sl = z_hbm.shape[1]
    n_rows, width = acc.shape
    half = n_rows // 2
    ch = n_rows // N_CHUNK
    n_tile = width // TILE
    last = n_tp - 1

    barrier = pltpu.get_barrier_semaphore()
    for peer in (to_right, to_left, to_x, to_y, to_p):
        pl.semaphore_signal(barrier, inc=1, device_id=peer, device_id_type=mesh_id)
    pl.semaphore_wait(barrier, 5)

    def o_copy(s, c):
        at = pl.ds(c * ch, ch)
        if s == 0:
            src = ob_hbm.at[pl.ds(c * ch - half, ch), :]
        elif s == 1 and c * ch < half:
            src = la_hbm.at[at, :]
        else:
            src = o_buf.at[s, at, :]
        return pltpu.make_async_remote_copy(src_ref=src, dst_ref=o_buf.at[s + 1, at, :], send_sem=o_send.at[s, c],
                                            recv_sem=o_recv.at[s, c], device_id=to_right, device_id_type=mesh_id)

    def rows(p, first=0, n=None):
        return pl.ds(pl.multiple_of(p * sl + first, sl // 2), sl if n is None else n)

    def w_copy(k, kind):
        hs = sl // 2
        own = z_hbm.at[(tp + n_tp - k - 1) % n_tp]
        idx, peer, where = {
            "own_x": (0, to_x, rows(p_me)), "own_y": (1, to_y, rows(p_me)), "own_p": (2, to_p, rows(p_me)),
            "dx": (3, to_x, rows(p_y, hs, hs)), "dy": (4, to_y, rows(p_x, 0, hs)),
            "px": (5, to_p, rows(p_x)), "py": (6, to_p, rows(p_y)),
            "pd0": (7, to_p, rows(p_d, 0, hs)), "pd1": (8, to_p, rows(p_d, hs, hs)),
        }[kind]
        src = own if idx < 3 else w_buf.at[k, where, :]
        return pltpu.make_async_remote_copy(src_ref=src, dst_ref=w_buf.at[k, where, :], send_sem=w_send.at[k, idx],
                                            recv_sem=w_recv.at[k, idx], device_id=peer, device_id_type=mesh_id)

    def w_own_local(k):
        return pltpu.make_async_copy(z_hbm.at[(tp + n_tp - k - 1) % n_tp], w_buf.at[k, rows(p_me), :], w_local.at[k])

    def start_own(k):
        for kind in ("own_x", "own_y", "own_p"):
            w_copy(k, kind).start()
        w_own_local(k).start()

    def pass_on(k):
        w_copy(k, "own_x").wait_recv()
        w_copy(k, "own_y").wait_recv()
        for kind in ("dx", "dy", "px", "py"):
            w_copy(k, kind).start()

    def pass_diag(k):
        w_copy(k, "dy").wait_recv()
        w_copy(k, "pd0").start()
        w_copy(k, "dx").wait_recv()
        w_copy(k, "pd1").start()

    def complete(k):
        w_own_local(k).wait()
        for kind in ("own_p", "px", "py", "pd0", "pd1"):
            w_copy(k, kind).wait_recv()

    def arrive(s, c):
        o_copy(s - 1, c).wait_recv()
        if s < last:
            o_copy(s, c).start()

    def tile_cols(t):
        return pl.ds(pl.multiple_of(t * TILE, TILE), TILE)

    def accum(s, r0, r1):
        def body(t, _):
            cols = tile_cols(t)
            acc[r0:r1, cols] += jnp.dot(o_buf[s, r0:r1, :], w_buf[s - 1, :, cols], preferred_element_type=jnp.float32)
            return 0

        lax.fori_loop(0, n_tile, body, 0)

    for c in (0, 1):
        o_copy(1, c).start()
    for c in (2, 3):
        o_copy(0, c).start()
    start_own(0)
    own = [pltpu.make_async_copy(oa_hbm, o_buf.at[0, pl.ds(0, half), :], own_sem.at[0]),
           pltpu.make_async_copy(ob_hbm, o_buf.at[0, pl.ds(half, half), :], own_sem.at[1]),
           pltpu.make_async_copy(la_hbm, o_buf.at[1, pl.ds(0, half), :], own_sem.at[2])]
    for d in own:
        d.start()

    def loads(t, slot):
        cols = tile_cols(t)
        return (pltpu.make_async_copy(w_hbm.at[:, cols], w_t.at[slot], ld_sem.at[slot, 0]),
                pltpu.make_async_copy(x_hbm.at[:, cols], x_t.at[slot], ld_sem.at[slot, 1]))

    for d in loads(0, 0):
        d.start()
    for d in own:
        d.wait()

    def first(t, _):
        slot = t % 2

        @pl.when(t + 1 < n_tile)
        def _():
            for d in loads(t + 1, (t + 1) % 2):
                d.start()

        for d in loads(t, slot):
            d.wait()
        acc[:, tile_cols(t)] = x_t[slot].astype(jnp.float32) + jnp.dot(o_buf[0], w_t[slot], preferred_element_type=jnp.float32)
        return 0

    lax.fori_loop(0, n_tile, first, 0)

    def store(r0, t, slot):
        return pltpu.make_async_copy(y_t.at[slot], out_hbm.at[pl.ds(r0, ch), tile_cols(t)], st_sem.at[slot])

    def finish(c):
        r0 = c * ch

        def body(t, _):
            slot = t % 2

            @pl.when(t >= 2)
            def _():
                store(r0, t - 2, slot).wait()

            cols = tile_cols(t)
            y = acc[r0:r0 + ch, cols] + jnp.dot(o_buf[last, r0:r0 + ch, :], w_buf[last - 1, :, cols], preferred_element_type=jnp.float32)
            y_t[slot] = y.astype(jnp.bfloat16)
            store(r0, t, slot).start()
            return 0

        lax.fori_loop(0, n_tile, body, 0)
        store(r0, n_tile - 2, n_tile % 2).wait()
        store(r0, n_tile - 1, (n_tile - 1) % 2).wait()

    pass_on(0)
    start_own(1)
    arrive(2, 0)
    arrive(2, 1)
    pass_diag(0)
    arrive(1, 2)
    complete(0)
    accum(1, 0, half)
    arrive(1, 3)
    accum(1, half, n_rows)
    pass_on(1)
    start_own(2)
    arrive(3, 0)
    pass_diag(1)
    arrive(3, 1)
    complete(1)
    accum(2, 0, half)
    arrive(2, 2)
    pass_on(2)
    arrive(2, 3)
    accum(2, half, n_rows)
    pass_diag(2)
    complete(2)
    finish(0)
    finish(1)
    arrive(3, 2)
    finish(2)
    arrive(3, 3)
    finish(3)

    for s in range(last):
        for c in range(N_CHUNK):
            if s > 0 or c >= 2:
                o_copy(s, c).wait_send()
        for kind in ("own_x", "own_y", "own_p", "dx", "dy", "px", "py", "pd0", "pd1"):
            w_copy(s, kind).wait_send()


def solution(mesh):
    n_tp, n_cp, n_dp = mesh.shape["tp"], mesh.shape["cp"], mesh.shape["dp"]
    plane = n_dp * n_cp
    ring = [(i, (i + 1) % n_tp) for i in range(n_tp)]

    def local_block(hidden, tok_pos, norm_gain, w_query, w_key, w_value, w_out):
        rows, width = hidden.shape
        q_cols, k_cols = w_query.shape[1], w_key.shape[1]
        n_kv = k_cols // HEAD
        plane_idx = lax.axis_index("dp") * n_cp + lax.axis_index("cp")

        slice_rows = w_out.shape[0] // plane
        own_slice = lax.dynamic_slice_in_dim(w_out, plane_idx * slice_rows, slice_rows, axis=0)
        z_slices = lax.all_gather(own_slice, "tp", axis=0, tiled=False)

        cos_tab, sin_tab = rope_tables(tok_pos)
        smem = pl.BlockSpec(memory_space=pltpu.SMEM)
        anym = pl.BlockSpec(memory_space=pl.ANY)
        vmem = pl.BlockSpec(memory_space=pltpu.VMEM)
        pos_row = tok_pos.reshape(rows // KB, 1, KB)
        n_rb = rows // FRONT_ROWS
        kv_all, pos_far, q_rot = pl.pallas_call(
            functools.partial(front_kernel, n_cp),
            out_shape=(jax.ShapeDtypeStruct((n_cp * rows, 2 * k_cols), jnp.bfloat16), jax.ShapeDtypeStruct((n_cp - 1,) + pos_row.shape, jnp.int32),
                       jax.ShapeDtypeStruct((rows, q_cols), jnp.bfloat16)),
            in_specs=[anym, anym, vmem, anym, anym, anym, vmem, vmem],
            out_specs=(anym, anym, anym),
            scratch_shapes=[
                pltpu.VMEM((2, FRONT_ROWS, width), jnp.bfloat16),
                pltpu.VMEM((rows, width), jnp.bfloat16),
                pltpu.VMEM((width, 2 * k_cols), jnp.bfloat16),
                pltpu.VMEM((width, q_cols), jnp.bfloat16),
                pltpu.VMEM((n_rb, FRONT_ROWS, 2 * k_cols), jnp.bfloat16),
                pltpu.VMEM((2, rows, FRONT_COLS), jnp.bfloat16),
                pltpu.SemaphoreType.DMA((2,)),
                pltpu.SemaphoreType.DMA((3,)),
                pltpu.SemaphoreType.DMA((n_rb,)),
                pltpu.SemaphoreType.DMA((2,)),
                pltpu.SemaphoreType.DMA((n_cp - 1,)),
                pltpu.SemaphoreType.DMA((n_cp - 1,)),
                pltpu.SemaphoreType.DMA((3, n_rb)),
                pltpu.SemaphoreType.DMA((3, n_rb)),
            ],
            compiler_params=pltpu.CompilerParams(collective_id=1, has_side_effects=True, vmem_limit_bytes=63 << 20),
            cost_estimate=pl.CostEstimate(flops=2 * rows * width * (q_cols + 2 * k_cols), bytes_accessed=24 << 20, transcendentals=0),
            name="front",
        )(hidden, pos_row, norm_gain.reshape(1, width), w_key, w_value, w_query, cos_tab, sin_tab)
        pos_rel = jnp.concatenate([pos_row, pos_far.reshape(-1, 1, KB)], axis=0)

        kmin, kmax = jnp.min(pos_rel, axis=(1, 2)), jnp.max(pos_rel, axis=(1, 2))
        n_q = rows // QB
        qpos = tok_pos.reshape(n_q, QB)
        qmin, qmax = jnp.min(qpos, axis=1), jnp.max(qpos, axis=1)
        pos_col = tok_pos.reshape(rows, 1)

        def attend(part, n_parts):
            steps = n_q // n_parts
            first = part * steps
            n_rows = (q_cols // HEAD) * QB
            blocks_max = n_cp * rows // KB
            return pl.pallas_call(
                functools.partial(attn_kernel, first),
                grid=(steps,),
                out_shape=jax.ShapeDtypeStruct((rows // n_parts, q_cols), jnp.bfloat16),
                in_specs=[smem] * 4 + [pl.BlockSpec((QB, q_cols), lambda i: (first + i, 0)), pl.BlockSpec((QB, 1), lambda i: (first + i, 0)),
                                       pl.BlockSpec(pos_rel.shape, lambda i: (0, 0, 0)), anym],
                out_specs=pl.BlockSpec((QB, q_cols), lambda i: (i, 0)),
                scratch_shapes=[
                    pltpu.VMEM((n_cp * rows, 2 * k_cols), jnp.bfloat16),
                    pltpu.VMEM((n_rows, HEAD), jnp.bfloat16),
                    pltpu.VMEM((n_rows // n_kv // PARTS, HEAD), jnp.int32),
                    pltpu.VMEM((n_rows, HEAD), jnp.float32),
                    pltpu.VMEM((n_rows, HEAD), jnp.float32),
                    pltpu.VMEM((n_rows, HEAD), jnp.float32),
                    pltpu.SMEM((blocks_max + WIDE,), jnp.int32),
                    pltpu.SMEM((blocks_max + WIDE + GROUP,), jnp.int32),
                    pltpu.SemaphoreType.DMA,
                ],
                cost_estimate=pl.CostEstimate(flops=4 * rows // n_parts * n_cp * rows * q_cols, bytes_accessed=8 << 20, transcendentals=0),
                name="attend",
            )(kmin, kmax, qmin, qmax, q_rot, pos_col, pos_rel, kv_all)

        o_a = attend(0, 2)
        left_a = lax.ppermute(o_a, "tp", ring)
        o_b = attend(1, 2)
        hidden_out = pl.pallas_call(
            functools.partial(out_kernel, n_tp, n_cp),
            out_shape=jax.ShapeDtypeStruct((rows, width), jnp.bfloat16),
            in_specs=[anym] * 6,
            out_specs=anym,
            scratch_shapes=[
                pltpu.VMEM((n_tp, rows, q_cols), jnp.bfloat16),
                pltpu.VMEM((n_tp - 1, q_cols, width), jnp.bfloat16),
                pltpu.VMEM((rows, width), jnp.float32),
                pltpu.VMEM((2, q_cols, TILE), jnp.bfloat16),
                pltpu.VMEM((2, rows, TILE), jnp.bfloat16),
                pltpu.VMEM((2, rows // N_CHUNK, TILE), jnp.bfloat16),
                pltpu.SemaphoreType.DMA((n_tp - 1, N_CHUNK)),
                pltpu.SemaphoreType.DMA((n_tp - 1, N_CHUNK)),
                pltpu.SemaphoreType.DMA((n_tp - 1, 9)),
                pltpu.SemaphoreType.DMA((n_tp - 1, 9)),
                pltpu.SemaphoreType.DMA((n_tp - 1,)),
                pltpu.SemaphoreType.DMA((2, 2)),
                pltpu.SemaphoreType.DMA((2,)),
                pltpu.SemaphoreType.DMA((3,)),
            ],
            compiler_params=pltpu.CompilerParams(collective_id=0, has_side_effects=True, vmem_limit_bytes=63 << 20),
            cost_estimate=pl.CostEstimate(flops=2 * n_tp * rows * q_cols * width, bytes_accessed=48 << 20, transcendentals=0),
            name="out_gather",
        )(o_a, o_b, left_a, w_out, z_slices, hidden)
        k_cache = kv_all[:rows, :k_cols].reshape(rows, n_kv, HEAD)
        v_cache = kv_all[:rows, k_cols:].reshape(rows, n_kv, HEAD)
        return hidden_out, k_cache, v_cache

    row_spec = P(("dp", "cp"), None)
    cache_spec = P(("dp", "cp"), "tp", None)
    return jax.shard_map(local_block, mesh=mesh, in_specs=(row_spec, P(("dp", "cp")), P(None), P(None, "tp"), P(None, "tp"), P(None, "tp"), P("tp", None)), out_specs=(row_spec, cache_spec, cache_spec), check_vma=False)
```

```python
import functools
import math

import jax
import jax.numpy as jnp
from jax import lax
from jax.experimental import pallas as pl
from jax.experimental.pallas import tpu as pltpu
from jax.sharding import PartitionSpec as P


HEAD = 128
THETA = 1000000
EPS = 1e-5
NEG_BIG = -1e30
KB = 128
GROUP = 4
WIDE = 8
PARTS = 1
AHEAD = 2
QB = 128


def rope_tables(tok_pos):
    inv_freq = 1.0 / (THETA ** (jnp.arange(0, HEAD, 2, dtype=jnp.float32) / HEAD))
    inv_freq = jnp.concatenate([inv_freq, inv_freq])
    sign = jnp.where(jnp.arange(HEAD) < HEAD // 2, -1.0, 1.0).astype(jnp.float32)
    angles = tok_pos.astype(jnp.float32)[:, None] * inv_freq[None, :]
    return jnp.cos(angles), jnp.sin(angles) * sign[None, :]


def rotate(x_f32, cos_tab, sin_tab):
    x = x_f32.astype(jnp.bfloat16).astype(jnp.float32)
    return (x * cos_tab + pltpu.roll(x, HEAD // 2, 1) * sin_tab).astype(jnp.bfloat16)


FRONT_ROWS = 256
FRONT_COLS = 256


def front_kernel(n_tp, n_cp, slice_rows, x_hbm, pos_hbm, gain_ref, wk_hbm, wv_hbm, wq_hbm, wo_hbm, cos_ref, sin_ref, kv_hbm, pos_out, q_hbm, wz_hbm, relay_hbm,
                 x_t, normed, wkv, wq_v, kv_t, q_t, x_sem, w_sem, kv_sem, q_sem, p_send, p_recv, s_send, s_recv, z_send, z_recv):
    mesh_id = pl.DeviceIdType.MESH
    tp, dp, cp = lax.axis_index("tp"), lax.axis_index("dp"), lax.axis_index("cp")
    to_right, to_left = {"tp": (tp + 1) % n_tp}, {"tp": (tp + n_tp - 1) % n_tp}
    core, chip = cp % 2, cp // 2
    cp_p, cp_y = cp + 1 - 2 * core, cp + 2 - 4 * chip
    to_p, to_y, to_d = {"cp": cp_p}, {"cp": cp_y}, {"cp": cp_y + 1 - 2 * core}
    rows = normed.shape[0]
    k_cols = wk_hbm.shape[1]
    n_rb = rows // FRONT_ROWS
    n_cb = wq_hbm.shape[1] // FRONT_COLS

    def x_load(r):
        return pltpu.make_async_copy(x_hbm.at[pl.ds(r * FRONT_ROWS, FRONT_ROWS), :], x_t.at[r % 2], x_sem.at[r % 2])

    weights = [pltpu.make_async_copy(wk_hbm, wkv.at[:, pl.ds(0, k_cols)], w_sem.at[0]),
               pltpu.make_async_copy(wv_hbm, wkv.at[:, pl.ds(k_cols, k_cols)], w_sem.at[1]),
               pltpu.make_async_copy(wq_hbm, wq_v, w_sem.at[2])]
    x_load(0).start()
    weights[0].start()
    weights[1].start()
    x_load(1).start()
    weights[2].start()

    barrier = pltpu.get_barrier_semaphore()
    for peer in (to_p, to_y, to_d, to_right, to_left):
        pl.semaphore_signal(barrier, inc=1, device_id=peer, device_id_type=mesh_id)
    pl.semaphore_wait(barrier, 5)

    hs = slice_rows // 2
    own = (dp * n_cp + cp) * slice_rows

    def z_copy(i):
        src, dst = ((wo_hbm.at[pl.ds(pl.multiple_of(own, hs), hs), :], wz_hbm),
                    (wo_hbm.at[pl.ds(pl.multiple_of(own + hs, hs), hs), :], relay_hbm.at[0]),
                    (wz_hbm, relay_hbm.at[1]))[i]
        return pltpu.make_async_remote_copy(src_ref=src, dst_ref=dst, send_sem=z_send.at[i], recv_sem=z_recv.at[i],
                                            device_id=to_right, device_id_type=mesh_id)

    z_copy(0).start()
    z_copy(1).start()

    pos_copies = [pltpu.make_async_remote_copy(src_ref=pos_hbm, dst_ref=pos_out.at[i], send_sem=p_send.at[i], recv_sem=p_recv.at[i],
                                               device_id=peer, device_id_type=mesh_id) for i, peer in enumerate((to_p, to_y, to_d))]
    for c in pos_copies:
        c.start()

    def send(kind, r):
        src = (0, 0, 2)[kind] * rows + r * FRONT_ROWS
        dst = (1, 2, 3)[kind] * rows + r * FRONT_ROWS
        return pltpu.make_async_remote_copy(src_ref=kv_hbm.at[pl.ds(src, FRONT_ROWS), :], dst_ref=kv_hbm.at[pl.ds(dst, FRONT_ROWS), :],
                                            send_sem=s_send.at[kind, r], recv_sem=s_recv.at[kind, r],
                                            device_id=(to_p, to_y, to_p)[kind], device_id_type=mesh_id)

    def kv_store(r):
        return pltpu.make_async_copy(kv_t.at[r], kv_hbm.at[pl.ds(r * FRONT_ROWS, FRONT_ROWS), :], kv_sem.at[r])

    def spread(r):
        kv_store(r).wait()
        send(1, r).start()
        send(0, r).start()

    for r in range(n_rb):
        at = slice(r * FRONT_ROWS, (r + 1) * FRONT_ROWS)
        x_load(r).wait()
        x = x_t[r % 2].astype(jnp.float32)
        var = jnp.mean(x * x, axis=-1, keepdims=True)
        normed[at, :] = (x * lax.rsqrt(var + EPS) * gain_ref[...]).astype(jnp.bfloat16)
        if r + 2 < n_rb:
            x_load(r + 2).start()
        if r == 0:
            weights[0].wait()
            weights[1].wait()
        kv = jnp.dot(normed[at, :], wkv[...], preferred_element_type=jnp.float32)
        for h in range(k_cols // HEAD):
            kv_t[r, :, h * HEAD:(h + 1) * HEAD] = rotate(kv[:, h * HEAD:(h + 1) * HEAD], cos_ref[at, :], sin_ref[at, :])
        kv_t[r, :, k_cols:] = kv[:, k_cols:].astype(jnp.bfloat16)
        kv_store(r).start()
        if r > 0:
            spread(r - 1)

    weights[2].wait()
    z_copy(0).wait_recv()
    z_copy(2).start()

    def q_store(c):
        return pltpu.make_async_copy(q_t.at[c % 2], q_hbm.at[:, pl.ds(c * FRONT_COLS, FRONT_COLS)], q_sem.at[c % 2])

    for c in range(n_cb):
        if c == 0:
            spread(n_rb - 1)
        if c >= 2:
            q_store(c - 2).wait()
        q = jnp.dot(normed[...], wq_v[:, c * FRONT_COLS:(c + 1) * FRONT_COLS], preferred_element_type=jnp.float32)
        for h in range(FRONT_COLS // HEAD):
            q_t[c % 2, :, h * HEAD:(h + 1) * HEAD] = rotate(q[:, h * HEAD:(h + 1) * HEAD], cos_ref[...], sin_ref[...])
        q_store(c).start()
        if c < n_rb:
            send(1, c).wait_recv()
            send(2, c).start()
    for r in range(n_cb, n_rb):
        send(1, r).wait_recv()
        send(2, r).start()

    q_store(n_cb - 2).wait()
    q_store(n_cb - 1).wait()
    for r in range(n_rb):
        send(0, r).wait_recv()
        send(2, r).wait_recv()
    for c in pos_copies:
        c.wait()
    z_copy(1).wait_recv()
    z_copy(2).wait_recv()
    for i in range(3):
        z_copy(i).wait_send()
    for kind in range(3):
        for r in range(n_rb):
            send(kind, r).wait_send()


def attn_kernel(first, kmin_ref, kmax_ref, qmin_ref, qmax_ref, q_ref, posq_ref, posk_ref, kv_hbm, o_ref,
                kv_s, q_s, pq_s, m_s, l_s, acc_s, full_l, part_l, sem):
    step = pl.program_id(0)
    n_blocks = kmin_ref.shape[0]
    n_kv = kv_hbm.shape[1] // (2 * HEAD)
    n_heads = q_ref.shape[1] // HEAD
    per_kv = n_heads // n_kv

    @pl.when(step == 0)
    def _():
        load = pltpu.make_async_copy(kv_hbm, kv_s, sem)
        load.start()
        load.wait()

    q_lo = qmin_ref[first + step]
    q_hi = qmax_ref[first + step]

    def classify(j, counts):
        n_full, n_part = counts
        lo, hi = kmin_ref[j], kmax_ref[j]
        is_full = hi <= q_lo
        is_part = jnp.logical_and(lo <= q_hi, jnp.logical_not(is_full))

        @pl.when(is_full)
        def _():
            full_l[n_full] = j

        @pl.when(is_part)
        def _():
            part_l[n_part] = j

        return n_full + is_full.astype(jnp.int32), n_part + is_part.astype(jnp.int32)

    n_full, n_part = lax.fori_loop(0, n_blocks, classify, (0, 0))
    n_groups = n_full // WIDE

    def move(i, n_part):
        part_l[n_part] = full_l[n_groups * WIDE + i]
        return n_part + 1

    n_part = lax.fori_loop(0, n_full - n_groups * WIDE, move, n_part)
    n_mgroups = (n_part + GROUP - 1) // GROUP

    def pad(i, _):
        part_l[n_part + i] = 0
        return 0

    lax.fori_loop(0, n_mgroups * GROUP - n_part, pad, 0)

    for h in range(n_heads):
        q_s[h * QB:(h + 1) * QB, :] = q_ref[:, h * HEAD:(h + 1) * HEAD]
    part_rows = per_kv * QB // PARTS
    for h in range(part_rows // QB):
        pq_s[h * QB:(h + 1) * QB, :] = jnp.broadcast_to(posq_ref[...], (QB, HEAD))
    m_s[...] = jnp.full_like(m_s, NEG_BIG)
    l_s[...] = jnp.zeros_like(l_s)
    acc_s[...] = jnp.zeros_like(acc_s)

    scale = HEAD ** -0.5 * math.log2(math.e)

    def absorb(blocks, pos_rows):
        def gather(c0):
            return jnp.concatenate([kv_s[pl.ds(pl.multiple_of(b * KB, KB), KB), c0:c0 + HEAD] for b in blocks], axis=0)

        ks = [gather(g * HEAD) for g in range(n_kv)]
        vs = [gather((n_kv + g) * HEAD) for g in range(n_kv)]
        n = len(blocks)
        chains = [(g, slice((g * PARTS + i) * part_rows, (g * PARTS + i + 1) * part_rows)) for i in range(PARTS) for g in range(n_kv)]

        def scores(g, sl):
            return lax.dot_general(q_s[sl, :], ks[g], (((1,), (1,)), ((), ())), preferred_element_type=jnp.float32)

        ahead = [scores(*c) for c in chains[:AHEAD]]
        for i, (g, sl) in enumerate(chains):
            s = ahead[i]
            if i + AHEAD < len(chains):
                ahead.append(scores(*chains[i + AHEAD]))
            cols = [s[:, c * KB:(c + 1) * KB] * scale for c in range(n)]
            if pos_rows is not None:
                cols = [jnp.where(pr <= pq_s[...], c, NEG_BIG) for pr, c in zip(pos_rows, cols)]
            top = cols[0]
            for c in cols[1:]:
                top = jnp.maximum(top, c)
            m_old = m_s[sl, :]
            m_new = jnp.maximum(m_old, jnp.max(top, axis=-1, keepdims=True))
            alpha = jnp.exp2(m_old - m_new)
            p = [jnp.exp2(c - m_new) for c in cols]
            total = p[0]
            for c in p[1:]:
                total = total + c
            l_s[sl, :] = l_s[sl, :] * alpha + total
            pv = jnp.dot(jnp.concatenate([c.astype(jnp.bfloat16) for c in p], axis=1), vs[g], preferred_element_type=jnp.float32)
            acc_s[sl, :] = acc_s[sl, :] * alpha + pv
            m_s[sl, :] = m_new

    def full_step(i, _):
        absorb([full_l[i * WIDE + c] for c in range(WIDE)], None)
        return 0

    lax.fori_loop(0, n_groups, full_step, 0)

    def part_step(i, _):
        blocks = [part_l[i * GROUP + c] for c in range(GROUP)]
        absorb(blocks, [posk_ref[b] + jnp.where(i * GROUP + c < n_part, 0, 1 << 30) for c, b in enumerate(blocks)])
        return 0

    lax.fori_loop(0, n_mgroups, part_step, 0)

    for h in range(n_heads):
        sl = slice(h * QB, (h + 1) * QB)
        o_ref[:, h * HEAD:(h + 1) * HEAD] = (acc_s[sl, :] / jnp.sum(l_s[sl, :], axis=-1, keepdims=True)).astype(jnp.bfloat16)


TILE = 512
N_CHUNK = 4


def out_kernel(n_tp, n_cp, sl, oa_hbm, ob_hbm, la_hbm, w_hbm, wz_hbm, relay_hbm, relay2_hbm, x_hbm, out_hbm, o_buf, w_buf, acc, w_t, x_t, y_t,
               o_send, o_recv, w_send, w_recv, w_local, ld_sem, st_sem, own_sem, z_send, z_recv):
    mesh_id = pl.DeviceIdType.MESH
    tp, dp, cp = lax.axis_index("tp"), lax.axis_index("dp"), lax.axis_index("cp")
    core, chip = cp % 2, cp // 2
    cp_y = cp + 2 - 4 * chip
    to_right, to_left = {"tp": (tp + 1) % n_tp}, {"tp": (tp + n_tp - 1) % n_tp}
    to_x, to_y, to_p = {"dp": 1 - dp}, {"cp": cp_y}, {"cp": cp + 1 - 2 * core}
    p_me, p_x, p_y, p_d = dp * n_cp + cp, (1 - dp) * n_cp + cp, dp * n_cp + cp_y, (1 - dp) * n_cp + cp_y
    n_rows, width = acc.shape
    half = n_rows // 2
    ch = n_rows // N_CHUNK
    n_tile = width // TILE
    last = n_tp - 1

    barrier = pltpu.get_barrier_semaphore()
    for peer in (to_right, to_left, to_x, to_y, to_p):
        pl.semaphore_signal(barrier, inc=1, device_id=peer, device_id_type=mesh_id)
    pl.semaphore_wait(barrier, 5)

    def o_copy(s, c):
        at = pl.ds(c * ch, ch)
        if s == 0:
            src = ob_hbm.at[pl.ds(c * ch - half, ch), :]
        elif s == 1 and c * ch < half:
            src = la_hbm.at[at, :]
        else:
            src = o_buf.at[s, at, :]
        return pltpu.make_async_remote_copy(src_ref=src, dst_ref=o_buf.at[s + 1, at, :], send_sem=o_send.at[s, c],
                                            recv_sem=o_recv.at[s, c], device_id=to_right, device_id_type=mesh_id)

    def rows(p, first=0, n=None):
        return pl.ds(pl.multiple_of(p * sl + first, sl // 2), sl if n is None else n)

    def w_copy(k, kind):
        hs = sl // 2
        idx, peer, where = {
            "own_x": (0, to_x, rows(p_me)), "own_y": (1, to_y, rows(p_me)), "own_p": (2, to_p, rows(p_me)),
            "dx": (3, to_x, rows(p_y, hs, hs)), "dy": (4, to_y, rows(p_x, 0, hs)),
            "px": (5, to_p, rows(p_x)), "py": (6, to_p, rows(p_y)),
            "pd0": (7, to_p, rows(p_d, 0, hs)), "pd1": (8, to_p, rows(p_d, hs, hs)),
        }[kind]
        at = w_buf.at[k, where, :]
        return pltpu.make_async_remote_copy(src_ref=at, dst_ref=at, send_sem=w_send.at[k, idx],
                                            recv_sem=w_recv.at[k, idx], device_id=peer, device_id_type=mesh_id)

    hs = sl // 2

    def w_own_half(k, h):
        src = ((wz_hbm, relay_hbm.at[0]), (relay_hbm.at[1], relay2_hbm.at[0]), (relay2_hbm.at[1], None))[k][h]
        return pltpu.make_async_copy(src, w_buf.at[k, rows(p_me, h * hs, hs), :], w_local.at[k, h])

    def w_last_half():
        return pltpu.make_async_remote_copy(src_ref=relay2_hbm.at[0], dst_ref=w_buf.at[last - 1, rows(p_me, hs, hs), :], send_sem=z_send,
                                            recv_sem=z_recv, device_id=to_right, device_id_type=mesh_id)

    def start_own(k):
        w_own_half(k, 0).wait()
        if k < last - 1:
            w_own_half(k, 1).wait()
        else:
            w_last_half().wait_recv()
        for kind in ("own_x", "own_y", "own_p"):
            w_copy(k, kind).start()

    def pass_on(k):
        w_copy(k, "own_x").wait_recv()
        w_copy(k, "own_y").wait_recv()
        for kind in ("dx", "dy", "px", "py"):
            w_copy(k, kind).start()

    def pass_diag(k):
        w_copy(k, "dy").wait_recv()
        w_copy(k, "pd0").start()
        w_copy(k, "dx").wait_recv()
        w_copy(k, "pd1").start()

    def complete(k):
        for kind in ("own_p", "px", "py", "pd0", "pd1"):
            w_copy(k, kind).wait_recv()

    def arrive(s, c):
        o_copy(s - 1, c).wait_recv()
        if s < last:
            o_copy(s, c).start()

    def tile_cols(t):
        return pl.ds(pl.multiple_of(t * TILE, TILE), TILE)

    def accum(s, r0, r1):
        def body(t, _):
            cols = tile_cols(t)
            acc[r0:r1, cols] += jnp.dot(o_buf[s, r0:r1, :], w_buf[s - 1, :, cols], preferred_element_type=jnp.float32)
            return 0

        lax.fori_loop(0, n_tile, body, 0)

    for k in range(last):
        w_own_half(k, 0).start()
        if k < last - 1:
            w_own_half(k, 1).start()
    for c in (0, 1):
        o_copy(1, c).start()
    w_last_half().start()
    for c in (2, 3):
        o_copy(0, c).start()
    start_own(0)
    own = [pltpu.make_async_copy(oa_hbm, o_buf.at[0, pl.ds(0, half), :], own_sem.at[0]),
           pltpu.make_async_copy(ob_hbm, o_buf.at[0, pl.ds(half, half), :], own_sem.at[1]),
           pltpu.make_async_copy(la_hbm, o_buf.at[1, pl.ds(0, half), :], own_sem.at[2])]
    for d in own:
        d.start()

    def loads(t, slot):
        cols = tile_cols(t)
        return (pltpu.make_async_copy(w_hbm.at[:, cols], w_t.at[slot], ld_sem.at[slot, 0]),
                pltpu.make_async_copy(x_hbm.at[:, cols], x_t.at[slot], ld_sem.at[slot, 1]))

    for d in loads(0, 0):
        d.start()
    for d in own:
        d.wait()

    def first(t, _):
        slot = t % 2

        @pl.when(t + 1 < n_tile)
        def _():
            for d in loads(t + 1, (t + 1) % 2):
                d.start()

        for d in loads(t, slot):
            d.wait()
        acc[:, tile_cols(t)] = x_t[slot].astype(jnp.float32) + jnp.dot(o_buf[0], w_t[slot], preferred_element_type=jnp.float32)
        return 0

    lax.fori_loop(0, n_tile, first, 0)

    def store(r0, t, slot):
        return pltpu.make_async_copy(y_t.at[slot], out_hbm.at[pl.ds(r0, ch), tile_cols(t)], st_sem.at[slot])

    def finish(c):
        r0 = c * ch

        def body(t, _):
            slot = t % 2

            @pl.when(t >= 2)
            def _():
                store(r0, t - 2, slot).wait()

            cols = tile_cols(t)
            y = acc[r0:r0 + ch, cols] + jnp.dot(o_buf[last, r0:r0 + ch, :], w_buf[last - 1, :, cols], preferred_element_type=jnp.float32)
            y_t[slot] = y.astype(jnp.bfloat16)
            store(r0, t, slot).start()
            return 0

        lax.fori_loop(0, n_tile, body, 0)
        store(r0, n_tile - 2, n_tile % 2).wait()
        store(r0, n_tile - 1, (n_tile - 1) % 2).wait()

    pass_on(0)
    start_own(1)
    arrive(2, 0)
    arrive(2, 1)
    pass_diag(0)
    arrive(1, 2)
    complete(0)
    accum(1, 0, half)
    arrive(1, 3)
    accum(1, half, n_rows)
    pass_on(1)
    start_own(2)
    arrive(3, 0)
    pass_diag(1)
    arrive(3, 1)
    complete(1)
    accum(2, 0, half)
    arrive(2, 2)
    pass_on(2)
    arrive(2, 3)
    accum(2, half, n_rows)
    pass_diag(2)
    complete(2)
    finish(0)
    finish(1)
    arrive(3, 2)
    finish(2)
    arrive(3, 3)
    finish(3)

    for s in range(last):
        for c in range(N_CHUNK):
            if s > 0 or c >= 2:
                o_copy(s, c).wait_send()
        for kind in ("own_x", "own_y", "own_p", "dx", "dy", "px", "py", "pd0", "pd1"):
            w_copy(s, kind).wait_send()
    w_last_half().wait_send()


def solution(mesh):
    n_tp, n_cp, n_dp = mesh.shape["tp"], mesh.shape["cp"], mesh.shape["dp"]
    plane = n_dp * n_cp
    ring = [(i, (i + 1) % n_tp) for i in range(n_tp)]

    def local_block(hidden, tok_pos, norm_gain, w_query, w_key, w_value, w_out):
        rows, width = hidden.shape
        q_cols, k_cols = w_query.shape[1], w_key.shape[1]
        n_kv = k_cols // HEAD
        slice_rows = w_out.shape[0] // plane
        cos_tab, sin_tab = rope_tables(tok_pos)
        smem = pl.BlockSpec(memory_space=pltpu.SMEM)
        anym = pl.BlockSpec(memory_space=pl.ANY)
        vmem = pl.BlockSpec(memory_space=pltpu.VMEM)
        pos_row = tok_pos.reshape(rows // KB, 1, KB)
        n_rb = rows // FRONT_ROWS
        kv_all, pos_far, q_rot, wz, relay = pl.pallas_call(
            functools.partial(front_kernel, n_tp, n_cp, slice_rows),
            out_shape=(jax.ShapeDtypeStruct((n_cp * rows, 2 * k_cols), jnp.bfloat16), jax.ShapeDtypeStruct((n_cp - 1,) + pos_row.shape, jnp.int32),
                       jax.ShapeDtypeStruct((rows, q_cols), jnp.bfloat16), jax.ShapeDtypeStruct((slice_rows // 2, width), jnp.bfloat16),
                       jax.ShapeDtypeStruct((2, slice_rows // 2, width), jnp.bfloat16)),
            in_specs=[anym, anym, vmem, anym, anym, anym, anym, vmem, vmem],
            out_specs=(anym,) * 5,
            scratch_shapes=[
                pltpu.VMEM((2, FRONT_ROWS, width), jnp.bfloat16),
                pltpu.VMEM((rows, width), jnp.bfloat16),
                pltpu.VMEM((width, 2 * k_cols), jnp.bfloat16),
                pltpu.VMEM((width, q_cols), jnp.bfloat16),
                pltpu.VMEM((n_rb, FRONT_ROWS, 2 * k_cols), jnp.bfloat16),
                pltpu.VMEM((2, rows, FRONT_COLS), jnp.bfloat16),
                pltpu.SemaphoreType.DMA((2,)),
                pltpu.SemaphoreType.DMA((3,)),
                pltpu.SemaphoreType.DMA((n_rb,)),
                pltpu.SemaphoreType.DMA((2,)),
                pltpu.SemaphoreType.DMA((n_cp - 1,)),
                pltpu.SemaphoreType.DMA((n_cp - 1,)),
                pltpu.SemaphoreType.DMA((3, n_rb)),
                pltpu.SemaphoreType.DMA((3, n_rb)),
                pltpu.SemaphoreType.DMA((3,)),
                pltpu.SemaphoreType.DMA((3,)),
            ],
            compiler_params=pltpu.CompilerParams(collective_id=1, has_side_effects=True, vmem_limit_bytes=63 << 20),
            cost_estimate=pl.CostEstimate(flops=2 * rows * width * (q_cols + 2 * k_cols), bytes_accessed=24 << 20, transcendentals=0),
            name="front",
        )(hidden, pos_row, norm_gain.reshape(1, width), w_key, w_value, w_query, w_out, cos_tab, sin_tab)
        relay2 = lax.ppermute(relay, "tp", ring)
        pos_rel = jnp.concatenate([pos_row, pos_far.reshape(-1, 1, KB)], axis=0)

        kmin, kmax = jnp.min(pos_rel, axis=(1, 2)), jnp.max(pos_rel, axis=(1, 2))
        n_q = rows // QB
        qpos = tok_pos.reshape(n_q, QB)
        qmin, qmax = jnp.min(qpos, axis=1), jnp.max(qpos, axis=1)
        pos_col = tok_pos.reshape(rows, 1)

        def attend(part, n_parts):
            steps = n_q // n_parts
            first = part * steps
            n_rows = (q_cols // HEAD) * QB
            blocks_max = n_cp * rows // KB
            return pl.pallas_call(
                functools.partial(attn_kernel, first),
                grid=(steps,),
                out_shape=jax.ShapeDtypeStruct((rows // n_parts, q_cols), jnp.bfloat16),
                in_specs=[smem] * 4 + [pl.BlockSpec((QB, q_cols), lambda i: (first + i, 0)), pl.BlockSpec((QB, 1), lambda i: (first + i, 0)),
                                       pl.BlockSpec(pos_rel.shape, lambda i: (0, 0, 0)), anym],
                out_specs=pl.BlockSpec((QB, q_cols), lambda i: (i, 0)),
                scratch_shapes=[
                    pltpu.VMEM((n_cp * rows, 2 * k_cols), jnp.bfloat16),
                    pltpu.VMEM((n_rows, HEAD), jnp.bfloat16),
                    pltpu.VMEM((n_rows // n_kv // PARTS, HEAD), jnp.int32),
                    pltpu.VMEM((n_rows, HEAD), jnp.float32),
                    pltpu.VMEM((n_rows, HEAD), jnp.float32),
                    pltpu.VMEM((n_rows, HEAD), jnp.float32),
                    pltpu.SMEM((blocks_max + WIDE,), jnp.int32),
                    pltpu.SMEM((blocks_max + WIDE + GROUP,), jnp.int32),
                    pltpu.SemaphoreType.DMA,
                ],
                cost_estimate=pl.CostEstimate(flops=4 * rows // n_parts * n_cp * rows * q_cols, bytes_accessed=8 << 20, transcendentals=0),
                name="attend",
            )(kmin, kmax, qmin, qmax, q_rot, pos_col, pos_rel, kv_all)

        o_a = attend(0, 2)
        left_a = lax.ppermute(o_a, "tp", ring)
        o_b = attend(1, 2)
        hidden_out = pl.pallas_call(
            functools.partial(out_kernel, n_tp, n_cp, slice_rows),
            out_shape=jax.ShapeDtypeStruct((rows, width), jnp.bfloat16),
            in_specs=[anym] * 8,
            out_specs=anym,
            scratch_shapes=[
                pltpu.VMEM((n_tp, rows, q_cols), jnp.bfloat16),
                pltpu.VMEM((n_tp - 1, q_cols, width), jnp.bfloat16),
                pltpu.VMEM((rows, width), jnp.float32),
                pltpu.VMEM((2, q_cols, TILE), jnp.bfloat16),
                pltpu.VMEM((2, rows, TILE), jnp.bfloat16),
                pltpu.VMEM((2, rows // N_CHUNK, TILE), jnp.bfloat16),
                pltpu.SemaphoreType.DMA((n_tp - 1, N_CHUNK)),
                pltpu.SemaphoreType.DMA((n_tp - 1, N_CHUNK)),
                pltpu.SemaphoreType.DMA((n_tp - 1, 9)),
                pltpu.SemaphoreType.DMA((n_tp - 1, 9)),
                pltpu.SemaphoreType.DMA((n_tp - 1, 2)),
                pltpu.SemaphoreType.DMA((2, 2)),
                pltpu.SemaphoreType.DMA((2,)),
                pltpu.SemaphoreType.DMA((3,)),
                pltpu.SemaphoreType.DMA,
                pltpu.SemaphoreType.DMA,
            ],
            compiler_params=pltpu.CompilerParams(collective_id=0, has_side_effects=True, vmem_limit_bytes=63 << 20),
            cost_estimate=pl.CostEstimate(flops=2 * n_tp * rows * q_cols * width, bytes_accessed=48 << 20, transcendentals=0),
            name="out_gather",
        )(o_a, o_b, left_a, w_out, wz, relay, relay2, hidden)
        k_cache = kv_all[:rows, :k_cols].reshape(rows, n_kv, HEAD)
        v_cache = kv_all[:rows, k_cols:].reshape(rows, n_kv, HEAD)
        return hidden_out, k_cache, v_cache

    row_spec = P(("dp", "cp"), None)
    cache_spec = P(("dp", "cp"), "tp", None)
    return jax.shard_map(local_block, mesh=mesh, in_specs=(row_spec, P(("dp", "cp")), P(None), P(None, "tp"), P(None, "tp"), P(None, "tp"), P("tp", None)), out_specs=(row_spec, cache_spec, cache_spec), check_vma=False)
```

```python
import functools
import math

import jax
import jax.numpy as jnp
from jax import lax
from jax.experimental import pallas as pl
from jax.experimental.pallas import tpu as pltpu
from jax.sharding import PartitionSpec as P


HEAD = 128
THETA = 1000000
EPS = 1e-5
NEG_BIG = -1e30
KB = 128
GROUP = 4
WIDE = 8
PARTS = 1
AHEAD = 2
QB = 128


def rope_tables(tok_pos):
    inv_freq = 1.0 / (THETA ** (jnp.arange(0, HEAD, 2, dtype=jnp.float32) / HEAD))
    inv_freq = jnp.concatenate([inv_freq, inv_freq])
    sign = jnp.where(jnp.arange(HEAD) < HEAD // 2, -1.0, 1.0).astype(jnp.float32)
    angles = tok_pos.astype(jnp.float32)[:, None] * inv_freq[None, :]
    return jnp.cos(angles), jnp.sin(angles) * sign[None, :]


def rotate(x_f32, cos_tab, sin_tab):
    x = x_f32.astype(jnp.bfloat16).astype(jnp.float32)
    return (x * cos_tab + pltpu.roll(x, HEAD // 2, 1) * sin_tab).astype(jnp.bfloat16)


FRONT_ROWS = 256
FRONT_COLS = 256


def front_kernel(n_tp, n_cp, slice_rows, x_hbm, pos_hbm, gain_ref, wk_hbm, wv_hbm, wq_hbm, wo_hbm, cos_ref, sin_ref, kv_hbm, pos_out, q_hbm, wz_hbm, wy_hbm, wx_hbm,
                 x_t, normed, wkv, wq_v, kv_t, q_t, x_sem, w_sem, kv_sem, q_sem, p_send, p_recv, s_send, s_recv, z_send, z_recv):
    mesh_id = pl.DeviceIdType.MESH
    tp, dp, cp = lax.axis_index("tp"), lax.axis_index("dp"), lax.axis_index("cp")
    to_right, to_left = {"tp": (tp + 1) % n_tp}, {"tp": (tp + n_tp - 1) % n_tp}
    core, chip = cp % 2, cp // 2
    cp_p, cp_y = cp + 1 - 2 * core, cp + 2 - 4 * chip
    to_p, to_y, to_d = {"cp": cp_p}, {"cp": cp_y}, {"cp": cp_y + 1 - 2 * core}
    rows = normed.shape[0]
    k_cols = wk_hbm.shape[1]
    n_rb = rows // FRONT_ROWS
    n_cb = wq_hbm.shape[1] // FRONT_COLS

    def x_load(r):
        return pltpu.make_async_copy(x_hbm.at[pl.ds(r * FRONT_ROWS, FRONT_ROWS), :], x_t.at[r % 2], x_sem.at[r % 2])

    weights = [pltpu.make_async_copy(wk_hbm, wkv.at[:, pl.ds(0, k_cols)], w_sem.at[0]),
               pltpu.make_async_copy(wv_hbm, wkv.at[:, pl.ds(k_cols, k_cols)], w_sem.at[1]),
               pltpu.make_async_copy(wq_hbm, wq_v, w_sem.at[2])]
    x_load(0).start()
    weights[0].start()
    weights[1].start()
    x_load(1).start()
    weights[2].start()

    barrier = pltpu.get_barrier_semaphore()
    for peer in (to_p, to_y, to_d, to_right, to_left):
        pl.semaphore_signal(barrier, inc=1, device_id=peer, device_id_type=mesh_id)
    pl.semaphore_wait(barrier, 5)

    hs = slice_rows // 2
    own = (dp * n_cp + cp) * slice_rows

    def z_copy(i):
        src, dst = ((wo_hbm.at[pl.ds(pl.multiple_of(own, hs), hs), :], wz_hbm),
                    (wo_hbm.at[pl.ds(pl.multiple_of(own + hs, hs), hs), :], wy_hbm),
                    (wz_hbm, wx_hbm))[i]
        return pltpu.make_async_remote_copy(src_ref=src, dst_ref=dst, send_sem=z_send.at[i], recv_sem=z_recv.at[i],
                                            device_id=to_right, device_id_type=mesh_id)

    z_copy(0).start()
    z_copy(1).start()

    pos_copies = [pltpu.make_async_remote_copy(src_ref=pos_hbm, dst_ref=pos_out.at[i], send_sem=p_send.at[i], recv_sem=p_recv.at[i],
                                               device_id=peer, device_id_type=mesh_id) for i, peer in enumerate((to_p, to_y, to_d))]
    for c in pos_copies:
        c.start()

    def send(kind, r):
        src = (0, 0, 2)[kind] * rows + r * FRONT_ROWS
        dst = (1, 2, 3)[kind] * rows + r * FRONT_ROWS
        return pltpu.make_async_remote_copy(src_ref=kv_hbm.at[pl.ds(src, FRONT_ROWS), :], dst_ref=kv_hbm.at[pl.ds(dst, FRONT_ROWS), :],
                                            send_sem=s_send.at[kind, r], recv_sem=s_recv.at[kind, r],
                                            device_id=(to_p, to_y, to_p)[kind], device_id_type=mesh_id)

    def kv_store(r):
        return pltpu.make_async_copy(kv_t.at[r], kv_hbm.at[pl.ds(r * FRONT_ROWS, FRONT_ROWS), :], kv_sem.at[r])

    def spread(r):
        kv_store(r).wait()
        send(1, r).start()
        send(0, r).start()

    for r in range(n_rb):
        at = slice(r * FRONT_ROWS, (r + 1) * FRONT_ROWS)
        x_load(r).wait()
        x = x_t[r % 2].astype(jnp.float32)
        var = jnp.mean(x * x, axis=-1, keepdims=True)
        normed[at, :] = (x * lax.rsqrt(var + EPS) * gain_ref[...]).astype(jnp.bfloat16)
        if r + 2 < n_rb:
            x_load(r + 2).start()
        if r == 0:
            weights[0].wait()
            weights[1].wait()
        kv = jnp.dot(normed[at, :], wkv[...], preferred_element_type=jnp.float32)
        for h in range(k_cols // HEAD):
            kv_t[r, :, h * HEAD:(h + 1) * HEAD] = rotate(kv[:, h * HEAD:(h + 1) * HEAD], cos_ref[at, :], sin_ref[at, :])
        kv_t[r, :, k_cols:] = kv[:, k_cols:].astype(jnp.bfloat16)
        kv_store(r).start()
        if r > 0:
            spread(r - 1)

    weights[2].wait()
    z_copy(0).wait_recv()
    z_copy(2).start()

    def q_store(c):
        return pltpu.make_async_copy(q_t.at[c % 2], q_hbm.at[:, pl.ds(c * FRONT_COLS, FRONT_COLS)], q_sem.at[c % 2])

    for c in range(n_cb):
        if c == 0:
            spread(n_rb - 1)
        if c >= 2:
            q_store(c - 2).wait()
        q = jnp.dot(normed[...], wq_v[:, c * FRONT_COLS:(c + 1) * FRONT_COLS], preferred_element_type=jnp.float32)
        for h in range(FRONT_COLS // HEAD):
            q_t[c % 2, :, h * HEAD:(h + 1) * HEAD] = rotate(q[:, h * HEAD:(h + 1) * HEAD], cos_ref[...], sin_ref[...])
        q_store(c).start()
        if c < n_rb:
            send(1, c).wait_recv()
            send(2, c).start()
    for r in range(n_cb, n_rb):
        send(1, r).wait_recv()
        send(2, r).start()

    q_store(n_cb - 2).wait()
    q_store(n_cb - 1).wait()
    for r in range(n_rb):
        send(0, r).wait_recv()
        send(2, r).wait_recv()
    for c in pos_copies:
        c.wait()
    z_copy(1).wait_recv()
    z_copy(2).wait_recv()
    for i in range(3):
        z_copy(i).wait_send()
    for kind in range(3):
        for r in range(n_rb):
            send(kind, r).wait_send()


def attn_kernel(first, kmin_ref, kmax_ref, qmin_ref, qmax_ref, q_ref, posq_ref, posk_ref, kv_hbm, o_ref,
                kv_s, q_s, pq_s, m_s, l_s, acc_s, full_l, part_l, sem):
    step = pl.program_id(0)
    n_blocks = kmin_ref.shape[0]
    n_kv = kv_hbm.shape[1] // (2 * HEAD)
    n_heads = q_ref.shape[1] // HEAD
    per_kv = n_heads // n_kv

    @pl.when(step == 0)
    def _():
        load = pltpu.make_async_copy(kv_hbm, kv_s, sem)
        load.start()
        load.wait()

    q_lo = qmin_ref[first + step]
    q_hi = qmax_ref[first + step]

    def classify(j, counts):
        n_full, n_part = counts
        lo, hi = kmin_ref[j], kmax_ref[j]
        is_full = hi <= q_lo
        is_part = jnp.logical_and(lo <= q_hi, jnp.logical_not(is_full))

        @pl.when(is_full)
        def _():
            full_l[n_full] = j

        @pl.when(is_part)
        def _():
            part_l[n_part] = j

        return n_full + is_full.astype(jnp.int32), n_part + is_part.astype(jnp.int32)

    n_full, n_part = lax.fori_loop(0, n_blocks, classify, (0, 0))
    n_groups = n_full // WIDE

    def move(i, n_part):
        part_l[n_part] = full_l[n_groups * WIDE + i]
        return n_part + 1

    n_part = lax.fori_loop(0, n_full - n_groups * WIDE, move, n_part)
    n_mgroups = (n_part + GROUP - 1) // GROUP

    def pad(i, _):
        part_l[n_part + i] = 0
        return 0

    lax.fori_loop(0, n_mgroups * GROUP - n_part, pad, 0)

    for h in range(n_heads):
        q_s[h * QB:(h + 1) * QB, :] = q_ref[:, h * HEAD:(h + 1) * HEAD]
    part_rows = per_kv * QB // PARTS
    for h in range(part_rows // QB):
        pq_s[h * QB:(h + 1) * QB, :] = jnp.broadcast_to(posq_ref[...], (QB, HEAD))
    m_s[...] = jnp.full_like(m_s, NEG_BIG)
    l_s[...] = jnp.zeros_like(l_s)
    acc_s[...] = jnp.zeros_like(acc_s)

    scale = HEAD ** -0.5 * math.log2(math.e)

    def absorb(blocks, pos_rows):
        def gather(c0):
            return jnp.concatenate([kv_s[pl.ds(pl.multiple_of(b * KB, KB), KB), c0:c0 + HEAD] for b in blocks], axis=0)

        ks = [gather(g * HEAD) for g in range(n_kv)]
        vs = [gather((n_kv + g) * HEAD) for g in range(n_kv)]
        n = len(blocks)
        chains = [(g, slice((g * PARTS + i) * part_rows, (g * PARTS + i + 1) * part_rows)) for i in range(PARTS) for g in range(n_kv)]

        def scores(g, sl):
            return lax.dot_general(q_s[sl, :], ks[g], (((1,), (1,)), ((), ())), preferred_element_type=jnp.float32)

        ahead = [scores(*c) for c in chains[:AHEAD]]
        for i, (g, sl) in enumerate(chains):
            s = ahead[i]
            if i + AHEAD < len(chains):
                ahead.append(scores(*chains[i + AHEAD]))
            cols = [s[:, c * KB:(c + 1) * KB] * scale for c in range(n)]
            if pos_rows is not None:
                cols = [jnp.where(pr <= pq_s[...], c, NEG_BIG) for pr, c in zip(pos_rows, cols)]
            top = cols[0]
            for c in cols[1:]:
                top = jnp.maximum(top, c)
            m_old = m_s[sl, :]
            m_new = jnp.maximum(m_old, jnp.max(top, axis=-1, keepdims=True))
            alpha = jnp.exp2(m_old - m_new)
            p = [jnp.exp2(c - m_new) for c in cols]
            total = p[0]
            for c in p[1:]:
                total = total + c
            l_s[sl, :] = l_s[sl, :] * alpha + total
            pv = jnp.dot(jnp.concatenate([c.astype(jnp.bfloat16) for c in p], axis=1), vs[g], preferred_element_type=jnp.float32)
            acc_s[sl, :] = acc_s[sl, :] * alpha + pv
            m_s[sl, :] = m_new

    def full_step(i, _):
        absorb([full_l[i * WIDE + c] for c in range(WIDE)], None)
        return 0

    lax.fori_loop(0, n_groups, full_step, 0)

    def part_step(i, _):
        blocks = [part_l[i * GROUP + c] for c in range(GROUP)]
        absorb(blocks, [posk_ref[b] + jnp.where(i * GROUP + c < n_part, 0, 1 << 30) for c, b in enumerate(blocks)])
        return 0

    lax.fori_loop(0, n_mgroups, part_step, 0)

    for h in range(n_heads):
        sl = slice(h * QB, (h + 1) * QB)
        o_ref[:, h * HEAD:(h + 1) * HEAD] = (acc_s[sl, :] / jnp.sum(l_s[sl, :], axis=-1, keepdims=True)).astype(jnp.bfloat16)


TILE = 512
TILE_IN = 256
N_CHUNK = 8
A_CHUNKS = 3


def out_kernel(n_tp, n_cp, sl, oa_hbm, ob_hbm, la_hbm, w_hbm, wh0, wh1, wh2, wh3, wh4, wh5, x_hbm, out_ref, o_buf, w_buf, acc, w_t, x_t,
               o_send, o_recv, w_send, w_recv, w_local, ld_sem, own_sem):
    mesh_id = pl.DeviceIdType.MESH
    tp, dp, cp = lax.axis_index("tp"), lax.axis_index("dp"), lax.axis_index("cp")
    core, chip = cp % 2, cp // 2
    cp_y = cp + 2 - 4 * chip
    to_right, to_left = {"tp": (tp + 1) % n_tp}, {"tp": (tp + n_tp - 1) % n_tp}
    to_x, to_y, to_p = {"dp": 1 - dp}, {"cp": cp_y}, {"cp": cp + 1 - 2 * core}
    p_me, p_x, p_y, p_d = dp * n_cp + cp, (1 - dp) * n_cp + cp, dp * n_cp + cp_y, (1 - dp) * n_cp + cp_y
    n_rows, width = acc.shape
    ch = n_rows // N_CHUNK
    n_a = A_CHUNKS * ch
    n_tile = width // TILE
    last = n_tp - 1

    barrier = pltpu.get_barrier_semaphore()
    for peer in (to_right, to_left, to_x, to_y, to_p):
        pl.semaphore_signal(barrier, inc=1, device_id=peer, device_id_type=mesh_id)
    pl.semaphore_wait(barrier, 5)

    def o_copy(s, c):
        at = pl.ds(c * ch, ch)
        if s == 0:
            src = ob_hbm.at[pl.ds(c * ch - n_a, ch), :]
        elif s == 1 and c < A_CHUNKS:
            src = la_hbm.at[at, :]
        else:
            src = o_buf.at[s, at, :]
        return pltpu.make_async_remote_copy(src_ref=src, dst_ref=o_buf.at[s + 1, at, :], send_sem=o_send.at[s, c],
                                            recv_sem=o_recv.at[s, c], device_id=to_right, device_id_type=mesh_id)

    def rows(p, first=0, n=None):
        return pl.ds(pl.multiple_of(p * sl + first, sl // 2), sl if n is None else n)

    def w_copy(k, kind):
        hs = sl // 2
        idx, peer, where = {
            "own_x": (0, to_x, rows(p_me)), "own_y": (1, to_y, rows(p_me)), "own_p": (2, to_p, rows(p_me)),
            "dx": (3, to_x, rows(p_y, hs, hs)), "dy": (4, to_y, rows(p_x, 0, hs)),
            "px": (5, to_p, rows(p_x)), "py": (6, to_p, rows(p_y)),
            "pd0": (7, to_p, rows(p_d, 0, hs)), "pd1": (8, to_p, rows(p_d, hs, hs)),
        }[kind]
        at = w_buf.at[k, where, :]
        return pltpu.make_async_remote_copy(src_ref=at, dst_ref=at, send_sem=w_send.at[k, idx],
                                            recv_sem=w_recv.at[k, idx], device_id=peer, device_id_type=mesh_id)

    hs = sl // 2

    def w_own_half(k, h):
        src = ((wh0, wh1), (wh2, wh3), (wh4, wh5))[k][h]
        return pltpu.make_async_copy(src, w_buf.at[k, rows(p_me, h * hs, hs), :], w_local.at[k, h])

    def start_own(k):
        for h in (0, 1):
            w_own_half(k, h).wait()
        for kind in ("own_x", "own_y", "own_p"):
            w_copy(k, kind).start()

    def pass_on(k):
        w_copy(k, "own_x").wait_recv()
        w_copy(k, "own_y").wait_recv()
        for kind in ("dx", "dy", "px", "py"):
            w_copy(k, kind).start()

    def pass_diag(k):
        w_copy(k, "dy").wait_recv()
        w_copy(k, "pd0").start()
        w_copy(k, "dx").wait_recv()
        w_copy(k, "pd1").start()

    def complete(k):
        for kind in ("own_p", "px", "py", "pd0", "pd1"):
            w_copy(k, kind).wait_recv()

    def arrive(s, c):
        o_copy(s - 1, c).wait_recv()
        if s < last:
            o_copy(s, c).start()

    def tile_cols(t, size=TILE):
        return pl.ds(pl.multiple_of(t * size, size), size)

    def accum(s, r0, r1):
        def body(t, _):
            cols = tile_cols(t)
            acc[r0:r1, cols] += jnp.dot(o_buf[s, r0:r1, :], w_buf[s - 1, :, cols], preferred_element_type=jnp.float32)
            return 0

        lax.fori_loop(0, n_tile, body, 0)

    for k in range(last):
        for h in (0, 1):
            w_own_half(k, h).start()
    for c in range(N_CHUNK):
        o_copy(1 if c < A_CHUNKS else 0, c).start()
    start_own(0)
    own = [pltpu.make_async_copy(oa_hbm, o_buf.at[0, pl.ds(0, n_a), :], own_sem.at[0]),
           pltpu.make_async_copy(ob_hbm, o_buf.at[0, pl.ds(n_a, n_rows - n_a), :], own_sem.at[1]),
           pltpu.make_async_copy(la_hbm, o_buf.at[1, pl.ds(0, n_a), :], own_sem.at[2])]
    for d in own:
        d.start()

    def loads(t, slot):
        cols = tile_cols(t, TILE_IN)
        return (pltpu.make_async_copy(w_hbm.at[:, cols], w_t.at[slot], ld_sem.at[slot, 0]),
                pltpu.make_async_copy(x_hbm.at[:, cols], x_t.at[slot], ld_sem.at[slot, 1]))

    for d in loads(0, 0):
        d.start()
    for d in own:
        d.wait()

    def first(t, _):
        slot = t % 2

        @pl.when(t + 1 < width // TILE_IN)
        def _():
            for d in loads(t + 1, (t + 1) % 2):
                d.start()

        for d in loads(t, slot):
            d.wait()
        acc[:, tile_cols(t, TILE_IN)] = x_t[slot].astype(jnp.float32) + jnp.dot(o_buf[0], w_t[slot], preferred_element_type=jnp.float32)
        return 0

    lax.fori_loop(0, width // TILE_IN, first, 0)

    def finish(r0, r1):
        def body(t, _):
            cols = tile_cols(t)
            y = acc[r0:r1, cols] + jnp.dot(o_buf[last, r0:r1, :], w_buf[last - 1, :, cols], preferred_element_type=jnp.float32)
            out_ref[r0:r1, cols] = y.astype(jnp.bfloat16)
            return 0

        lax.fori_loop(0, n_tile, body, 0)

    pass_on(0)
    start_own(1)
    for c in range(A_CHUNKS):
        arrive(2, c)
    arrive(1, 3)
    arrive(1, 4)
    pass_diag(0)
    arrive(1, 5)
    complete(0)
    accum(1, 0, 6 * ch)
    arrive(1, 6)
    arrive(1, 7)
    accum(1, 6 * ch, n_rows)
    pass_on(1)
    start_own(2)
    pass_diag(1)
    arrive(2, 3)
    complete(1)
    accum(2, 0, 4 * ch)
    arrive(2, 4)
    arrive(2, 5)
    accum(2, 4 * ch, 6 * ch)
    arrive(2, 6)
    pass_on(2)
    arrive(2, 7)
    accum(2, 6 * ch, n_rows)
    pass_diag(2)
    complete(2)
    for c in range(5):
        arrive(3, c)
    finish(0, 5 * ch)
    arrive(3, 5)
    arrive(3, 6)
    finish(5 * ch, 7 * ch)
    arrive(3, 7)
    finish(7 * ch, n_rows)

    for s in range(last):
        for c in range(N_CHUNK):
            if s > 0 or c >= A_CHUNKS:
                o_copy(s, c).wait_send()
        for kind in ("own_x", "own_y", "own_p", "dx", "dy", "px", "py", "pd0", "pd1"):
            w_copy(s, kind).wait_send()


def solution(mesh):
    n_tp, n_cp, n_dp = mesh.shape["tp"], mesh.shape["cp"], mesh.shape["dp"]
    plane = n_dp * n_cp
    ring = [(i, (i + 1) % n_tp) for i in range(n_tp)]

    def local_block(hidden, tok_pos, norm_gain, w_query, w_key, w_value, w_out):
        rows, width = hidden.shape
        q_cols, k_cols = w_query.shape[1], w_key.shape[1]
        n_kv = k_cols // HEAD
        slice_rows = w_out.shape[0] // plane
        cos_tab, sin_tab = rope_tables(tok_pos)
        smem = pl.BlockSpec(memory_space=pltpu.SMEM)
        anym = pl.BlockSpec(memory_space=pl.ANY)
        vmem = pl.BlockSpec(memory_space=pltpu.VMEM)
        pos_row = tok_pos.reshape(rows // KB, 1, KB)
        n_rb = rows // FRONT_ROWS
        kv_all, pos_far, q_rot, *near = pl.pallas_call(
            functools.partial(front_kernel, n_tp, n_cp, slice_rows),
            out_shape=(jax.ShapeDtypeStruct((n_cp * rows, 2 * k_cols), jnp.bfloat16), jax.ShapeDtypeStruct((n_cp - 1,) + pos_row.shape, jnp.int32),
                       jax.ShapeDtypeStruct((rows, q_cols), jnp.bfloat16), *[jax.ShapeDtypeStruct((slice_rows // 2, width), jnp.bfloat16)] * 3),
            in_specs=[anym, anym, vmem, anym, anym, anym, anym, vmem, vmem],
            out_specs=(anym,) * 6,
            scratch_shapes=[
                pltpu.VMEM((2, FRONT_ROWS, width), jnp.bfloat16),
                pltpu.VMEM((rows, width), jnp.bfloat16),
                pltpu.VMEM((width, 2 * k_cols), jnp.bfloat16),
                pltpu.VMEM((width, q_cols), jnp.bfloat16),
                pltpu.VMEM((n_rb, FRONT_ROWS, 2 * k_cols), jnp.bfloat16),
                pltpu.VMEM((2, rows, FRONT_COLS), jnp.bfloat16),
                pltpu.SemaphoreType.DMA((2,)),
                pltpu.SemaphoreType.DMA((3,)),
                pltpu.SemaphoreType.DMA((n_rb,)),
                pltpu.SemaphoreType.DMA((2,)),
                pltpu.SemaphoreType.DMA((n_cp - 1,)),
                pltpu.SemaphoreType.DMA((n_cp - 1,)),
                pltpu.SemaphoreType.DMA((3, n_rb)),
                pltpu.SemaphoreType.DMA((3, n_rb)),
                pltpu.SemaphoreType.DMA((3,)),
                pltpu.SemaphoreType.DMA((3,)),
            ],
            compiler_params=pltpu.CompilerParams(collective_id=1, has_side_effects=True, vmem_limit_bytes=63 << 20),
            cost_estimate=pl.CostEstimate(flops=2 * rows * width * (q_cols + 2 * k_cols), bytes_accessed=24 << 20, transcendentals=0),
            name="front",
        )(hidden, pos_row, norm_gain.reshape(1, width), w_key, w_value, w_query, w_out, cos_tab, sin_tab)
        far_y = lax.ppermute(near[1], "tp", ring)
        far_x = lax.ppermute(near[2], "tp", ring)
        far_last = lax.ppermute(far_y, "tp", ring)
        pos_rel = jnp.concatenate([pos_row, pos_far.reshape(-1, 1, KB)], axis=0)

        kmin, kmax = jnp.min(pos_rel, axis=(1, 2)), jnp.max(pos_rel, axis=(1, 2))
        n_q = rows // QB
        qpos = tok_pos.reshape(n_q, QB)
        qmin, qmax = jnp.min(qpos, axis=1), jnp.max(qpos, axis=1)
        pos_col = tok_pos.reshape(rows, 1)

        def attend(first, steps):
            n_rows = (q_cols // HEAD) * QB
            blocks_max = n_cp * rows // KB
            return pl.pallas_call(
                functools.partial(attn_kernel, first),
                grid=(steps,),
                out_shape=jax.ShapeDtypeStruct((steps * QB, q_cols), jnp.bfloat16),
                in_specs=[smem] * 4 + [pl.BlockSpec((QB, q_cols), lambda i: (first + i, 0)), pl.BlockSpec((QB, 1), lambda i: (first + i, 0)),
                                       pl.BlockSpec(pos_rel.shape, lambda i: (0, 0, 0)), anym],
                out_specs=pl.BlockSpec((QB, q_cols), lambda i: (i, 0)),
                scratch_shapes=[
                    pltpu.VMEM((n_cp * rows, 2 * k_cols), jnp.bfloat16),
                    pltpu.VMEM((n_rows, HEAD), jnp.bfloat16),
                    pltpu.VMEM((n_rows // n_kv // PARTS, HEAD), jnp.int32),
                    pltpu.VMEM((n_rows, HEAD), jnp.float32),
                    pltpu.VMEM((n_rows, HEAD), jnp.float32),
                    pltpu.VMEM((n_rows, HEAD), jnp.float32),
                    pltpu.SMEM((blocks_max + WIDE,), jnp.int32),
                    pltpu.SMEM((blocks_max + WIDE + GROUP,), jnp.int32),
                    pltpu.SemaphoreType.DMA,
                ],
                cost_estimate=pl.CostEstimate(flops=4 * steps * QB * n_cp * rows * q_cols, bytes_accessed=8 << 20, transcendentals=0),
                name="attend",
            )(kmin, kmax, qmin, qmax, q_rot, pos_col, pos_rel, kv_all)

        o_a = attend(0, A_CHUNKS)
        left_a = lax.ppermute(o_a, "tp", ring)
        o_b = attend(A_CHUNKS, n_q - A_CHUNKS)
        hidden_out = pl.pallas_call(
            functools.partial(out_kernel, n_tp, n_cp, slice_rows),
            out_shape=pltpu.VMEM((rows, width), jnp.bfloat16),
            in_specs=[anym] * 11,
            out_specs=vmem,
            scratch_shapes=[
                pltpu.VMEM((n_tp, rows, q_cols), jnp.bfloat16),
                pltpu.VMEM((n_tp - 1, q_cols, width), jnp.bfloat16),
                pltpu.VMEM((rows, width), jnp.float32),
                pltpu.VMEM((2, q_cols, TILE_IN), jnp.bfloat16),
                pltpu.VMEM((2, rows, TILE_IN), jnp.bfloat16),
                pltpu.SemaphoreType.DMA((n_tp - 1, N_CHUNK)),
                pltpu.SemaphoreType.DMA((n_tp - 1, N_CHUNK)),
                pltpu.SemaphoreType.DMA((n_tp - 1, 9)),
                pltpu.SemaphoreType.DMA((n_tp - 1, 9)),
                pltpu.SemaphoreType.DMA((n_tp - 1, 2)),
                pltpu.SemaphoreType.DMA((2, 2)),
                pltpu.SemaphoreType.DMA((3,)),
            ],
            compiler_params=pltpu.CompilerParams(collective_id=0, has_side_effects=True, vmem_limit_bytes=53 << 20),
            cost_estimate=pl.CostEstimate(flops=2 * n_tp * rows * q_cols * width, bytes_accessed=48 << 20, transcendentals=0),
            name="out_gather",
        )(o_a, o_b, left_a, w_out, *near, far_y, far_x, far_last, hidden)
        k_cache = kv_all[:rows, :k_cols].reshape(rows, n_kv, HEAD)
        v_cache = kv_all[:rows, k_cols:].reshape(rows, n_kv, HEAD)
        return hidden_out, k_cache, v_cache

    row_spec = P(("dp", "cp"), None)
    cache_spec = P(("dp", "cp"), "tp", None)
    return jax.shard_map(local_block, mesh=mesh, in_specs=(row_spec, P(("dp", "cp")), P(None), P(None, "tp"), P(None, "tp"), P(None, "tp"), P("tp", None)), out_specs=(row_spec, cache_spec, cache_spec), check_vma=False)
```

```python
import functools
import math

import jax
import jax.numpy as jnp
import numpy as np
from jax import lax
from jax.experimental import pallas as pl
from jax.experimental.pallas import tpu as pltpu
from jax.sharding import PartitionSpec as P


HEAD = 128
THETA = 1000000
EPS = 1e-5
NEG_BIG = -1e30
KB = 128
GROUP = 4
WIDE = 8
PARTS = 1
AHEAD = 2
QB = 128


def rope_freqs():
    freq = (1.0 / (float(THETA) ** (np.arange(0, HEAD, 2) / HEAD))).astype(np.float32)
    return jnp.asarray(np.concatenate([freq, freq])[None, :])


def rotate(x_f32, cos_tab, sin_tab):
    x = x_f32.astype(jnp.bfloat16).astype(jnp.float32)
    return (x * cos_tab + pltpu.roll(x, HEAD // 2, 1) * sin_tab).astype(jnp.bfloat16)


FRONT_ROWS = 256
FRONT_COLS = 256


def front_kernel(n_tp, n_cp, slice_rows, x_hbm, pos_ref, gain_ref, wk_hbm, wv_hbm, wq_hbm, wo_hbm, freq_ref, kv_hbm, pos_out, q_hbm, wz_hbm, wy_hbm, wx_hbm,
                 x_t, normed, wkv, wq_v, kv_t, q_t, cos_ref, sin_ref, x_sem, w_sem, kv_sem, q_sem, p_send, p_recv, s_send, s_recv, z_send, z_recv, own_pos_sem):
    mesh_id = pl.DeviceIdType.MESH
    tp, dp, cp = lax.axis_index("tp"), lax.axis_index("dp"), lax.axis_index("cp")
    to_right, to_left = {"tp": (tp + 1) % n_tp}, {"tp": (tp + n_tp - 1) % n_tp}
    core, chip = cp % 2, cp // 2
    cp_p, cp_y = cp + 1 - 2 * core, cp + 2 - 4 * chip
    to_p, to_y, to_d = {"cp": cp_p}, {"cp": cp_y}, {"cp": cp_y + 1 - 2 * core}
    rows = normed.shape[0]
    k_cols = wk_hbm.shape[1]
    n_rb = rows // FRONT_ROWS
    n_cb = wq_hbm.shape[1] // FRONT_COLS

    def x_load(r):
        return pltpu.make_async_copy(x_hbm.at[pl.ds(r * FRONT_ROWS, FRONT_ROWS), :], x_t.at[r % 2], x_sem.at[r % 2])

    weights = [pltpu.make_async_copy(wk_hbm, wkv.at[:, pl.ds(0, k_cols)], w_sem.at[0]),
               pltpu.make_async_copy(wv_hbm, wkv.at[:, pl.ds(k_cols, k_cols)], w_sem.at[1]),
               pltpu.make_async_copy(wq_hbm, wq_v, w_sem.at[2])]
    x_load(0).start()
    weights[0].start()
    weights[1].start()
    x_load(1).start()
    weights[2].start()

    barrier = pltpu.get_barrier_semaphore()
    for peer in (to_p, to_y, to_d, to_right, to_left):
        pl.semaphore_signal(barrier, inc=1, device_id=peer, device_id_type=mesh_id)
    pl.semaphore_wait(barrier, 5)

    hs = slice_rows // 2
    own = (dp * n_cp + cp) * slice_rows

    def z_copy(i):
        src, dst = ((wo_hbm.at[pl.ds(pl.multiple_of(own, hs), hs), :], wz_hbm),
                    (wo_hbm.at[pl.ds(pl.multiple_of(own + hs, hs), hs), :], wy_hbm),
                    (wz_hbm, wx_hbm))[i]
        return pltpu.make_async_remote_copy(src_ref=src, dst_ref=dst, send_sem=z_send.at[i], recv_sem=z_recv.at[i],
                                            device_id=to_right, device_id_type=mesh_id)

    z_copy(0).start()
    z_copy(1).start()

    pos_copies = [pltpu.make_async_remote_copy(src_ref=pos_ref, dst_ref=pos_out.at[i + 1], send_sem=p_send.at[i], recv_sem=p_recv.at[i],
                                               device_id=peer, device_id_type=mesh_id) for i, peer in enumerate((to_p, to_y, to_d))]
    pos_copies.append(pltpu.make_async_copy(pos_ref, pos_out.at[0], own_pos_sem))
    for c in pos_copies:
        c.start()

    def send(kind, r):
        src = (0, 0, 2)[kind] * rows + r * FRONT_ROWS
        dst = (1, 2, 3)[kind] * rows + r * FRONT_ROWS
        return pltpu.make_async_remote_copy(src_ref=kv_hbm.at[pl.ds(src, FRONT_ROWS), :], dst_ref=kv_hbm.at[pl.ds(dst, FRONT_ROWS), :],
                                            send_sem=s_send.at[kind, r], recv_sem=s_recv.at[kind, r],
                                            device_id=(to_p, to_y, to_p)[kind], device_id_type=mesh_id)

    def kv_store(r):
        return pltpu.make_async_copy(kv_t.at[r], kv_hbm.at[pl.ds(r * FRONT_ROWS, FRONT_ROWS), :], kv_sem.at[r])

    def spread(r):
        kv_store(r).wait()
        send(1, r).start()
        send(0, r).start()

    sign = jnp.where(lax.broadcasted_iota(jnp.int32, (KB, HEAD), 1) < HEAD // 2, -1.0, 1.0).astype(jnp.float32)

    def rope_rows(r):
        for j in range(r * FRONT_ROWS // KB, (r + 1) * FRONT_ROWS // KB):
            pos = jnp.transpose(jnp.broadcast_to(pos_ref[j].astype(jnp.float32), (HEAD, KB)))
            angle = pos * freq_ref[...]
            cos_ref[j * KB:(j + 1) * KB, :] = jnp.cos(angle)
            sin_ref[j * KB:(j + 1) * KB, :] = jnp.sin(angle) * sign

    for r in range(n_rb):
        at = slice(r * FRONT_ROWS, (r + 1) * FRONT_ROWS)
        rope_rows(r)
        x_load(r).wait()
        x = x_t[r % 2].astype(jnp.float32)
        var = jnp.mean(x * x, axis=-1, keepdims=True)
        normed[at, :] = (x * lax.rsqrt(var + EPS) * gain_ref[...]).astype(jnp.bfloat16)
        if r + 2 < n_rb:
            x_load(r + 2).start()
        if r == 0:
            weights[0].wait()
            weights[1].wait()
        kv = jnp.dot(normed[at, :], wkv[...], preferred_element_type=jnp.float32)
        for h in range(k_cols // HEAD):
            kv_t[r, :, h * HEAD:(h + 1) * HEAD] = rotate(kv[:, h * HEAD:(h + 1) * HEAD], cos_ref[at, :], sin_ref[at, :])
        kv_t[r, :, k_cols:] = kv[:, k_cols:].astype(jnp.bfloat16)
        kv_store(r).start()
        if r > 0:
            spread(r - 1)

    weights[2].wait()
    z_copy(0).wait_recv()
    z_copy(2).start()

    def q_store(c):
        return pltpu.make_async_copy(q_t.at[c % 2], q_hbm.at[:, pl.ds(c * FRONT_COLS, FRONT_COLS)], q_sem.at[c % 2])

    for c in range(n_cb):
        if c == 0:
            spread(n_rb - 1)
        if c >= 2:
            q_store(c - 2).wait()
        q = jnp.dot(normed[...], wq_v[:, c * FRONT_COLS:(c + 1) * FRONT_COLS], preferred_element_type=jnp.float32)
        for h in range(FRONT_COLS // HEAD):
            q_t[c % 2, :, h * HEAD:(h + 1) * HEAD] = rotate(q[:, h * HEAD:(h + 1) * HEAD], cos_ref[...], sin_ref[...])
        q_store(c).start()
        if c < n_rb:
            send(1, c).wait_recv()
            send(2, c).start()
    for r in range(n_cb, n_rb):
        send(1, r).wait_recv()
        send(2, r).start()

    q_store(n_cb - 2).wait()
    q_store(n_cb - 1).wait()
    for r in range(n_rb):
        send(0, r).wait_recv()
        send(2, r).wait_recv()
    for c in pos_copies:
        c.wait()
    z_copy(1).wait_recv()
    z_copy(2).wait_recv()
    for i in range(3):
        z_copy(i).wait_send()
    for kind in range(3):
        for r in range(n_rb):
            send(kind, r).wait_send()


def attn_kernel(first, kmin_ref, kmax_ref, q_ref, posk_ref, kv_hbm, o_ref,
                kv_s, q_s, pq_s, m_s, l_s, acc_s, full_l, part_l, sem):
    step = pl.program_id(0)
    n_blocks = kmin_ref.shape[0]
    n_kv = kv_hbm.shape[1] // (2 * HEAD)
    n_heads = q_ref.shape[1] // HEAD
    per_kv = n_heads // n_kv

    @pl.when(step == 0)
    def _():
        load = pltpu.make_async_copy(kv_hbm, kv_s, sem)
        load.start()
        load.wait()

    q_lo = kmin_ref[first + step]
    q_hi = kmax_ref[first + step]

    def classify(j, counts):
        n_full, n_part = counts
        lo, hi = kmin_ref[j], kmax_ref[j]
        is_full = hi <= q_lo
        is_part = jnp.logical_and(lo <= q_hi, jnp.logical_not(is_full))

        @pl.when(is_full)
        def _():
            full_l[n_full] = j

        @pl.when(is_part)
        def _():
            part_l[n_part] = j

        return n_full + is_full.astype(jnp.int32), n_part + is_part.astype(jnp.int32)

    n_full, n_part = lax.fori_loop(0, n_blocks, classify, (0, 0))
    n_groups = n_full // WIDE

    def move(i, n_part):
        part_l[n_part] = full_l[n_groups * WIDE + i]
        return n_part + 1

    n_part = lax.fori_loop(0, n_full - n_groups * WIDE, move, n_part)
    n_mgroups = (n_part + GROUP - 1) // GROUP

    def pad(i, _):
        part_l[n_part + i] = 0
        return 0

    lax.fori_loop(0, n_mgroups * GROUP - n_part, pad, 0)

    for h in range(n_heads):
        q_s[h * QB:(h + 1) * QB, :] = q_ref[:, h * HEAD:(h + 1) * HEAD]
    part_rows = per_kv * QB // PARTS
    pos_q = jnp.transpose(jnp.broadcast_to(posk_ref[first + step], (HEAD, QB)))
    for h in range(part_rows // QB):
        pq_s[h * QB:(h + 1) * QB, :] = pos_q
    m_s[...] = jnp.full_like(m_s, NEG_BIG)
    l_s[...] = jnp.zeros_like(l_s)
    acc_s[...] = jnp.zeros_like(acc_s)

    scale = HEAD ** -0.5 * math.log2(math.e)

    def absorb(blocks, pos_rows):
        def gather(c0):
            return jnp.concatenate([kv_s[pl.ds(pl.multiple_of(b * KB, KB), KB), c0:c0 + HEAD] for b in blocks], axis=0)

        ks = [gather(g * HEAD) for g in range(n_kv)]
        vs = [gather((n_kv + g) * HEAD) for g in range(n_kv)]
        n = len(blocks)
        chains = [(g, slice((g * PARTS + i) * part_rows, (g * PARTS + i + 1) * part_rows)) for i in range(PARTS) for g in range(n_kv)]

        def scores(g, sl):
            return lax.dot_general(q_s[sl, :], ks[g], (((1,), (1,)), ((), ())), preferred_element_type=jnp.float32)

        ahead = [scores(*c) for c in chains[:AHEAD]]
        for i, (g, sl) in enumerate(chains):
            s = ahead[i]
            if i + AHEAD < len(chains):
                ahead.append(scores(*chains[i + AHEAD]))
            cols = [s[:, c * KB:(c + 1) * KB] * scale for c in range(n)]
            if pos_rows is not None:
                cols = [jnp.where(pr <= pq_s[...], c, NEG_BIG) for pr, c in zip(pos_rows, cols)]
            top = cols[0]
            for c in cols[1:]:
                top = jnp.maximum(top, c)
            m_old = m_s[sl, :]
            m_new = jnp.maximum(m_old, jnp.max(top, axis=-1, keepdims=True))
            alpha = jnp.exp2(m_old - m_new)
            p = [jnp.exp2(c - m_new) for c in cols]
            total = p[0]
            for c in p[1:]:
                total = total + c
            l_s[sl, :] = l_s[sl, :] * alpha + total
            pv = jnp.dot(jnp.concatenate([c.astype(jnp.bfloat16) for c in p], axis=1), vs[g], preferred_element_type=jnp.float32)
            acc_s[sl, :] = acc_s[sl, :] * alpha + pv
            m_s[sl, :] = m_new

    def full_step(i, _):
        absorb([full_l[i * WIDE + c] for c in range(WIDE)], None)
        return 0

    lax.fori_loop(0, n_groups, full_step, 0)

    def part_step(i, _):
        blocks = [part_l[i * GROUP + c] for c in range(GROUP)]
        absorb(blocks, [posk_ref[b] + jnp.where(i * GROUP + c < n_part, 0, 1 << 30) for c, b in enumerate(blocks)])
        return 0

    lax.fori_loop(0, n_mgroups, part_step, 0)

    for h in range(n_heads):
        sl = slice(h * QB, (h + 1) * QB)
        o_ref[:, h * HEAD:(h + 1) * HEAD] = (acc_s[sl, :] / jnp.sum(l_s[sl, :], axis=-1, keepdims=True)).astype(jnp.bfloat16)


TILE = 512
TILE_IN = 256
N_CHUNK = 8
A_CHUNKS = 3


def out_kernel(n_tp, n_cp, sl, oa_hbm, ob_hbm, la_hbm, w_hbm, wh0, wh1, wh2, wh3, wh4, wh5, x_hbm, out_ref, o_buf, w_buf, acc, w_t, x_t,
               o_send, o_recv, w_send, w_recv, w_local, ld_sem, own_sem):
    mesh_id = pl.DeviceIdType.MESH
    tp, dp, cp = lax.axis_index("tp"), lax.axis_index("dp"), lax.axis_index("cp")
    core, chip = cp % 2, cp // 2
    cp_y = cp + 2 - 4 * chip
    to_right, to_left = {"tp": (tp + 1) % n_tp}, {"tp": (tp + n_tp - 1) % n_tp}
    to_x, to_y, to_p = {"dp": 1 - dp}, {"cp": cp_y}, {"cp": cp + 1 - 2 * core}
    p_me, p_x, p_y, p_d = dp * n_cp + cp, (1 - dp) * n_cp + cp, dp * n_cp + cp_y, (1 - dp) * n_cp + cp_y
    n_rows, width = acc.shape
    ch = n_rows // N_CHUNK
    n_a = A_CHUNKS * ch
    n_tile = width // TILE
    last = n_tp - 1

    barrier = pltpu.get_barrier_semaphore()
    for peer in (to_right, to_left, to_x, to_y, to_p):
        pl.semaphore_signal(barrier, inc=1, device_id=peer, device_id_type=mesh_id)
    pl.semaphore_wait(barrier, 5)

    def o_copy(s, c):
        at = pl.ds(c * ch, ch)
        if s == 0:
            src = ob_hbm.at[pl.ds(c * ch - n_a, ch), :]
        elif s == 1 and c < A_CHUNKS:
            src = la_hbm.at[at, :]
        else:
            src = o_buf.at[s, at, :]
        return pltpu.make_async_remote_copy(src_ref=src, dst_ref=o_buf.at[s + 1, at, :], send_sem=o_send.at[s, c],
                                            recv_sem=o_recv.at[s, c], device_id=to_right, device_id_type=mesh_id)

    def rows(p, first=0, n=None):
        return pl.ds(pl.multiple_of(p * sl + first, sl // 2), sl if n is None else n)

    def w_copy(k, kind):
        hs = sl // 2
        idx, peer, where = {
            "own_x": (0, to_x, rows(p_me)), "own_y": (1, to_y, rows(p_me)), "own_p": (2, to_p, rows(p_me)),
            "dx": (3, to_x, rows(p_y, hs, hs)), "dy": (4, to_y, rows(p_x, 0, hs)),
            "px": (5, to_p, rows(p_x)), "py": (6, to_p, rows(p_y)),
            "pd0": (7, to_p, rows(p_d, 0, hs)), "pd1": (8, to_p, rows(p_d, hs, hs)),
        }[kind]
        at = w_buf.at[k, where, :]
        return pltpu.make_async_remote_copy(src_ref=at, dst_ref=at, send_sem=w_send.at[k, idx],
                                            recv_sem=w_recv.at[k, idx], device_id=peer, device_id_type=mesh_id)

    hs = sl // 2

    def w_own_half(k, h):
        src = ((wh0, wh1), (wh2, wh3), (wh4, wh5))[k][h]
        return pltpu.make_async_copy(src, w_buf.at[k, rows(p_me, h * hs, hs), :], w_local.at[k, h])

    def start_own(k):
        for h in (0, 1):
            w_own_half(k, h).wait()
        for kind in ("own_x", "own_y", "own_p"):
            w_copy(k, kind).start()

    def pass_on(k):
        w_copy(k, "own_x").wait_recv()
        w_copy(k, "own_y").wait_recv()
        for kind in ("dx", "dy", "px", "py"):
            w_copy(k, kind).start()

    def pass_diag(k):
        w_copy(k, "dy").wait_recv()
        w_copy(k, "pd0").start()
        w_copy(k, "dx").wait_recv()
        w_copy(k, "pd1").start()

    def complete(k):
        for kind in ("own_p", "px", "py", "pd0", "pd1"):
            w_copy(k, kind).wait_recv()

    def arrive(s, c):
        o_copy(s - 1, c).wait_recv()
        if s < last:
            o_copy(s, c).start()

    def tile_cols(t, size=TILE):
        return pl.ds(pl.multiple_of(t * size, size), size)

    def accum(s, r0, r1):
        def body(t, _):
            cols = tile_cols(t)
            acc[r0:r1, cols] += jnp.dot(o_buf[s, r0:r1, :], w_buf[s - 1, :, cols], preferred_element_type=jnp.float32)
            return 0

        lax.fori_loop(0, n_tile, body, 0)

    for k in range(last):
        for h in (0, 1):
            w_own_half(k, h).start()
    for c in range(N_CHUNK):
        o_copy(1 if c < A_CHUNKS else 0, c).start()
    start_own(0)
    own = [pltpu.make_async_copy(oa_hbm, o_buf.at[0, pl.ds(0, n_a), :], own_sem.at[0]),
           pltpu.make_async_copy(ob_hbm, o_buf.at[0, pl.ds(n_a, n_rows - n_a), :], own_sem.at[1]),
           pltpu.make_async_copy(la_hbm, o_buf.at[1, pl.ds(0, n_a), :], own_sem.at[2])]
    for d in own:
        d.start()

    def loads(t, slot):
        cols = tile_cols(t, TILE_IN)
        return (pltpu.make_async_copy(w_hbm.at[:, cols], w_t.at[slot], ld_sem.at[slot, 0]),
                pltpu.make_async_copy(x_hbm.at[:, cols], x_t.at[slot], ld_sem.at[slot, 1]))

    for d in loads(0, 0):
        d.start()
    for d in own:
        d.wait()

    def first(t, _):
        slot = t % 2

        @pl.when(t + 1 < width // TILE_IN)
        def _():
            for d in loads(t + 1, (t + 1) % 2):
                d.start()

        for d in loads(t, slot):
            d.wait()
        acc[:, tile_cols(t, TILE_IN)] = x_t[slot].astype(jnp.float32) + jnp.dot(o_buf[0], w_t[slot], preferred_element_type=jnp.float32)
        return 0

    lax.fori_loop(0, width // TILE_IN, first, 0)

    def finish(r0, r1):
        def body(t, _):
            cols = tile_cols(t)
            y = acc[r0:r1, cols] + jnp.dot(o_buf[last, r0:r1, :], w_buf[last - 1, :, cols], preferred_element_type=jnp.float32)
            out_ref[r0:r1, cols] = y.astype(jnp.bfloat16)
            return 0

        lax.fori_loop(0, n_tile, body, 0)

    pass_on(0)
    start_own(1)
    for c in range(A_CHUNKS):
        arrive(2, c)
    arrive(1, 3)
    arrive(1, 4)
    pass_diag(0)
    arrive(1, 5)
    complete(0)
    accum(1, 0, 6 * ch)
    arrive(1, 6)
    arrive(1, 7)
    accum(1, 6 * ch, n_rows)
    pass_on(1)
    start_own(2)
    pass_diag(1)
    arrive(2, 3)
    complete(1)
    accum(2, 0, 4 * ch)
    arrive(2, 4)
    arrive(2, 5)
    accum(2, 4 * ch, 6 * ch)
    arrive(2, 6)
    pass_on(2)
    arrive(2, 7)
    accum(2, 6 * ch, n_rows)
    pass_diag(2)
    complete(2)
    for c in range(5):
        arrive(3, c)
    finish(0, 5 * ch)
    arrive(3, 5)
    arrive(3, 6)
    finish(5 * ch, 7 * ch)
    arrive(3, 7)
    finish(7 * ch, n_rows)

    for s in range(last):
        for c in range(N_CHUNK):
            if s > 0 or c >= A_CHUNKS:
                o_copy(s, c).wait_send()
        for kind in ("own_x", "own_y", "own_p", "dx", "dy", "px", "py", "pd0", "pd1"):
            w_copy(s, kind).wait_send()


def solution(mesh):
    n_tp, n_cp, n_dp = mesh.shape["tp"], mesh.shape["cp"], mesh.shape["dp"]
    plane = n_dp * n_cp
    ring = [(i, (i + 1) % n_tp) for i in range(n_tp)]

    def local_block(hidden, tok_pos, norm_gain, w_query, w_key, w_value, w_out):
        rows, width = hidden.shape
        q_cols, k_cols = w_query.shape[1], w_key.shape[1]
        n_kv = k_cols // HEAD
        slice_rows = w_out.shape[0] // plane
        freqs = rope_freqs()
        smem = pl.BlockSpec(memory_space=pltpu.SMEM)
        anym = pl.BlockSpec(memory_space=pl.ANY)
        vmem = pl.BlockSpec(memory_space=pltpu.VMEM)
        pos_row = tok_pos.reshape(rows // KB, 1, KB)
        n_rb = rows // FRONT_ROWS
        kv_all, pos_all, q_rot, *near = pl.pallas_call(
            functools.partial(front_kernel, n_tp, n_cp, slice_rows),
            out_shape=(jax.ShapeDtypeStruct((n_cp * rows, 2 * k_cols), jnp.bfloat16), jax.ShapeDtypeStruct((n_cp,) + pos_row.shape, jnp.int32),
                       jax.ShapeDtypeStruct((rows, q_cols), jnp.bfloat16), *[jax.ShapeDtypeStruct((slice_rows // 2, width), jnp.bfloat16)] * 3),
            in_specs=[anym, vmem, vmem, anym, anym, anym, anym, vmem],
            out_specs=(anym,) * 6,
            scratch_shapes=[
                pltpu.VMEM((2, FRONT_ROWS, width), jnp.bfloat16),
                pltpu.VMEM((rows, width), jnp.bfloat16),
                pltpu.VMEM((width, 2 * k_cols), jnp.bfloat16),
                pltpu.VMEM((width, q_cols), jnp.bfloat16),
                pltpu.VMEM((n_rb, FRONT_ROWS, 2 * k_cols), jnp.bfloat16),
                pltpu.VMEM((2, rows, FRONT_COLS), jnp.bfloat16),
                pltpu.VMEM((rows, HEAD), jnp.float32),
                pltpu.VMEM((rows, HEAD), jnp.float32),
                pltpu.SemaphoreType.DMA((2,)),
                pltpu.SemaphoreType.DMA((3,)),
                pltpu.SemaphoreType.DMA((n_rb,)),
                pltpu.SemaphoreType.DMA((2,)),
                pltpu.SemaphoreType.DMA((n_cp - 1,)),
                pltpu.SemaphoreType.DMA((n_cp - 1,)),
                pltpu.SemaphoreType.DMA((3, n_rb)),
                pltpu.SemaphoreType.DMA((3, n_rb)),
                pltpu.SemaphoreType.DMA((3,)),
                pltpu.SemaphoreType.DMA((3,)),
                pltpu.SemaphoreType.DMA,
            ],
            compiler_params=pltpu.CompilerParams(collective_id=1, has_side_effects=True, vmem_limit_bytes=63 << 20),
            cost_estimate=pl.CostEstimate(flops=2 * rows * width * (q_cols + 2 * k_cols), bytes_accessed=24 << 20, transcendentals=0),
            name="front",
        )(hidden, pos_row, norm_gain.reshape(1, width), w_key, w_value, w_query, w_out, freqs)
        far_y = lax.ppermute(near[1], "tp", ring)
        far_x = lax.ppermute(near[2], "tp", ring)
        far_last = lax.ppermute(far_y, "tp", ring)
        pos_rel = pos_all.reshape(-1, 1, KB)

        kmin, kmax = jnp.min(pos_rel, axis=(1, 2)), jnp.max(pos_rel, axis=(1, 2))
        n_q = rows // QB

        def attend(first, steps):
            n_rows = (q_cols // HEAD) * QB
            blocks_max = n_cp * rows // KB
            return pl.pallas_call(
                functools.partial(attn_kernel, first),
                grid=(steps,),
                out_shape=jax.ShapeDtypeStruct((steps * QB, q_cols), jnp.bfloat16),
                in_specs=[smem] * 2 + [pl.BlockSpec((QB, q_cols), lambda i: (first + i, 0)), pl.BlockSpec(pos_rel.shape, lambda i: (0, 0, 0)), anym],
                out_specs=pl.BlockSpec((QB, q_cols), lambda i: (i, 0)),
                scratch_shapes=[
                    pltpu.VMEM((n_cp * rows, 2 * k_cols), jnp.bfloat16),
                    pltpu.VMEM((n_rows, HEAD), jnp.bfloat16),
                    pltpu.VMEM((n_rows // n_kv // PARTS, HEAD), jnp.int32),
                    pltpu.VMEM((n_rows, HEAD), jnp.float32),
                    pltpu.VMEM((n_rows, HEAD), jnp.float32),
                    pltpu.VMEM((n_rows, HEAD), jnp.float32),
                    pltpu.SMEM((blocks_max + WIDE,), jnp.int32),
                    pltpu.SMEM((blocks_max + WIDE + GROUP,), jnp.int32),
                    pltpu.SemaphoreType.DMA,
                ],
                cost_estimate=pl.CostEstimate(flops=4 * steps * QB * n_cp * rows * q_cols, bytes_accessed=8 << 20, transcendentals=0),
                name="attend",
            )(kmin, kmax, q_rot, pos_rel, kv_all)

        o_a = attend(0, A_CHUNKS)
        left_a = lax.ppermute(o_a, "tp", ring)
        o_b = attend(A_CHUNKS, n_q - A_CHUNKS)
        hidden_out = pl.pallas_call(
            functools.partial(out_kernel, n_tp, n_cp, slice_rows),
            out_shape=pltpu.VMEM((rows, width), jnp.bfloat16),
            in_specs=[anym] * 11,
            out_specs=vmem,
            scratch_shapes=[
                pltpu.VMEM((n_tp, rows, q_cols), jnp.bfloat16),
                pltpu.VMEM((n_tp - 1, q_cols, width), jnp.bfloat16),
                pltpu.VMEM((rows, width), jnp.float32),
                pltpu.VMEM((2, q_cols, TILE_IN), jnp.bfloat16),
                pltpu.VMEM((2, rows, TILE_IN), jnp.bfloat16),
                pltpu.SemaphoreType.DMA((n_tp - 1, N_CHUNK)),
                pltpu.SemaphoreType.DMA((n_tp - 1, N_CHUNK)),
                pltpu.SemaphoreType.DMA((n_tp - 1, 9)),
                pltpu.SemaphoreType.DMA((n_tp - 1, 9)),
                pltpu.SemaphoreType.DMA((n_tp - 1, 2)),
                pltpu.SemaphoreType.DMA((2, 2)),
                pltpu.SemaphoreType.DMA((3,)),
            ],
            compiler_params=pltpu.CompilerParams(collective_id=0, has_side_effects=True, vmem_limit_bytes=53 << 20),
            cost_estimate=pl.CostEstimate(flops=2 * n_tp * rows * q_cols * width, bytes_accessed=48 << 20, transcendentals=0),
            name="out_gather",
        )(o_a, o_b, left_a, w_out, *near, far_y, far_x, far_last, hidden)
        k_cache = kv_all[:rows, :k_cols].reshape(rows, n_kv, HEAD)
        v_cache = kv_all[:rows, k_cols:].reshape(rows, n_kv, HEAD)
        return hidden_out, k_cache, v_cache

    row_spec = P(("dp", "cp"), None)
    cache_spec = P(("dp", "cp"), "tp", None)
    return jax.shard_map(local_block, mesh=mesh, in_specs=(row_spec, P(("dp", "cp")), P(None), P(None, "tp"), P(None, "tp"), P(None, "tp"), P("tp", None)), out_specs=(row_spec, cache_spec, cache_spec), check_vma=False)
```

```python
import functools
import math

import jax
import jax.numpy as jnp
import numpy as np
from jax import lax
from jax.experimental import pallas as pl
from jax.experimental.pallas import tpu as pltpu
from jax.sharding import PartitionSpec as P


HEAD = 128
THETA = 1000000
EPS = 1e-5
NEG_BIG = -1e30
KB = 128
GROUP = 4
WIDE = 8
PARTS = 1
AHEAD = 2
QB = 128


def rope_freqs():
    freq = (1.0 / (float(THETA) ** (np.arange(0, HEAD, 2) / HEAD))).astype(np.float32)
    return jnp.asarray(np.concatenate([freq, freq])[None, :])


def rotate(x_f32, cos_tab, sin_tab):
    x = x_f32.astype(jnp.bfloat16).astype(jnp.float32)
    return (x * cos_tab + pltpu.roll(x, HEAD // 2, 1) * sin_tab).astype(jnp.bfloat16)


FRONT_ROWS = 256
FRONT_COLS = 256


def front_kernel(n_tp, n_cp, slice_rows, x_hbm, pos_ref, gain_ref, wk_hbm, wv_hbm, wq_hbm, wo_hbm, freq_ref, kv_hbm, pos_out, q_hbm, k_hbm, v_hbm, wz_hbm, wy_hbm, wx_hbm,
                 x_t, normed, wkv, wq_v, kv_t, q_t, cos_ref, sin_ref, x_sem, w_sem, kv_sem, q_sem, p_send, p_recv, s_send, s_recv, z_send, z_recv, own_pos_sem, cache_sem):
    mesh_id = pl.DeviceIdType.MESH
    tp, dp, cp = lax.axis_index("tp"), lax.axis_index("dp"), lax.axis_index("cp")
    to_right, to_left = {"tp": (tp + 1) % n_tp}, {"tp": (tp + n_tp - 1) % n_tp}
    core, chip = cp % 2, cp // 2
    cp_p, cp_y = cp + 1 - 2 * core, cp + 2 - 4 * chip
    to_p, to_y, to_d = {"cp": cp_p}, {"cp": cp_y}, {"cp": cp_y + 1 - 2 * core}
    rows = normed.shape[0]
    k_cols = wk_hbm.shape[1]
    n_rb = rows // FRONT_ROWS
    n_cb = wq_hbm.shape[1] // FRONT_COLS

    def x_load(r):
        return pltpu.make_async_copy(x_hbm.at[pl.ds(r * FRONT_ROWS, FRONT_ROWS), :], x_t.at[r % 2], x_sem.at[r % 2])

    weights = [pltpu.make_async_copy(wk_hbm, wkv.at[:, pl.ds(0, k_cols)], w_sem.at[0]),
               pltpu.make_async_copy(wv_hbm, wkv.at[:, pl.ds(k_cols, k_cols)], w_sem.at[1]),
               pltpu.make_async_copy(wq_hbm, wq_v, w_sem.at[2])]
    x_load(0).start()
    weights[0].start()
    weights[1].start()
    x_load(1).start()
    weights[2].start()

    barrier = pltpu.get_barrier_semaphore()
    for peer in (to_p, to_y, to_d, to_right, to_left):
        pl.semaphore_signal(barrier, inc=1, device_id=peer, device_id_type=mesh_id)
    pl.semaphore_wait(barrier, 5)

    hs = slice_rows // 2
    own = (dp * n_cp + cp) * slice_rows

    def z_copy(i):
        src, dst = ((wo_hbm.at[pl.ds(pl.multiple_of(own, hs), hs), :], wz_hbm),
                    (wo_hbm.at[pl.ds(pl.multiple_of(own + hs, hs), hs), :], wy_hbm),
                    (wz_hbm, wx_hbm))[i]
        return pltpu.make_async_remote_copy(src_ref=src, dst_ref=dst, send_sem=z_send.at[i], recv_sem=z_recv.at[i],
                                            device_id=to_right, device_id_type=mesh_id)

    z_copy(0).start()
    z_copy(1).start()

    n_pos = pos_ref.shape[0]
    pos_copies = [pltpu.make_async_remote_copy(src_ref=pos_ref, dst_ref=pos_out.at[pl.ds((i + 1) * n_pos, n_pos)], send_sem=p_send.at[i], recv_sem=p_recv.at[i],
                                               device_id=peer, device_id_type=mesh_id) for i, peer in enumerate((to_p, to_y, to_d))]
    pos_copies.append(pltpu.make_async_copy(pos_ref, pos_out.at[pl.ds(0, n_pos)], own_pos_sem))
    for c in pos_copies:
        c.start()

    def send(kind, r):
        src = (0, 0, 2)[kind] * rows + r * FRONT_ROWS
        dst = (1, 2, 3)[kind] * rows + r * FRONT_ROWS
        return pltpu.make_async_remote_copy(src_ref=kv_hbm.at[pl.ds(src, FRONT_ROWS), :], dst_ref=kv_hbm.at[pl.ds(dst, FRONT_ROWS), :],
                                            send_sem=s_send.at[kind, r], recv_sem=s_recv.at[kind, r],
                                            device_id=(to_p, to_y, to_p)[kind], device_id_type=mesh_id)

    def kv_store(r):
        return pltpu.make_async_copy(kv_t.at[r], kv_hbm.at[pl.ds(r * FRONT_ROWS, FRONT_ROWS), :], kv_sem.at[r])

    def cache_stores(r):
        at = pl.ds(r * FRONT_ROWS, FRONT_ROWS)
        return (pltpu.make_async_copy(kv_t.at[r, :, pl.ds(0, k_cols)], k_hbm.at[at, :], cache_sem.at[r, 0]),
                pltpu.make_async_copy(kv_t.at[r, :, pl.ds(k_cols, k_cols)], v_hbm.at[at, :], cache_sem.at[r, 1]))

    def spread(r):
        kv_store(r).wait()
        send(1, r).start()
        send(0, r).start()

    sign = jnp.where(lax.broadcasted_iota(jnp.int32, (KB, HEAD), 1) < HEAD // 2, -1.0, 1.0).astype(jnp.float32)

    def rope_rows(r):
        for j in range(r * FRONT_ROWS // KB, (r + 1) * FRONT_ROWS // KB):
            pos = jnp.transpose(jnp.broadcast_to(pos_ref[j].astype(jnp.float32), (HEAD, KB)))
            angle = pos * freq_ref[...]
            cos_ref[j * KB:(j + 1) * KB, :] = jnp.cos(angle)
            sin_ref[j * KB:(j + 1) * KB, :] = jnp.sin(angle) * sign

    for r in range(n_rb):
        at = slice(r * FRONT_ROWS, (r + 1) * FRONT_ROWS)
        rope_rows(r)
        x_load(r).wait()
        x = x_t[r % 2].astype(jnp.float32)
        var = jnp.mean(x * x, axis=-1, keepdims=True)
        normed[at, :] = (x * lax.rsqrt(var + EPS) * gain_ref[...]).astype(jnp.bfloat16)
        if r + 2 < n_rb:
            x_load(r + 2).start()
        if r == 0:
            weights[0].wait()
            weights[1].wait()
        kv = jnp.dot(normed[at, :], wkv[...], preferred_element_type=jnp.float32)
        for h in range(k_cols // HEAD):
            kv_t[r, :, h * HEAD:(h + 1) * HEAD] = rotate(kv[:, h * HEAD:(h + 1) * HEAD], cos_ref[at, :], sin_ref[at, :])
        kv_t[r, :, k_cols:] = kv[:, k_cols:].astype(jnp.bfloat16)
        kv_store(r).start()
        for c in cache_stores(r):
            c.start()
        if r > 0:
            spread(r - 1)

    weights[2].wait()
    z_copy(0).wait_recv()
    z_copy(2).start()

    def q_store(c):
        return pltpu.make_async_copy(q_t.at[c % 2], q_hbm.at[:, pl.ds(c * FRONT_COLS, FRONT_COLS)], q_sem.at[c % 2])

    for c in range(n_cb):
        if c == 0:
            spread(n_rb - 1)
        if c >= 2:
            q_store(c - 2).wait()
        q = jnp.dot(normed[...], wq_v[:, c * FRONT_COLS:(c + 1) * FRONT_COLS], preferred_element_type=jnp.float32)
        for h in range(FRONT_COLS // HEAD):
            q_t[c % 2, :, h * HEAD:(h + 1) * HEAD] = rotate(q[:, h * HEAD:(h + 1) * HEAD], cos_ref[...], sin_ref[...])
        q_store(c).start()
        if c < n_rb:
            send(1, c).wait_recv()
            send(2, c).start()
    for r in range(n_cb, n_rb):
        send(1, r).wait_recv()
        send(2, r).start()

    q_store(n_cb - 2).wait()
    q_store(n_cb - 1).wait()
    for r in range(n_rb):
        send(0, r).wait_recv()
        send(2, r).wait_recv()
    for c in pos_copies:
        c.wait()
    for r in range(n_rb):
        for c in cache_stores(r):
            c.wait()
    z_copy(1).wait_recv()
    z_copy(2).wait_recv()
    for i in range(3):
        z_copy(i).wait_send()
    for kind in range(3):
        for r in range(n_rb):
            send(kind, r).wait_send()


def attn_kernel(first, kmin_ref, kmax_ref, q_ref, posk_ref, kv_hbm, o_ref,
                kv_s, q_s, pq_s, m_s, l_s, acc_s, full_l, part_l, sem):
    step = pl.program_id(0)
    n_blocks = kmin_ref.shape[0]
    n_kv = kv_hbm.shape[1] // (2 * HEAD)
    n_heads = q_ref.shape[1] // HEAD
    per_kv = n_heads // n_kv

    @pl.when(step == 0)
    def _():
        pltpu.make_async_copy(kv_hbm, kv_s, sem).start()

    q_lo = kmin_ref[first + step]
    q_hi = kmax_ref[first + step]

    def classify(j, counts):
        n_full, n_part = counts
        lo, hi = kmin_ref[j], kmax_ref[j]
        is_full = hi <= q_lo
        is_part = jnp.logical_and(lo <= q_hi, jnp.logical_not(is_full))

        full_l[n_full] = j
        part_l[n_part] = j
        return n_full + is_full.astype(jnp.int32), n_part + is_part.astype(jnp.int32)

    n_full, n_part = lax.fori_loop(0, n_blocks, classify, (0, 0), unroll=8)
    n_groups = n_full // WIDE

    def move(i, n_part):
        part_l[n_part] = full_l[n_groups * WIDE + i]
        return n_part + 1

    n_part = lax.fori_loop(0, n_full - n_groups * WIDE, move, n_part)
    n_mgroups = (n_part + GROUP - 1) // GROUP

    def pad(i, _):
        part_l[n_part + i] = 0
        return 0

    lax.fori_loop(0, n_mgroups * GROUP - n_part, pad, 0)

    for h in range(n_heads):
        q_s[h * QB:(h + 1) * QB, :] = q_ref[:, h * HEAD:(h + 1) * HEAD]
    part_rows = per_kv * QB // PARTS
    pos_q = jnp.transpose(jnp.broadcast_to(posk_ref[first + step], (HEAD, QB)))
    for h in range(part_rows // QB):
        pq_s[h * QB:(h + 1) * QB, :] = pos_q
    m_s[...] = jnp.full_like(m_s, NEG_BIG)
    l_s[...] = jnp.zeros_like(l_s)
    acc_s[...] = jnp.zeros_like(acc_s)

    @pl.when(step == 0)
    def _():
        pltpu.make_async_copy(kv_hbm, kv_s, sem).wait()

    scale = HEAD ** -0.5 * math.log2(math.e)

    def absorb(blocks, pos_rows):
        def gather(c0):
            return jnp.concatenate([kv_s[pl.ds(pl.multiple_of(b * KB, KB), KB), c0:c0 + HEAD] for b in blocks], axis=0)

        ks = [gather(g * HEAD) for g in range(n_kv)]
        vs = [gather((n_kv + g) * HEAD) for g in range(n_kv)]
        n = len(blocks)
        chains = [(g, slice((g * PARTS + i) * part_rows, (g * PARTS + i + 1) * part_rows)) for i in range(PARTS) for g in range(n_kv)]

        def scores(g, sl):
            return lax.dot_general(q_s[sl, :], ks[g], (((1,), (1,)), ((), ())), preferred_element_type=jnp.float32)

        ahead = [scores(*c) for c in chains[:AHEAD]]
        for i, (g, sl) in enumerate(chains):
            s = ahead[i]
            if i + AHEAD < len(chains):
                ahead.append(scores(*chains[i + AHEAD]))
            cols = [s[:, c * KB:(c + 1) * KB] * scale for c in range(n)]
            if pos_rows is not None:
                cols = [jnp.where(pr <= pq_s[...], c, NEG_BIG) for pr, c in zip(pos_rows, cols)]
            top = cols[0]
            for c in cols[1:]:
                top = jnp.maximum(top, c)
            m_old = m_s[sl, :]
            m_new = jnp.maximum(m_old, jnp.max(top, axis=-1, keepdims=True))
            alpha = jnp.exp2(m_old - m_new)
            p = [jnp.exp2(c - m_new) for c in cols]
            total = p[0]
            for c in p[1:]:
                total = total + c
            l_s[sl, :] = l_s[sl, :] * alpha + total
            pv = jnp.dot(jnp.concatenate([c.astype(jnp.bfloat16) for c in p], axis=1), vs[g], preferred_element_type=jnp.float32)
            acc_s[sl, :] = acc_s[sl, :] * alpha + pv
            m_s[sl, :] = m_new

    def full_step(i, _):
        absorb([full_l[i * WIDE + c] for c in range(WIDE)], None)
        return 0

    lax.fori_loop(0, n_groups, full_step, 0)

    def part_step(i, _):
        blocks = [part_l[i * GROUP + c] for c in range(GROUP)]
        absorb(blocks, [posk_ref[b] + jnp.where(i * GROUP + c < n_part, 0, 1 << 30) for c, b in enumerate(blocks)])
        return 0

    lax.fori_loop(0, n_mgroups, part_step, 0)

    for h in range(n_heads):
        sl = slice(h * QB, (h + 1) * QB)
        o_ref[:, h * HEAD:(h + 1) * HEAD] = (acc_s[sl, :] / jnp.sum(l_s[sl, :], axis=-1, keepdims=True)).astype(jnp.bfloat16)


TILE = 512
TILE_IN = 256
N_CHUNK = 8
A_CHUNKS = 3


def out_kernel(n_tp, n_cp, sl, oa_hbm, ob_hbm, la_hbm, w_hbm, wh0, wh1, wh2, wh3, wh4, wh5, x_hbm, out_ref, o_buf, w_buf, acc, w_t, x_t,
               o_send, o_recv, w_send, w_recv, w_local, ld_sem, own_sem):
    mesh_id = pl.DeviceIdType.MESH
    tp, dp, cp = lax.axis_index("tp"), lax.axis_index("dp"), lax.axis_index("cp")
    core, chip = cp % 2, cp // 2
    cp_y = cp + 2 - 4 * chip
    to_right, to_left = {"tp": (tp + 1) % n_tp}, {"tp": (tp + n_tp - 1) % n_tp}
    to_x, to_y, to_p = {"dp": 1 - dp}, {"cp": cp_y}, {"cp": cp + 1 - 2 * core}
    p_me, p_x, p_y, p_d = dp * n_cp + cp, (1 - dp) * n_cp + cp, dp * n_cp + cp_y, (1 - dp) * n_cp + cp_y
    n_rows, width = acc.shape
    ch = n_rows // N_CHUNK
    n_a = A_CHUNKS * ch
    n_tile = width // TILE
    last = n_tp - 1

    barrier = pltpu.get_barrier_semaphore()
    for peer in (to_right, to_left, to_x, to_y, to_p):
        pl.semaphore_signal(barrier, inc=1, device_id=peer, device_id_type=mesh_id)
    pl.semaphore_wait(barrier, 5)

    def o_copy(s, c):
        at = pl.ds(c * ch, ch)
        if s == 0:
            src = ob_hbm.at[pl.ds(c * ch - n_a, ch), :]
        elif s == 1 and c < A_CHUNKS:
            src = la_hbm.at[at, :]
        else:
            src = o_buf.at[s, at, :]
        return pltpu.make_async_remote_copy(src_ref=src, dst_ref=o_buf.at[s + 1, at, :], send_sem=o_send.at[s, c],
                                            recv_sem=o_recv.at[s, c], device_id=to_right, device_id_type=mesh_id)

    def rows(p, first=0, n=None):
        return pl.ds(pl.multiple_of(p * sl + first, sl // 2), sl if n is None else n)

    def w_copy(k, kind):
        hs = sl // 2
        idx, peer, where = {
            "own_x": (0, to_x, rows(p_me)), "own_y": (1, to_y, rows(p_me)), "own_p": (2, to_p, rows(p_me)),
            "dx": (3, to_x, rows(p_y, hs, hs)), "dy": (4, to_y, rows(p_x, 0, hs)),
            "px": (5, to_p, rows(p_x)), "py": (6, to_p, rows(p_y)),
            "pd0": (7, to_p, rows(p_d, 0, hs)), "pd1": (8, to_p, rows(p_d, hs, hs)),
        }[kind]
        at = w_buf.at[k, where, :]
        return pltpu.make_async_remote_copy(src_ref=at, dst_ref=at, send_sem=w_send.at[k, idx],
                                            recv_sem=w_recv.at[k, idx], device_id=peer, device_id_type=mesh_id)

    hs = sl // 2

    def w_own_half(k, h):
        src = ((wh0, wh1), (wh2, wh3), (wh4, wh5))[k][h]
        return pltpu.make_async_copy(src, w_buf.at[k, rows(p_me, h * hs, hs), :], w_local.at[k, h])

    def start_own(k):
        for h in (0, 1):
            w_own_half(k, h).wait()
        for kind in ("own_x", "own_y", "own_p"):
            w_copy(k, kind).start()

    def pass_on(k):
        w_copy(k, "own_x").wait_recv()
        w_copy(k, "own_y").wait_recv()
        for kind in ("dx", "dy", "px", "py"):
            w_copy(k, kind).start()

    def pass_diag(k):
        w_copy(k, "dy").wait_recv()
        w_copy(k, "pd0").start()
        w_copy(k, "dx").wait_recv()
        w_copy(k, "pd1").start()

    def complete(k):
        for kind in ("own_p", "px", "py", "pd0", "pd1"):
            w_copy(k, kind).wait_recv()

    def arrive(s, c):
        o_copy(s - 1, c).wait_recv()
        if s < last:
            o_copy(s, c).start()

    def tile_cols(t, size=TILE):
        return pl.ds(pl.multiple_of(t * size, size), size)

    def accum(s, r0, r1):
        def body(t, _):
            cols = tile_cols(t)
            acc[r0:r1, cols] += jnp.dot(o_buf[s, r0:r1, :], w_buf[s - 1, :, cols], preferred_element_type=jnp.float32)
            return 0

        lax.fori_loop(0, n_tile, body, 0)

    for c in range(N_CHUNK):
        o_copy(1 if c < A_CHUNKS else 0, c).start()
    for k in range(last):
        for h in (0, 1):
            w_own_half(k, h).start()
    start_own(0)
    own = [pltpu.make_async_copy(oa_hbm, o_buf.at[0, pl.ds(0, n_a), :], own_sem.at[0]),
           pltpu.make_async_copy(ob_hbm, o_buf.at[0, pl.ds(n_a, n_rows - n_a), :], own_sem.at[1]),
           pltpu.make_async_copy(la_hbm, o_buf.at[1, pl.ds(0, n_a), :], own_sem.at[2])]
    for d in own:
        d.start()

    def loads(t, slot):
        cols = tile_cols(t, TILE_IN)
        return (pltpu.make_async_copy(w_hbm.at[:, cols], w_t.at[slot], ld_sem.at[slot, 0]),
                pltpu.make_async_copy(x_hbm.at[:, cols], x_t.at[slot], ld_sem.at[slot, 1]))

    for d in loads(0, 0):
        d.start()
    for d in own:
        d.wait()

    def first(t, _):
        slot = t % 2

        @pl.when(t + 1 < width // TILE_IN)
        def _():
            for d in loads(t + 1, (t + 1) % 2):
                d.start()

        for d in loads(t, slot):
            d.wait()
        acc[:, tile_cols(t, TILE_IN)] = x_t[slot].astype(jnp.float32) + jnp.dot(o_buf[0], w_t[slot], preferred_element_type=jnp.float32)
        return 0

    lax.fori_loop(0, width // TILE_IN, first, 0)

    def finish(r0, r1):
        def body(t, _):
            cols = tile_cols(t)
            y = acc[r0:r1, cols] + jnp.dot(o_buf[last, r0:r1, :], w_buf[last - 1, :, cols], preferred_element_type=jnp.float32)
            out_ref[r0:r1, cols] = y.astype(jnp.bfloat16)
            return 0

        lax.fori_loop(0, n_tile, body, 0)

    pass_on(0)
    start_own(1)
    for c in range(A_CHUNKS):
        arrive(2, c)
    arrive(1, 3)
    arrive(1, 4)
    pass_diag(0)
    arrive(1, 5)
    complete(0)
    accum(1, 0, 6 * ch)
    arrive(1, 6)
    arrive(1, 7)
    accum(1, 6 * ch, n_rows)
    pass_on(1)
    start_own(2)
    pass_diag(1)
    arrive(2, 3)
    complete(1)
    accum(2, 0, 4 * ch)
    arrive(2, 4)
    arrive(2, 5)
    accum(2, 4 * ch, 6 * ch)
    arrive(2, 6)
    pass_on(2)
    arrive(2, 7)
    accum(2, 6 * ch, n_rows)
    pass_diag(2)
    complete(2)
    for c in range(5):
        arrive(3, c)
    finish(0, 5 * ch)
    arrive(3, 5)
    arrive(3, 6)
    finish(5 * ch, 7 * ch)
    arrive(3, 7)
    finish(7 * ch, n_rows)

    for s in range(last):
        for c in range(N_CHUNK):
            if s > 0 or c >= A_CHUNKS:
                o_copy(s, c).wait_send()
        for kind in ("own_x", "own_y", "own_p", "dx", "dy", "px", "py", "pd0", "pd1"):
            w_copy(s, kind).wait_send()


def solution(mesh):
    n_tp, n_cp, n_dp = mesh.shape["tp"], mesh.shape["cp"], mesh.shape["dp"]
    plane = n_dp * n_cp
    ring = [(i, (i + 1) % n_tp) for i in range(n_tp)]

    def local_block(hidden, tok_pos, norm_gain, w_query, w_key, w_value, w_out):
        rows, width = hidden.shape
        q_cols, k_cols = w_query.shape[1], w_key.shape[1]
        n_kv = k_cols // HEAD
        slice_rows = w_out.shape[0] // plane
        freqs = rope_freqs()
        smem = pl.BlockSpec(memory_space=pltpu.SMEM)
        anym = pl.BlockSpec(memory_space=pl.ANY)
        vmem = pl.BlockSpec(memory_space=pltpu.VMEM)
        pos_row = tok_pos.reshape(rows // KB, 1, KB)
        n_rb = rows // FRONT_ROWS
        kv_all, pos_rel, q_rot, k_own, v_own, *near = pl.pallas_call(
            functools.partial(front_kernel, n_tp, n_cp, slice_rows),
            out_shape=(jax.ShapeDtypeStruct((n_cp * rows, 2 * k_cols), jnp.bfloat16), jax.ShapeDtypeStruct((n_cp * rows // KB, 1, KB), jnp.int32),
                       jax.ShapeDtypeStruct((rows, q_cols), jnp.bfloat16),
                       *[jax.ShapeDtypeStruct((rows, k_cols), jnp.bfloat16)] * 2, *[jax.ShapeDtypeStruct((slice_rows // 2, width), jnp.bfloat16)] * 3),
            in_specs=[anym, vmem, vmem, anym, anym, anym, anym, vmem],
            out_specs=(anym,) * 8,
            scratch_shapes=[
                pltpu.VMEM((2, FRONT_ROWS, width), jnp.bfloat16),
                pltpu.VMEM((rows, width), jnp.bfloat16),
                pltpu.VMEM((width, 2 * k_cols), jnp.bfloat16),
                pltpu.VMEM((width, q_cols), jnp.bfloat16),
                pltpu.VMEM((n_rb, FRONT_ROWS, 2 * k_cols), jnp.bfloat16),
                pltpu.VMEM((2, rows, FRONT_COLS), jnp.bfloat16),
                pltpu.VMEM((rows, HEAD), jnp.float32),
                pltpu.VMEM((rows, HEAD), jnp.float32),
                pltpu.SemaphoreType.DMA((2,)),
                pltpu.SemaphoreType.DMA((3,)),
                pltpu.SemaphoreType.DMA((n_rb,)),
                pltpu.SemaphoreType.DMA((2,)),
                pltpu.SemaphoreType.DMA((n_cp - 1,)),
                pltpu.SemaphoreType.DMA((n_cp - 1,)),
                pltpu.SemaphoreType.DMA((3, n_rb)),
                pltpu.SemaphoreType.DMA((3, n_rb)),
                pltpu.SemaphoreType.DMA((3,)),
                pltpu.SemaphoreType.DMA((3,)),
                pltpu.SemaphoreType.DMA,
                pltpu.SemaphoreType.DMA((n_rb, 2)),
            ],
            compiler_params=pltpu.CompilerParams(collective_id=1, has_side_effects=True, vmem_limit_bytes=63 << 20),
            cost_estimate=pl.CostEstimate(flops=2 * rows * width * (q_cols + 2 * k_cols), bytes_accessed=24 << 20, transcendentals=0),
            name="front",
        )(hidden, pos_row, norm_gain.reshape(1, width), w_key, w_value, w_query, w_out, freqs)
        far_y = lax.ppermute(near[1], "tp", ring)
        far_x = lax.ppermute(near[2], "tp", ring)
        far_last = lax.ppermute(far_y, "tp", ring)

        kmin, kmax = jnp.min(pos_rel, axis=(1, 2)), jnp.max(pos_rel, axis=(1, 2))
        n_q = rows // QB

        def attend(first, steps):
            n_rows = (q_cols // HEAD) * QB
            blocks_max = n_cp * rows // KB
            return pl.pallas_call(
                functools.partial(attn_kernel, first),
                grid=(steps,),
                out_shape=jax.ShapeDtypeStruct((steps * QB, q_cols), jnp.bfloat16),
                in_specs=[smem] * 2 + [pl.BlockSpec((QB, q_cols), lambda i: (first + i, 0)), pl.BlockSpec(pos_rel.shape, lambda i: (0, 0, 0)), anym],
                out_specs=pl.BlockSpec((QB, q_cols), lambda i: (i, 0)),
                scratch_shapes=[
                    pltpu.VMEM((n_cp * rows, 2 * k_cols), jnp.bfloat16),
                    pltpu.VMEM((n_rows, HEAD), jnp.bfloat16),
                    pltpu.VMEM((n_rows // n_kv // PARTS, HEAD), jnp.int32),
                    pltpu.VMEM((n_rows, HEAD), jnp.float32),
                    pltpu.VMEM((n_rows, HEAD), jnp.float32),
                    pltpu.VMEM((n_rows, HEAD), jnp.float32),
                    pltpu.SMEM((blocks_max + WIDE,), jnp.int32),
                    pltpu.SMEM((blocks_max + WIDE + GROUP,), jnp.int32),
                    pltpu.SemaphoreType.DMA,
                ],
                cost_estimate=pl.CostEstimate(flops=4 * steps * QB * n_cp * rows * q_cols, bytes_accessed=8 << 20, transcendentals=0),
                compiler_params=pltpu.CompilerParams(vmem_limit_bytes=63 << 20),
                name="attend",
            )(kmin, kmax, q_rot, pos_rel, kv_all)

        o_a = attend(0, A_CHUNKS)
        left_a = lax.ppermute(o_a, "tp", ring)
        o_b = attend(A_CHUNKS, n_q - A_CHUNKS)
        hidden_out = pl.pallas_call(
            functools.partial(out_kernel, n_tp, n_cp, slice_rows),
            out_shape=pltpu.VMEM((rows, width), jnp.bfloat16),
            in_specs=[anym] * 11,
            out_specs=vmem,
            scratch_shapes=[
                pltpu.VMEM((n_tp, rows, q_cols), jnp.bfloat16),
                pltpu.VMEM((n_tp - 1, q_cols, width), jnp.bfloat16),
                pltpu.VMEM((rows, width), jnp.float32),
                pltpu.VMEM((2, q_cols, TILE_IN), jnp.bfloat16),
                pltpu.VMEM((2, rows, TILE_IN), jnp.bfloat16),
                pltpu.SemaphoreType.DMA((n_tp - 1, N_CHUNK)),
                pltpu.SemaphoreType.DMA((n_tp - 1, N_CHUNK)),
                pltpu.SemaphoreType.DMA((n_tp - 1, 9)),
                pltpu.SemaphoreType.DMA((n_tp - 1, 9)),
                pltpu.SemaphoreType.DMA((n_tp - 1, 2)),
                pltpu.SemaphoreType.DMA((2, 2)),
                pltpu.SemaphoreType.DMA((3,)),
            ],
            compiler_params=pltpu.CompilerParams(collective_id=0, has_side_effects=True, vmem_limit_bytes=53 << 20),
            cost_estimate=pl.CostEstimate(flops=2 * n_tp * rows * q_cols * width, bytes_accessed=48 << 20, transcendentals=0),
            name="out_gather",
        )(o_a, o_b, left_a, w_out, *near, far_y, far_x, far_last, hidden)
        k_cache = k_own.reshape(rows, n_kv, HEAD)
        v_cache = v_own.reshape(rows, n_kv, HEAD)
        return hidden_out, k_cache, v_cache

    row_spec = P(("dp", "cp"), None)
    cache_spec = P(("dp", "cp"), "tp", None)
    return jax.shard_map(local_block, mesh=mesh, in_specs=(row_spec, P(("dp", "cp")), P(None), P(None, "tp"), P(None, "tp"), P(None, "tp"), P("tp", None)), out_specs=(row_spec, cache_spec, cache_spec), check_vma=False)
```
